128 devices in a mesh: row: 16 (over z_hi, y, core), col: 8 (over x, z_lo).
Axes of the slice: x: 4, y: 4, z: 4 (z_hi: 2, z_lo: 2; z = z_hi * 2 + z_lo), core: 2. Of those that a mesh axis runs over, the one named last changes fastest.
Arguments:
- observed: float32 [2048, 4096], P('row', 'col'), may hold values from -6 to 6
- psf_table: bfloat16 [64, 31, 31], replicated, may hold values from 0.049804688 to 1
- psf_index: int32 [16, 32], P('row', 'col'), may hold values from 0 to 63
- start_image: float32 [2048, 4096], P('row', 'col'), may hold values from -6 to 6
- blur_dual: float32 [2048, 4096], P('row', 'col'), may hold values from -6 to 6
- tv_dual: float32 [2, 2048, 4096], P(None, 'row', 'col'), may hold values from -1.8 to 1.8
Outputs:
- restored: float32 [2048, 4096], P('row', 'col')
- blur_dual_out: float32 [2048, 4096], P('row', 'col')
The draws below stay inside these ranges and needn't reach their ends.
Inputs may be any that keep to these rules, and one draw needn't show every extreme that they name: `psf_index`: each entry names a row of psf_table.
All inputs are finite; a program needn't handle non-finite values.
Results may differ from the reference program's by a relative error of at most 0.0003.
Values may be sent and summed in bfloat16 or wider, within the bound.
No kernel may reach another device: no remote copies, remote signals or barrier semaphores. Data moves between devices by JAX's collectives and lax.ppermute only.
A program may use at most 128 MiB of HBM per device.

```python
import math
import jax
import jax.numpy as jnp
from jax import lax

KS = 31
PR = 128
PC = 128
NPSF = 64
ITERS = 2
NX = 2048
NY = 4096
NPC = 32
N_ROW = 16


def plant(values, own_key, low, high):
    spot = [jax.random.randint(jax.random.fold_in(own_key, axis), (), 0, length) for axis, length in enumerate(values.shape)]
    widest = values.shape.index(max(values.shape))
    neighbour = spot[:widest] + [(spot[widest] + 1) % values.shape[widest]] + spot[widest + 1:]
    return values.at[tuple(spot)].set(low).at[tuple(neighbour)].set(high)


def steps_of(own_key, extent, split, low, largest):
    level = 1.0
    for position, parts in split:
        steps = jax.random.uniform(jax.random.fold_in(jax.random.fold_in(own_key, 6), position), (parts,), jnp.float32, low / len(split), largest / len(split))
        level = level * jnp.repeat(jnp.exp(steps), extent[position] // parts).reshape((-1,) + (1,) * (len(extent) - 1 - position))
    return level


def noise(rng, shape, scale, limit, split=(), kind=jnp.bfloat16):
    factor_of = steps_of(rng, shape, split, -0.22, 0.18) if split else 1.0
    array = jax.random.normal(rng, shape, jnp.float32) * scale * factor_of
    return jnp.minimum(jnp.maximum(array, -limit), limit).astype(kind)


def setup_inputs(seed: int = 0) -> dict:
    key_of = jax.random.split(jax.random.key(seed), 7)
    observed = noise(key_of[0], (NX, NY), 1.0, 6.0, ((0, 16), (1, 8)), jnp.float32)
    psf_table = jnp.clip(jnp.exp(jax.random.uniform(key_of[1], (NPSF, KS, KS), jnp.float32, math.log(0.049804688), math.log(1.0))), 0.049804688, 1.0).astype(jnp.bfloat16)
    psf_index = plant(jax.random.randint(key_of[2], (N_ROW, NPC), 0, NPSF), jax.random.fold_in(key_of[2], 1), 0, NPSF - 1).astype(jnp.int32)
    start_image = noise(key_of[3], (NX, NY), 1.0, 6.0, ((0, 16), (1, 8)), jnp.float32)
    blur_dual = noise(key_of[4], (NX, NY), 1.0, 6.0, ((0, 16), (1, 8)), jnp.float32)
    tv_dual = noise(key_of[5], (2, NX, NY), 0.3, 1.8, ((1, 16), (2, 8)), jnp.float32)
    return {"observed": observed, "psf_table": psf_table, "psf_index": psf_index, "start_image": start_image, "blur_dual": blur_dual, "tv_dual": tv_dual}


sigma_step = 0.15
tau_step = 0.6
tv_weight = 0.5
group_size = 4

def make_select(kernel_size, patch_cols):
    half_width = kernel_size // 2
    column_in = jnp.arange(patch_cols + 2 * half_width, dtype=jnp.int32)[None, :, None]
    column_out = jnp.arange(patch_cols, dtype=jnp.int32)[None, None, :]
    tap_index = jnp.arange(kernel_size, dtype=jnp.int32)[:, None, None]
    return (column_in - column_out == tap_index).astype(jnp.float32)

def strip_pass(strip_in, observed_s, dual_s, index_s, kern_flat, select):
    kernel_size = select.shape[0]
    patch_cols = select.shape[2]
    half_width = (select.shape[1] - patch_cols) // 2
    patch_rows, width = observed_s.shape
    group_span = group_size * patch_cols
    group_count = width // group_span
    table_size = kern_flat.shape[0]

    def one_group(spread_sum, group_id):
        first_col = group_id * group_span
        window = lax.dynamic_slice_in_dim(strip_in, first_col, group_span + 2 * half_width, 1)
        pieces = jnp.stack([window[:, member * patch_cols:member * patch_cols + patch_cols + 2 * half_width] for member in range(group_size)])
        stacked = jnp.stack([pieces[:, tap_row:tap_row + patch_rows, :] for tap_row in range(kernel_size)], axis=2)
        patch_ids = lax.dynamic_slice_in_dim(index_s, group_id * group_size, group_size)
        onehot = (patch_ids[:, None] == jnp.arange(table_size, dtype=jnp.int32)[None, :]).astype(jnp.float32)
        kernels = jnp.dot(onehot, kern_flat, precision=lax.Precision.HIGHEST).reshape(group_size, kernel_size, kernel_size)
        toeplitz = jnp.einsum('pab,bkj->pakj', kernels, select, precision=lax.Precision.HIGHEST)
        blurred = jnp.einsum('piak,pakj->pij', stacked, toeplitz, precision=lax.Precision.HIGHEST)
        blurred = blurred.transpose(1, 0, 2).reshape(patch_rows, group_span)
        seen_group = lax.dynamic_slice_in_dim(observed_s, first_col, group_span, 1)
        dual_group = lax.dynamic_slice_in_dim(dual_s, first_col, group_span, 1)
        dual_new = (dual_group + sigma_step * (blurred - seen_group)) / (1.0 + sigma_step)
        rounded = lax.optimization_barrier(dual_new.astype(jnp.bfloat16)).astype(jnp.float32)
        rounded = rounded.reshape(patch_rows, group_size, patch_cols).transpose(1, 0, 2)
        padded_dual = jnp.pad(rounded, ((0, 0), (kernel_size - 1, kernel_size - 1), (0, 0)))
        shifted = jnp.stack([padded_dual[:, kernel_size - 1 - tap_row:kernel_size - 1 - tap_row + patch_rows + 2 * half_width, :] for tap_row in range(kernel_size)], axis=2)
        spread = jnp.einsum('praj,pakj->prk', shifted, toeplitz, precision=lax.Precision.HIGHEST)
        merged = jnp.zeros((patch_rows + 2 * half_width, group_span + 2 * half_width), jnp.float32)
        for member in range(group_size):
            merged = merged.at[:, member * patch_cols:member * patch_cols + patch_cols + 2 * half_width].add(spread[member])
        previous = lax.dynamic_slice_in_dim(spread_sum, first_col, group_span + 2 * half_width, 1)
        spread_sum = lax.dynamic_update_slice_in_dim(spread_sum, previous + merged, first_col, 1)
        return (spread_sum, dual_new)
    start_sum = jnp.zeros((patch_rows + 2 * half_width, width + 2 * half_width), jnp.float32)
    spread_sum, duals = lax.scan(one_group, start_sum, jnp.arange(group_count, dtype=jnp.int32))
    return (duals.transpose(1, 0, 2).reshape(patch_rows, width), spread_sum)

def reference(observed, psf_table, psf_index, start_image, blur_dual, tv_dual):
    half_width = KS // 2
    table = psf_table.astype(jnp.float32)
    normed = table / lax.optimization_barrier(jnp.sum(table, axis=(1, 2), keepdims=True))
    kern_flat = lax.optimization_barrier(normed.astype(jnp.bfloat16)).astype(jnp.float32).reshape(NPSF, KS * KS)
    select = make_select(KS, PC)
    restored = start_image
    extrapolated = start_image
    dual_now = blur_dual
    tv_rows = tv_dual[0]
    tv_cols = tv_dual[1]
    keep_rows = (jnp.arange(NX, dtype=jnp.int32) < NX - 1)[:, None]
    keep_cols = (jnp.arange(NY, dtype=jnp.int32) < NY - 1)[None, :]
    for step in range(ITERS):
        padded = lax.optimization_barrier(jnp.pad(extrapolated, half_width).astype(jnp.bfloat16)).astype(jnp.float32)

        def one_strip(carry, strip_id):
            start_row = strip_id * PR
            strip_in = lax.dynamic_slice_in_dim(padded, start_row, PR + 2 * half_width, 0)
            seen_strip = lax.dynamic_slice_in_dim(observed, start_row, PR, 0)
            dual_strip = lax.dynamic_slice_in_dim(dual_now, start_row, PR, 0)
            index_strip = lax.dynamic_index_in_dim(psf_index, strip_id, 0, keepdims=False)
            new_dual, spread_sum = strip_pass(strip_in, seen_strip, dual_strip, index_strip, kern_flat, select)
            return (carry, (new_dual, spread_sum))
        unused, (dual_strips, spread_strips) = lax.scan(one_strip, jnp.zeros((), jnp.float32), jnp.arange(N_ROW, dtype=jnp.int32))
        dual_now = dual_strips.reshape(NX, NY)

        def add_strip(strip_id, total):
            piece = spread_strips[strip_id]
            start_row = (strip_id * PR).astype(jnp.int32)
            zero_col = jnp.zeros((), jnp.int32)
            previous = lax.dynamic_slice(total, (start_row, zero_col), piece.shape)
            return lax.dynamic_update_slice(total, previous + piece, (start_row, zero_col))
        total = lax.fori_loop(0, N_ROW, add_strip, jnp.zeros((NX + 2 * half_width, NY + 2 * half_width), jnp.float32))
        adjoint = total[half_width:half_width + NX, half_width:half_width + NY]
        below = jnp.concatenate([extrapolated[1:], jnp.zeros((1, NY), jnp.float32)], axis=0)
        right = jnp.concatenate([extrapolated[:, 1:], jnp.zeros((NX, 1), jnp.float32)], axis=1)
        grad_rows = jnp.where(keep_rows, below - extrapolated, 0.0)
        grad_cols = jnp.where(keep_cols, right - extrapolated, 0.0)
        moved_rows = tv_rows + sigma_step * grad_rows
        moved_cols = tv_cols + sigma_step * grad_cols
        shrink = jnp.maximum(1.0, jnp.sqrt(moved_rows * moved_rows + moved_cols * moved_cols) / tv_weight)
        tv_rows = moved_rows / shrink
        tv_cols = moved_cols / shrink
        masked_rows = jnp.where(keep_rows, tv_rows, 0.0)
        masked_cols = jnp.where(keep_cols, tv_cols, 0.0)
        diverge = masked_rows - jnp.concatenate([jnp.zeros((1, NY), jnp.float32), masked_rows[:-1]], axis=0)
        diverge = diverge + masked_cols - jnp.concatenate([jnp.zeros((NX, 1), jnp.float32), masked_cols[:, :-1]], axis=1)
        next_image = restored - tau_step * (adjoint - diverge)
        extrapolated = 2.0 * next_image - restored
        restored = next_image
    return (restored, dual_now)
```

```python
import jax
import jax.numpy as jnp
from jax import lax
from jax.experimental import pallas as pl
from jax.experimental.pallas import tpu as pltpu
from jax.sharding import PartitionSpec as P

SIGMA = 0.15
TAU = 0.6
TV = 0.5
F32 = jnp.float32
BF16 = jnp.bfloat16

ROWS = 128
COLS = 512
XO = 48
YO = 32
WIDE = 640
SEGS = ((0, 16, 32), (16, 128, 144), (144, 16, 32))
PATCHES = ((0,), (1, 2, 3, 4), (5, 6, 7, 8), (9, 10, 11, 12), (13, 14, 15, 16), (17,))


def iota(shape, dim):
    return lax.broadcasted_iota(jnp.int32, shape, dim)


def split(value):
    hi = value.astype(BF16).astype(F32)
    return hi, value - hi


def lanes(value, shift):
    shift = shift % value.shape[1]
    return pltpu.roll(value, shift, 1) if shift else value


def rows(value, shift):
    shift = shift % value.shape[0]
    return pltpu.roll(value, shift, 0) if shift else value


def between(shape, lo, hi):
    lane = iota(shape, 1)
    return (lane >= lo) & (lane < hi)


def flags():
    row = lax.axis_index("row")
    col = lax.axis_index("col")
    return (
        row > 0,
        row < lax.axis_size("row") - 1,
        col > 0,
        col < lax.axis_size("col") - 1,
    )


def pack_rows_kernel(x_ref, y_ref, o_ref, q_ref, idx_ref, down_ref, up_ref):
    for out, near, far, edge in ((down_ref, 112, 96, 127), (up_ref, 0, 0, 0)):
        out[0:32] = x_ref[far : far + 32].astype(BF16)
        seen = o_ref[near : near + 16]
        hi, lo = split(y_ref[near : near + 16] - SIGMA * seen)
        out[32:48] = hi.astype(BF16)
        out[48:64] = lo.astype(BF16)
        out[64:80] = seen.astype(BF16)
        a_hi, a_lo = split(q_ref[0, edge : edge + 1])
        b_hi, b_lo = split(q_ref[1, edge : edge + 1])
        x_lo = split(x_ref[edge : edge + 1])[1]
        row = iota((16, COLS), 0)
        misc = jnp.zeros((16, COLS), F32)
        for place, part in enumerate((x_lo, a_hi, a_lo, b_hi, b_lo, idx_ref[0:1])):
            misc = jnp.where(row == place, part, misc)
        out[80:96] = misc.astype(BF16)


def pack_cols_kernel(x_ref, y_ref, o_ref, q_ref, idx_ref, top_ref, bot_ref, right_ref, left_ref):
    for out, base, spots in (
        (right_ref, 384, (48, 64, 80, 96, (97, 98, 99, 100, 101))),
        (left_ref, 0, (48, 0, 16, 32, (96, 97, 98, 99, 100))),
    ):
        own = slice(base, base + 128)
        top = top_ref[:, own].astype(F32)
        bot = bot_ref[:, own].astype(F32)
        seen = o_ref[:, own]
        x = x_ref[:, own]
        c_hi, c_lo = split(y_ref[:, own] - SIGMA * seen)
        x_hi, x_lo = split(x)

        def rolled(middle, section, shift, size):
            first = lanes(top[section : section + size], shift)
            last = lanes(bot[section : section + size], shift)
            return jnp.concatenate([first, lanes(middle, shift), last], axis=0)

        shape = (192, 128)
        fill = jnp.zeros((32, 128), F32)
        buf = rolled(x_hi, 0, spots[0], 32)
        right = base > 0
        x_at = 16 if right else 48
        buf = jnp.where(between(shape, x_at, x_at + 32), buf, 0.0)
        at = 48 if right else 0
        for which, (middle, section) in enumerate(((c_hi, 32), (c_lo, 48), (seen, 64))):
            part = jnp.concatenate([rolled(middle, section, spots[1 + which], 16), fill], axis=0)
            start = at + 16 * which
            buf = jnp.where(between(shape, start, start + 16), part, buf)
        a_hi, a_lo = split(q_ref[0, :, own])
        b_hi, b_lo = split(q_ref[1, :, own])
        rix = iota((32, 128), 0)
        for which, middle in enumerate((x_lo, a_hi, a_lo, b_hi, b_lo)):
            shift = spots[4][which]
            first = jnp.where(rix == 31, top[80 + which : 81 + which], 0.0)
            last = jnp.where(rix == 0, bot[80 + which : 81 + which], 0.0)
            part = jnp.concatenate(
                [lanes(first, shift), lanes(middle, shift), lanes(last, shift)], axis=0
            )
            buf = jnp.where(between(shape, 96 + which, 97 + which), part, buf)
        spot = 4 if right else 1
        row = iota((192, 1), 0)
        mine = idx_ref[0:1, spot : spot + 1]
        above = top_ref[85:86, spot : spot + 1].astype(F32)
        below = bot_ref[85:86, spot : spot + 1].astype(F32)
        entry = jnp.where(row == 0, above, jnp.where(row == 1, mine, below))
        buf = jnp.where(between(shape, 101, 102), entry, buf)
        out[...] = buf.astype(BF16)


def pack_cols2_kernel(xb_ref, top_ref, bot_ref, right_ref, left_ref):
    for out, tile, at in ((right_ref, 4, 16), (left_ref, 0, 48)):
        own = slice(128 * tile, 128 * tile + 128)
        hi, lo = split(xb_ref[:, own])
        top = top_ref[:, own].astype(F32)
        bot = bot_ref[:, own].astype(F32)
        shape = (192, 128)
        buf = jnp.concatenate([top[0:32], hi, bot[0:32]], axis=0)
        rix = iota((32, 128), 0)
        low = jnp.concatenate(
            [
                jnp.where(rix == 31, top[32:33], 0.0),
                lo,
                jnp.where(rix == 0, bot[32:33], 0.0),
            ],
            axis=0,
        )
        source = 47 if tile == 4 else 48
        buf = jnp.where(between(shape, at, at + 32), buf, 0.0)
        buf = jnp.where(between(shape, 96, 97), lanes(low, 96 - source), buf)
        out[...] = buf.astype(BF16)


def build_taps(tab_ref, t_ref):
    k = iota((32, 128), 0)
    j = iota((32, 128), 1) % 32
    lower = j <= k
    for patch in range(18):
        at = 8 * (patch // 6) + patch % 6
        for a1 in range(4):
            for half in range(2):
                e = 2 * a1 + half
                line = tab_ref[at : at + 1, 128 * e : 128 * e + 128]
                spread = jnp.broadcast_to(line, (32, 128))
                low = pltpu.roll(spread, 97, 1, stride=1, stride_axis=0)
                high = pltpu.roll(low, 32, 1)
                block = jnp.concatenate(
                    [jnp.where(lower, low, 0.0), jnp.where(lower, 0.0, high)], axis=0
                )
                t_ref[patch, 64 * a1 : 64 * a1 + 64, 128 * half : 128 * half + 128] = block.astype(
                    BF16
                )


def windows(xe_ref, p_ref):
    low = between((192, 128), 0, 64)
    tail = between((192, 128), 96, 128)
    for tile in range(5):
        here = slice(128 * tile, 128 * tile + 128)
        x0 = xe_ref[0:192, here]
        x8 = xe_ref[8:200, here]
        p_ref[4 * tile] = jnp.where(low, x0, lanes(x8, 64)).astype(BF16)
        p_ref[4 * tile + 1] = jnp.where(low, lanes(x0, 96), lanes(x8, 32)).astype(BF16)
        if tile < 4:
            after = slice(128 * tile + 128, 128 * tile + 256)
            p_ref[4 * tile + 2] = jnp.where(low, lanes(x0, 64), x8).astype(BF16)
            w0 = jnp.where(tail, x0, xe_ref[0:192, after])
            w8 = jnp.where(tail, x8, xe_ref[8:200, after])
            p_ref[4 * tile + 3] = jnp.where(low, lanes(w0, 32), lanes(w8, 96)).astype(BF16)


def blur(p_ref, t_ref, a_ref, c_ref, y_ref, row_ok, col_ok):
    for seg, (first, size, padded) in enumerate(SEGS):
        for patch, blocks in enumerate(PATCHES):
            lhs = jnp.concatenate(
                [
                    jnp.concatenate(
                        [
                            p_ref[b, first : first + padded],
                            p_ref[b, first + 16 : first + 16 + padded],
                        ],
                        axis=1,
                    )
                    for b in blocks
                ],
                axis=0,
            )
            v = jnp.dot(lhs, t_ref[6 * seg + patch], preferred_element_type=F32)
            for place, b in enumerate(blocks):
                part = v[place * padded : place * padded + padded]
                a_ref[b, 0:padded] = part[:, :128] + rows(part[:, 128:], -4)
        low = between((padded, 128), 0, 64)
        even = iota((padded, 128), 1) % 64 < 32
        for tile in range(5):
            a = [a_ref[4 * tile + p, 0:padded] for p in range(2 if tile == 4 else 4)]
            if tile == 4:
                a += [jnp.zeros_like(a[0])] * 2
            e = []
            for p in range(2):
                z = lanes(jnp.where(low, a[p + 2], a[p]), 64)
                e.append(jnp.where(low, a[p], z) + rows(jnp.where(low, z, a[p + 2]), -2))
            m1 = jnp.where(even, e[0], lanes(e[1], 32))
            m2 = jnp.where(even, lanes(e[0], 96), e[1])
            blurred = (m1 + rows(m2, -1))[0:size]
            here = slice(128 * tile, 128 * tile + 128)
            new = (c_ref[first : first + size, here] + SIGMA * blurred) / (1.0 + SIGMA)
            keep = col_ok(tile, size) & row_ok(seg)
            y_ref[first : first + size, here] = jnp.where(keep, new, 0.0)


def adjoint(y_ref, t_ref, l_ref, f_ref, z_ref):
    z_ref[...] = jnp.zeros_like(z_ref)
    for seg, (first, size, padded) in enumerate(SEGS):
        low = between((padded, 128), 0, 64)
        even = iota((padded, 128), 1) % 64 < 32
        for tile in range(5):
            here = slice(128 * tile, 128 * tile + 128)
            o = jnp.concatenate(
                [y_ref[first : first + size, here], jnp.zeros((padded - size, 128), F32)], axis=0
            )
            o1 = rows(o, 1)
            e = [jnp.where(even, o, lanes(o1, 32)), jnp.where(even, lanes(o, 96), o1)]
            for p in range(2):
                s = rows(e[p], 2)
                parts = [(p, jnp.where(low, e[p], lanes(s, 64)))]
                if tile < 4:
                    parts.append((p + 2, jnp.where(low, lanes(e[p], 64), s)))
                for place, part in parts:
                    b = 4 * tile + place
                    l_ref[b, 0:padded, 0:128] = part.astype(BF16)
                    l_ref[b, 0:padded, 128:256] = rows(part, 4).astype(BF16)
        for patch, blocks in enumerate(PATCHES):
            lhs = jnp.concatenate([l_ref[b, 0:padded] for b in blocks], axis=0)
            g = lax.dot_general(
                lhs, t_ref[6 * seg + patch], (((1,), (1,)), ((), ())), preferred_element_type=F32
            )
            zero = jnp.zeros((16, 128), F32)
            for place, b in enumerate(blocks):
                part = g[place * padded : place * padded + padded]
                f_ref[b, 0 : padded + 16] = jnp.concatenate(
                    [part[:, :128], zero], axis=0
                ) + jnp.concatenate([zero, part[:, 128:]], axis=0)
        tall = padded + 24
        low = between((tall, 128), 0, 64)
        head = between((tall, 128), 0, 32)
        pad8 = jnp.zeros((8, 128), F32)
        for tile in range(5):
            both = []
            for p in range(2):
                fa = f_ref[4 * tile + p, 0 : padded + 16]
                a0 = jnp.concatenate([fa, pad8], axis=0)
                a8 = jnp.concatenate([pad8, fa], axis=0)
                if tile < 4:
                    fb = f_ref[4 * tile + p + 2, 0 : padded + 16]
                    b0 = jnp.concatenate([fb, pad8], axis=0)
                    b8 = jnp.concatenate([pad8, fb], axis=0)
                    both.append(jnp.where(low, a0, b8) + lanes(jnp.where(low, b0, a8), 64))
                else:
                    both.append(jnp.where(low, a0 + lanes(a8, 64), 0.0))
            turned = lanes(both[1], 32)
            here = slice(128 * tile, 128 * tile + 128)
            span = slice(first, first + tall)
            z_ref[span, here] += both[0] + jnp.where(head, 0.0, turned)
            if tile < 4:
                after = slice(128 * tile + 128, 128 * tile + 256)
                z_ref[span, after] += jnp.where(head, turned, 0.0)


def total_variation(xe_ref, q1_ref, q2_ref, q1o_ref, q2o_ref, place_row, place_col, limit_row, limit_col):
    for chunk in range(9):
        start = 16 * chunk
        x = xe_ref[24 + start : 40 + start, 0:WIDE]
        tall = xe_ref[24 + start : 48 + start, 0:WIDE]
        below = rows(tall, -1)[0:16]
        right = lanes(x, -1)
        r = place_row - 8 + start + iota((16, WIDE), 0)
        c = place_col - XO + iota((16, WIDE), 1)
        g1 = jnp.where(r < limit_row, below - x, 0.0)
        g2 = jnp.where(c < limit_col, right - x, 0.0)
        span = slice(start, start + 16)
        u1 = q1_ref[span] + SIGMA * g1
        u2 = q2_ref[span] + SIGMA * g2
        shrink = jnp.maximum(1.0, jnp.sqrt(u1 * u1 + u2 * u2) / TV)
        inv = 1.0 / shrink
        q1o_ref[span] = u1 * inv
        q2o_ref[span] = u2 * inv


def divergence(q1_ref, q2_ref, chunk, place_row, place_col, limit_row, limit_col):
    start = 8 + 16 * chunk
    m1 = q1_ref[start - 8 : start + 16]
    m2 = q2_ref[start : start + 16]
    r = place_row + 16 * chunk - 8 + iota((24, WIDE), 0)
    c = place_col - XO + iota((16, WIDE), 1)
    m1 = jnp.where((r >= 0) & (r < limit_row), m1, 0.0)
    m2 = jnp.where((c >= 0) & (c < limit_col), m2, 0.0)
    return (m1 - rows(m1, 1))[8:24] + (m2 - lanes(m2, 1))


def places():
    row = lax.axis_index("row")
    col = lax.axis_index("col")
    return (
        row * ROWS,
        col * COLS,
        lax.axis_size("row") * ROWS - 1,
        lax.axis_size("col") * COLS - 1,
    )


def masks():
    top, bot, left, right = flags()

    def row_ok(seg):
        if seg == 1:
            return jnp.bool_(True)
        return top if seg == 0 else bot

    def col_ok(tile, size):
        lane = iota((size, 128), 1)
        if tile == 0:
            return (lane >= YO) | left
        if tile == 4:
            return (lane < YO) | right
        return jnp.ones((size, 128), jnp.bool_)

    return row_ok, col_ok


def widen(value, shift):
    pad = jnp.zeros((value.shape[0], WIDE - COLS), F32)
    return lanes(jnp.concatenate([value, pad], axis=1), shift)


def select_tables(table_ref, idx_ref, top_ref, bot_ref, lf_ref, rt_ref, tab_ref):
    lane = iota((1, 128), 1)
    total = jnp.full((1, 128), -1.0, F32)
    lines = (top_ref[80:96, 0:128].astype(F32)[5:6], idx_ref[0:1, 0:128], bot_ref[80:96, 0:128].astype(F32)[5:6])
    lf = lf_ref[0:16].astype(F32)
    rt = rt_ref[0:16].astype(F32)
    for r in range(3):
        line = jnp.where(lane == 0, lf[r : r + 1, 101:102], lines[r])
        line = jnp.where(lane == 5, rt[r : r + 1, 101:102], line)
        line = lanes(line, 8 * r) if r else line
        total = jnp.where((lane >= 8 * r) & (lane < 8 * r + 6), line, total)
    onehot = jnp.where(total == iota((64, 128), 0).astype(F32), 1.0, 0.0).astype(BF16)
    picked = lax.dot_general(
        onehot, table_ref[...], (((0,), (0,)), ((), ())), preferred_element_type=F32
    )
    tab_ref[...] = picked[0:24]


def first_kernel(
    x_ref, y_ref, o_ref, q_ref, idx_ref, table_ref, top_ref, bot_ref, lf_ref, rt_ref,
    x1_ref, xb_ref, c2_ref, q1o_ref, q2o_ref, tab_ref, down_ref, up_ref,
    xe_ref, c_ref, ob_ref, ys_ref, q1_ref, q2_ref, t_ref, p_ref, a_ref, l_ref, f_ref, z_ref,
):
    top_ok, bot_ok, left_ok, right_ok = flags()
    row0, col0, limit_row, limit_col = places()
    select_tables(table_ref, idx_ref, top_ref, bot_ref, lf_ref, rt_ref, tab_ref)
    build_taps(tab_ref, t_ref)
    misc_t = top_ref[80:96].astype(F32)
    misc_b = bot_ref[80:96].astype(F32)
    rix = iota((32, COLS), 0)
    above = top_ref[0:32].astype(F32) + jnp.where(rix == 31, misc_t[0:1], 0.0)
    below = bot_ref[0:32].astype(F32) + jnp.where(rix == 0, misc_b[0:1], 0.0)
    own = widen(x_ref[...], XO)
    xe_ref[0:32, 0:WIDE] = widen(jnp.where(top_ok, above, 0.0), XO)
    xe_ref[32:160, 0:WIDE] = own
    xe_ref[160:192, 0:WIDE] = widen(jnp.where(bot_ok, below, 0.0), XO)
    xe_ref[192:208, :] = jnp.zeros((16, 768), F32)
    xe_ref[0:208, 640:768] = jnp.zeros((208, 128), F32)
    rr = iota((192, 128), 0)
    rows_ok = ((rr >= 32) | top_ok) & ((rr < 160) | bot_ok)
    lf = jnp.where(rows_ok & left_ok, lf_ref[...].astype(F32), 0.0)
    rt = jnp.where(rows_ok & right_ok, rt_ref[...].astype(F32), 0.0)
    shape = (192, 128)
    add = jnp.where(between(shape, 16, 48), lf, 0.0)
    xe_ref[0:192, 0:128] += add + jnp.where(between(shape, 47, 48), lanes(lf, 79), 0.0)
    add = jnp.where(between(shape, 48, 80), rt, 0.0)
    xe_ref[0:192, 512:640] += add + jnp.where(between(shape, 48, 49), lanes(rt, 80), 0.0)
    seen = o_ref[...]
    c_ref[16:144] = widen(y_ref[...] - SIGMA * seen, YO)
    ob_ref[16:144] = widen(seen, YO)
    for ref, span in ((top_ref, slice(0, 16)), (bot_ref, slice(144, 160))):
        c_ref[span] = widen(ref[32:48].astype(F32) + ref[48:64].astype(F32), YO)
        ob_ref[span] = widen(ref[64:80].astype(F32), YO)
    lf = lf_ref[0:160].astype(F32)
    rt = rt_ref[0:160].astype(F32)
    shape = (160, 128)
    at = between(shape, 16, 32)
    c_ref[:, 0:128] = jnp.where(at, lanes(lf, 96) + lanes(lf, 80), c_ref[:, 0:128])
    ob_ref[:, 0:128] = jnp.where(at, lanes(lf, 64), ob_ref[:, 0:128])
    at = between(shape, 32, 48)
    c_ref[:, 512:640] = jnp.where(at, lanes(rt, 32) + lanes(rt, 16), c_ref[:, 512:640])
    ob_ref[:, 512:640] = jnp.where(at, rt, ob_ref[:, 512:640])
    lf = lf_ref[24:168].astype(F32)
    edge = between((144, 128), 47, 48)
    r8 = iota((8, COLS), 0)
    for comp, ref in ((0, q1_ref), (1, q2_ref)):
        line = misc_t[1 + 2 * comp : 2 + 2 * comp] + misc_t[2 + 2 * comp : 3 + 2 * comp]
        ref[0:8] = widen(jnp.where(r8 == 7, line, 0.0), XO)
        ref[8:136] = widen(q_ref[comp], XO)
        ref[136:144] = jnp.zeros((8, WIDE), F32)
        side = lanes(lf, 78 - 2 * comp) + lanes(lf, 77 - 2 * comp)
        ref[:, 0:128] = jnp.where(edge, side, ref[:, 0:128])
    row_ok, col_ok = masks()
    windows(xe_ref, p_ref)
    blur(p_ref, t_ref, a_ref, c_ref, ys_ref, row_ok, col_ok)
    total_variation(xe_ref, q1_ref, q2_ref, q1o_ref, q2o_ref, row0, col0, limit_row, limit_col)
    adjoint(ys_ref, t_ref, l_ref, f_ref, z_ref)
    c2_ref[...] = ys_ref[...] - SIGMA * ob_ref[...]
    for chunk in range(8):
        span = slice(16 * chunk, 16 * chunk + 16)
        ext = slice(32 + 16 * chunk, 48 + 16 * chunk)
        div = divergence(q1o_ref, q2o_ref, chunk, row0, col0, limit_row, limit_col)
        x = xe_ref[ext, 0:WIDE]
        new = x - TAU * (z_ref[ext, 0:WIDE] - div)
        x1_ref[span] = new
        xb_ref[span] = 2.0 * new - x
    row = iota((16, WIDE), 0)
    down_ref[0:32] = xb_ref[96:128].astype(BF16)
    up_ref[0:32] = xb_ref[0:32].astype(BF16)
    down_ref[32:48] = jnp.where(row == 0, split(xb_ref[127:128])[1], 0.0).astype(BF16)
    up_ref[32:48] = jnp.where(row == 0, split(xb_ref[0:1])[1], 0.0).astype(BF16)


def second_kernel(
    x1_ref, xb_ref, c2_ref, q1i_ref, q2i_ref, tab_ref, top_ref, bot_ref, lf_ref, rt_ref,
    x2_ref, y2_ref,
    xe_ref, ys_ref, q1_ref, q2_ref, t_ref, p_ref, a_ref, l_ref, f_ref, z_ref,
):
    top_ok, bot_ok, left_ok, right_ok = flags()
    row0, col0, limit_row, limit_col = places()
    build_taps(tab_ref, t_ref)
    lane = iota((32, WIDE), 1)
    own_lane = (lane >= XO) & (lane < XO + COLS)
    rix = iota((32, WIDE), 0)
    above = top_ref[0:32].astype(F32) + jnp.where(rix == 31, top_ref[32:48].astype(F32)[0:1], 0.0)
    below = bot_ref[0:32].astype(F32) + jnp.where(rix == 0, bot_ref[32:48].astype(F32)[0:1], 0.0)
    xe_ref[0:32, 0:WIDE] = jnp.where(own_lane & top_ok, above, 0.0)
    for chunk in range(4):
        span = slice(32 * chunk, 32 * chunk + 32)
        xe_ref[32 + 32 * chunk : 64 + 32 * chunk, 0:WIDE] = jnp.where(own_lane, xb_ref[span], 0.0)
    xe_ref[160:192, 0:WIDE] = jnp.where(own_lane & bot_ok, below, 0.0)
    xe_ref[192:208, :] = jnp.zeros((16, 768), F32)
    xe_ref[0:208, 640:768] = jnp.zeros((208, 128), F32)
    rr = iota((192, 128), 0)
    rows_ok = ((rr >= 32) | top_ok) & ((rr < 160) | bot_ok)
    lf = jnp.where(rows_ok & left_ok, lf_ref[...].astype(F32), 0.0)
    rt = jnp.where(rows_ok & right_ok, rt_ref[...].astype(F32), 0.0)
    shape = (192, 128)
    add = jnp.where(between(shape, 16, 48), lf, 0.0)
    xe_ref[0:192, 0:128] += add + jnp.where(between(shape, 47, 48), lanes(lf, 79), 0.0)
    add = jnp.where(between(shape, 48, 80), rt, 0.0)
    xe_ref[0:192, 512:640] += add + jnp.where(between(shape, 48, 49), lanes(rt, 80), 0.0)
    row_ok, col_ok = masks()
    windows(xe_ref, p_ref)
    blur(p_ref, t_ref, a_ref, c2_ref, ys_ref, row_ok, col_ok)
    total_variation(xe_ref, q1i_ref, q2i_ref, q1_ref, q2_ref, row0, col0, limit_row, limit_col)
    adjoint(ys_ref, t_ref, l_ref, f_ref, z_ref)
    for chunk in range(8):
        span = slice(16 * chunk, 16 * chunk + 16)
        ext = slice(32 + 16 * chunk, 48 + 16 * chunk)
        div = divergence(q1_ref, q2_ref, chunk, row0, col0, limit_row, limit_col)
        new = x1_ref[span] - TAU * (z_ref[ext, 0:WIDE] - div)
        x2_ref[span] = lanes(new, -XO)[:, :COLS]
        y2_ref[span] = lanes(ys_ref[16 + 16 * chunk : 32 + 16 * chunk], -YO)[:, :COLS]


def work_scratch():
    return [
        pltpu.VMEM((18, 256, 256), BF16),
        pltpu.VMEM((18, 192, 128), BF16),
        pltpu.VMEM((18, 144, 128), F32),
        pltpu.VMEM((18, 144, 256), BF16),
        pltpu.VMEM((18, 160, 128), F32),
        pltpu.VMEM((208, WIDE), F32),
    ]


def field(*shape, dtype=F32):
    return jax.ShapeDtypeStruct(shape, dtype)


def call(kernel, outs, scratch, *args, name):
    return pl.pallas_call(
        kernel,
        out_shape=outs,
        scratch_shapes=scratch,
        compiler_params=pltpu.CompilerParams(vmem_limit_bytes=56 * 1024 * 1024),
        name=name,
    )(*args)


def ring(block, axis, distance):
    count = lax.axis_size(axis)
    return lax.ppermute(block, axis, [(i, (i + distance) % count) for i in range(count)])


def per_device(observed, psf_table, psf_index, start_image, blur_dual, tv_dual):
    table = psf_table.astype(F32)
    normed = (table / jnp.sum(table, axis=(1, 2), keepdims=True)).astype(BF16)
    normed = jnp.pad(normed[:, :, ::-1], ((0, 0), (1, 0), (0, 1))).reshape(64, 1024)
    idx = jnp.pad(psf_index.astype(F32), ((0, 0), (1, COLS - 5)))
    strip = field(96, COLS, dtype=BF16)
    side = field(192, 128, dtype=BF16)
    down, up = call(
        pack_rows_kernel, (strip, strip), [], start_image, blur_dual, observed, tv_dual, idx,
        name="pack_rows",
    )
    top = ring(down, "row", 1)
    bot = ring(up, "row", -1)
    to_right, to_left = call(
        pack_cols_kernel, (side, side), [],
        start_image, blur_dual, observed, tv_dual, idx, top, bot, name="pack_cols",
    )
    lf = ring(to_right, "col", 1)
    rt = ring(to_left, "col", -1)
    q_ext = field(144, WIDE)
    strip2 = field(48, WIDE, dtype=BF16)
    x1, xb, c2, q1, q2, tab, down, up = call(
        first_kernel,
        (
            field(ROWS, WIDE), field(ROWS, WIDE), field(160, WIDE), q_ext, q_ext,
            field(24, 1024), strip2, strip2,
        ),
        [
            pltpu.VMEM((208, 768), F32), pltpu.VMEM((160, WIDE), F32),
            pltpu.VMEM((160, WIDE), F32), pltpu.VMEM((160, WIDE), F32),
            pltpu.VMEM((144, WIDE), F32), pltpu.VMEM((144, WIDE), F32),
        ] + work_scratch(),
        start_image, blur_dual, observed, tv_dual, idx, normed, top, bot, lf, rt,
        name="first",
    )
    top = ring(down, "row", 1)
    bot = ring(up, "row", -1)
    to_right, to_left = call(pack_cols2_kernel, (side, side), [], xb, top, bot, name="pack_cols2")
    lf = ring(to_right, "col", 1)
    rt = ring(to_left, "col", -1)
    return call(
        second_kernel,
        (field(ROWS, COLS), field(ROWS, COLS)),
        [
            pltpu.VMEM((208, 768), F32), pltpu.VMEM((160, WIDE), F32),
            pltpu.VMEM((144, WIDE), F32), pltpu.VMEM((144, WIDE), F32),
        ] + work_scratch(),
        x1, xb, c2, q1, q2, tab, top, bot, lf, rt, name="second",
    )


def solution(mesh):
    placed = (
        P("row", "col"),
        P(),
        P("row", "col"),
        P("row", "col"),
        P("row", "col"),
        P(None, "row", "col"),
    )
    return jax.shard_map(
        per_device,
        mesh=mesh,
        in_specs=placed,
        out_specs=(P("row", "col"), P("row", "col")),
        check_vma=False,
    )
```

```python
import jax
import jax.numpy as jnp
from jax import lax
from jax.experimental import pallas as pl
from jax.experimental.pallas import tpu as pltpu
from jax.sharding import PartitionSpec as P

SIGMA = 0.15
TAU = 0.6
TV = 0.5
F32 = jnp.float32
BF16 = jnp.bfloat16

ROWS = 128
COLS = 512
XO = 48
YO = 32
WIDE = 640
SEGS = ((0, 16, 32), (16, 128, 144), (144, 16, 32))
PATCHES = ((0,), (1, 2, 3, 4), (5, 6, 7, 8), (9, 10, 11, 12), (13, 14, 15, 16), (17,))


def iota(shape, dim):
    return lax.broadcasted_iota(jnp.int32, shape, dim)


def split(value):
    hi = value.astype(BF16).astype(F32)
    return hi, value - hi


def lanes(value, shift):
    shift = shift % value.shape[1]
    return pltpu.roll(value, shift, 1) if shift else value


def rows(value, shift):
    shift = shift % value.shape[0]
    return pltpu.roll(value, shift, 0) if shift else value


def between(shape, lo, hi):
    lane = iota(shape, 1)
    return (lane >= lo) & (lane < hi)


def flags():
    row = lax.axis_index("row")
    col = lax.axis_index("col")
    return (
        row > 0,
        row < lax.axis_size("row") - 1,
        col > 0,
        col < lax.axis_size("col") - 1,
    )


def pack_rows_kernel(x_ref, y_ref, o_ref, q_ref, idx_ref, down_ref, up_ref):
    for out, near, far, edge in ((down_ref, 112, 96, 127), (up_ref, 0, 0, 0)):
        out[0:32] = x_ref[far : far + 32].astype(BF16)
        seen = o_ref[near : near + 16]
        hi, lo = split(y_ref[near : near + 16] - SIGMA * seen)
        out[32:48] = hi.astype(BF16)
        out[48:64] = lo.astype(BF16)
        out[64:80] = seen.astype(BF16)
        a_hi, a_lo = split(q_ref[0, edge : edge + 1])
        b_hi, b_lo = split(q_ref[1, edge : edge + 1])
        x_lo = split(x_ref[edge : edge + 1])[1]
        row = iota((16, COLS), 0)
        misc = jnp.zeros((16, COLS), F32)
        for place, part in enumerate((x_lo, a_hi, a_lo, b_hi, b_lo, idx_ref[0:1])):
            misc = jnp.where(row == place, part, misc)
        out[80:96] = misc.astype(BF16)


def pack_cols_kernel(x_ref, y_ref, o_ref, q_ref, idx_ref, top_ref, bot_ref, right_ref, left_ref):
    for out, base, spots in (
        (right_ref, 384, (48, 64, 80, 96, (97, 98, 99, 100, 101))),
        (left_ref, 0, (48, 0, 16, 32, (96, 97, 98, 99, 100))),
    ):
        own = slice(base, base + 128)
        top = top_ref[:, own].astype(F32)
        bot = bot_ref[:, own].astype(F32)
        seen = o_ref[:, own]
        x = x_ref[:, own]
        c_hi, c_lo = split(y_ref[:, own] - SIGMA * seen)
        x_hi, x_lo = split(x)

        def rolled(middle, section, shift, size):
            first = lanes(top[section : section + size], shift)
            last = lanes(bot[section : section + size], shift)
            return jnp.concatenate([first, lanes(middle, shift), last], axis=0)

        shape = (192, 128)
        fill = jnp.zeros((32, 128), F32)
        buf = rolled(x_hi, 0, spots[0], 32)
        right = base > 0
        x_at = 16 if right else 48
        buf = jnp.where(between(shape, x_at, x_at + 32), buf, 0.0)
        at = 48 if right else 0
        for which, (middle, section) in enumerate(((c_hi, 32), (c_lo, 48), (seen, 64))):
            part = jnp.concatenate([rolled(middle, section, spots[1 + which], 16), fill], axis=0)
            start = at + 16 * which
            buf = jnp.where(between(shape, start, start + 16), part, buf)
        a_hi, a_lo = split(q_ref[0, :, own])
        b_hi, b_lo = split(q_ref[1, :, own])
        rix = iota((32, 128), 0)
        for which, middle in enumerate((x_lo, a_hi, a_lo, b_hi, b_lo)):
            shift = spots[4][which]
            first = jnp.where(rix == 31, top[80 + which : 81 + which], 0.0)
            last = jnp.where(rix == 0, bot[80 + which : 81 + which], 0.0)
            part = jnp.concatenate(
                [lanes(first, shift), lanes(middle, shift), lanes(last, shift)], axis=0
            )
            buf = jnp.where(between(shape, 96 + which, 97 + which), part, buf)
        spot = 4 if right else 1
        row = iota((192, 1), 0)
        mine = idx_ref[0:1, spot : spot + 1]
        above = top_ref[85:86, spot : spot + 1].astype(F32)
        below = bot_ref[85:86, spot : spot + 1].astype(F32)
        entry = jnp.where(row == 0, above, jnp.where(row == 1, mine, below))
        buf = jnp.where(between(shape, 101, 102), entry, buf)
        out[...] = buf.astype(BF16)


def pack_cols2_kernel(xb_ref, top_ref, bot_ref, right_ref, left_ref):
    for out, tile, at in ((right_ref, 4, 16), (left_ref, 0, 48)):
        own = slice(128 * tile, 128 * tile + 128)
        hi, lo = split(xb_ref[:, own])
        top = top_ref[:, own].astype(F32)
        bot = bot_ref[:, own].astype(F32)
        shape = (192, 128)
        buf = jnp.concatenate([top[0:32], hi, bot[0:32]], axis=0)
        rix = iota((32, 128), 0)
        low = jnp.concatenate(
            [
                jnp.where(rix == 31, top[32:33], 0.0),
                lo,
                jnp.where(rix == 0, bot[32:33], 0.0),
            ],
            axis=0,
        )
        source = 47 if tile == 4 else 48
        buf = jnp.where(between(shape, at, at + 32), buf, 0.0)
        buf = jnp.where(between(shape, 96, 97), lanes(low, 96 - source), buf)
        out[...] = buf.astype(BF16)


def build_taps(tab_ref, t_ref):
    k = iota((32, 128), 0)
    j = iota((32, 128), 1) % 32
    lower = j <= k
    for patch in range(18):
        at = 8 * (patch // 6) + patch % 6
        for a1 in range(4):
            for half in range(2):
                e = 2 * a1 + half
                line = tab_ref[at : at + 1, 128 * e : 128 * e + 128]
                spread = jnp.broadcast_to(line, (32, 128))
                low = pltpu.roll(spread, 97, 1, stride=1, stride_axis=0)
                high = pltpu.roll(low, 32, 1)
                block = jnp.concatenate(
                    [jnp.where(lower, low, 0.0), jnp.where(lower, 0.0, high)], axis=0
                )
                t_ref[patch, 64 * a1 : 64 * a1 + 64, 128 * half : 128 * half + 128] = block.astype(
                    BF16
                )


def windows(xe_ref, p_ref):
    low = between((192, 128), 0, 64)
    tail = between((192, 128), 96, 128)
    for tile in range(5):
        here = slice(128 * tile, 128 * tile + 128)
        x0 = xe_ref[0:192, here]
        x8 = xe_ref[8:200, here]
        p_ref[4 * tile] = jnp.where(low, x0, lanes(x8, 64)).astype(BF16)
        p_ref[4 * tile + 1] = jnp.where(low, lanes(x0, 96), lanes(x8, 32)).astype(BF16)
        if tile < 4:
            after = slice(128 * tile + 128, 128 * tile + 256)
            p_ref[4 * tile + 2] = jnp.where(low, lanes(x0, 64), x8).astype(BF16)
            w0 = jnp.where(tail, x0, xe_ref[0:192, after])
            w8 = jnp.where(tail, x8, xe_ref[8:200, after])
            p_ref[4 * tile + 3] = jnp.where(low, lanes(w0, 32), lanes(w8, 96)).astype(BF16)


def blur(p_ref, t_ref, a_ref, c_ref, y_ref, row_ok, col_ok):
    for seg, (first, size, padded) in enumerate(SEGS):
        for patch, blocks in enumerate(PATCHES):
            lhs = jnp.concatenate(
                [
                    jnp.concatenate(
                        [
                            p_ref[b, first : first + padded],
                            p_ref[b, first + 16 : first + 16 + padded],
                        ],
                        axis=1,
                    )
                    for b in blocks
                ],
                axis=0,
            )
            v = jnp.dot(lhs, t_ref[6 * seg + patch], preferred_element_type=F32)
            for place, b in enumerate(blocks):
                part = v[place * padded : place * padded + padded]
                a_ref[b, 0:padded] = part[:, :128] + rows(part[:, 128:], -4)
        low = between((padded, 128), 0, 64)
        even = iota((padded, 128), 1) % 64 < 32
        for tile in range(5):
            a = [a_ref[4 * tile + p, 0:padded] for p in range(2 if tile == 4 else 4)]
            if tile == 4:
                a += [jnp.zeros_like(a[0])] * 2
            e = []
            for p in range(2):
                z = lanes(jnp.where(low, a[p + 2], a[p]), 64)
                e.append(jnp.where(low, a[p], z) + rows(jnp.where(low, z, a[p + 2]), -2))
            m1 = jnp.where(even, e[0], lanes(e[1], 32))
            m2 = jnp.where(even, lanes(e[0], 96), e[1])
            blurred = (m1 + rows(m2, -1))[0:size]
            here = slice(128 * tile, 128 * tile + 128)
            new = (c_ref[first : first + size, here] + SIGMA * blurred) / (1.0 + SIGMA)
            keep = col_ok(tile, size) & row_ok(seg)
            y_ref[first : first + size, here] = jnp.where(keep, new, 0.0)


def adjoint(y_ref, t_ref, l_ref, f_ref, z_ref):
    z_ref[...] = jnp.zeros_like(z_ref)
    for seg, (first, size, padded) in enumerate(SEGS):
        low = between((padded, 128), 0, 64)
        even = iota((padded, 128), 1) % 64 < 32
        for tile in range(5):
            here = slice(128 * tile, 128 * tile + 128)
            o = jnp.concatenate(
                [y_ref[first : first + size, here], jnp.zeros((padded - size, 128), F32)], axis=0
            )
            o1 = rows(o, 1)
            e = [jnp.where(even, o, lanes(o1, 32)), jnp.where(even, lanes(o, 96), o1)]
            for p in range(2):
                s = rows(e[p], 2)
                parts = [(p, jnp.where(low, e[p], lanes(s, 64)))]
                if tile < 4:
                    parts.append((p + 2, jnp.where(low, lanes(e[p], 64), s)))
                for place, part in parts:
                    b = 4 * tile + place
                    l_ref[b, 0:padded, 0:128] = part.astype(BF16)
                    l_ref[b, 0:padded, 128:256] = rows(part, 4).astype(BF16)
        for patch, blocks in enumerate(PATCHES):
            lhs = jnp.concatenate([l_ref[b, 0:padded] for b in blocks], axis=0)
            g = lax.dot_general(
                lhs, t_ref[6 * seg + patch], (((1,), (1,)), ((), ())), preferred_element_type=F32
            )
            zero = jnp.zeros((16, 128), F32)
            for place, b in enumerate(blocks):
                part = g[place * padded : place * padded + padded]
                f_ref[b, 0 : padded + 16] = jnp.concatenate(
                    [part[:, :128], zero], axis=0
                ) + jnp.concatenate([zero, part[:, 128:]], axis=0)
        tall = padded + 24
        low = between((tall, 128), 0, 64)
        head = between((tall, 128), 0, 32)
        pad8 = jnp.zeros((8, 128), F32)
        for tile in range(5):
            both = []
            for p in range(2):
                fa = f_ref[4 * tile + p, 0 : padded + 16]
                a0 = jnp.concatenate([fa, pad8], axis=0)
                a8 = jnp.concatenate([pad8, fa], axis=0)
                if tile < 4:
                    fb = f_ref[4 * tile + p + 2, 0 : padded + 16]
                    b0 = jnp.concatenate([fb, pad8], axis=0)
                    b8 = jnp.concatenate([pad8, fb], axis=0)
                    both.append(jnp.where(low, a0, b8) + lanes(jnp.where(low, b0, a8), 64))
                else:
                    both.append(jnp.where(low, a0 + lanes(a8, 64), 0.0))
            turned = lanes(both[1], 32)
            here = slice(128 * tile, 128 * tile + 128)
            span = slice(first, first + tall)
            z_ref[span, here] += both[0] + jnp.where(head, 0.0, turned)
            if tile < 4:
                after = slice(128 * tile + 128, 128 * tile + 256)
                z_ref[span, after] += jnp.where(head, turned, 0.0)


def total_variation(xe_ref, q1_ref, q2_ref, q1o_ref, q2o_ref, place_row, place_col, limit_row, limit_col):
    for chunk in range(9):
        start = 16 * chunk
        x = xe_ref[24 + start : 40 + start, 0:WIDE]
        tall = xe_ref[24 + start : 48 + start, 0:WIDE]
        below = rows(tall, -1)[0:16]
        right = lanes(x, -1)
        r = place_row - 8 + start + iota((16, WIDE), 0)
        c = place_col - XO + iota((16, WIDE), 1)
        g1 = jnp.where(r < limit_row, below - x, 0.0)
        g2 = jnp.where(c < limit_col, right - x, 0.0)
        span = slice(start, start + 16)
        u1 = q1_ref[span] + SIGMA * g1
        u2 = q2_ref[span] + SIGMA * g2
        shrink = jnp.maximum(1.0, jnp.sqrt(u1 * u1 + u2 * u2) / TV)
        inv = 1.0 / shrink
        q1o_ref[span] = u1 * inv
        q2o_ref[span] = u2 * inv


def divergence(q1_ref, q2_ref, chunk, place_row, place_col, limit_row, limit_col):
    start = 8 + 16 * chunk
    m1 = q1_ref[start - 8 : start + 16]
    m2 = q2_ref[start : start + 16]
    r = place_row + 16 * chunk - 8 + iota((24, WIDE), 0)
    c = place_col - XO + iota((16, WIDE), 1)
    m1 = jnp.where((r >= 0) & (r < limit_row), m1, 0.0)
    m2 = jnp.where((c >= 0) & (c < limit_col), m2, 0.0)
    return (m1 - rows(m1, 1))[8:24] + (m2 - lanes(m2, 1))


def places():
    row = lax.axis_index("row")
    col = lax.axis_index("col")
    return (
        row * ROWS,
        col * COLS,
        lax.axis_size("row") * ROWS - 1,
        lax.axis_size("col") * COLS - 1,
    )


def masks():
    top, bot, left, right = flags()

    def row_ok(seg):
        if seg == 1:
            return jnp.bool_(True)
        return top if seg == 0 else bot

    def col_ok(tile, size):
        lane = iota((size, 128), 1)
        if tile == 0:
            return (lane >= YO) | left
        if tile == 4:
            return (lane < YO) | right
        return jnp.ones((size, 128), jnp.bool_)

    return row_ok, col_ok


def widen(value, shift):
    pad = jnp.zeros((value.shape[0], WIDE - COLS), F32)
    return lanes(jnp.concatenate([value, pad], axis=1), shift)


def select_tables(table_ref, idx_ref, top_ref, bot_ref, lf_ref, rt_ref, tab_ref):
    lane = iota((1, 128), 1)
    total = jnp.full((1, 128), -1.0, F32)
    lines = (top_ref[80:96, 0:128].astype(F32)[5:6], idx_ref[0:1, 0:128], bot_ref[80:96, 0:128].astype(F32)[5:6])
    lf = lf_ref[0:16].astype(F32)
    rt = rt_ref[0:16].astype(F32)
    for r in range(3):
        line = jnp.where(lane == 0, lf[r : r + 1, 101:102], lines[r])
        line = jnp.where(lane == 5, rt[r : r + 1, 101:102], line)
        line = lanes(line, 8 * r) if r else line
        total = jnp.where((lane >= 8 * r) & (lane < 8 * r + 6), line, total)
    onehot = jnp.where(total == iota((64, 128), 0).astype(F32), 1.0, 0.0).astype(BF16)
    picked = lax.dot_general(
        onehot, table_ref[...], (((0,), (0,)), ((), ())), preferred_element_type=F32
    )
    tab_ref[...] = picked[0:24]


def first_kernel(
    x_ref, y_ref, o_ref, q_ref, idx_ref, table_ref, top_ref, bot_ref, lf_ref, rt_ref,
    x1_ref, xb_ref, c2_ref, q1o_ref, q2o_ref, tab_ref, down_ref, up_ref,
    xe_ref, c_ref, ob_ref, ys_ref, q1_ref, q2_ref, t_ref, p_ref, a_ref, l_ref, f_ref, z_ref,
):
    top_ok, bot_ok, left_ok, right_ok = flags()
    row0, col0, limit_row, limit_col = places()
    select_tables(table_ref, idx_ref, top_ref, bot_ref, lf_ref, rt_ref, tab_ref)
    build_taps(tab_ref, t_ref)
    misc_t = top_ref[80:96].astype(F32)
    misc_b = bot_ref[80:96].astype(F32)
    rix = iota((32, COLS), 0)
    above = top_ref[0:32].astype(F32) + jnp.where(rix == 31, misc_t[0:1], 0.0)
    below = bot_ref[0:32].astype(F32) + jnp.where(rix == 0, misc_b[0:1], 0.0)
    own = widen(x_ref[...], XO)
    xe_ref[0:32, 0:WIDE] = widen(jnp.where(top_ok, above, 0.0), XO)
    xe_ref[32:160, 0:WIDE] = own
    xe_ref[160:192, 0:WIDE] = widen(jnp.where(bot_ok, below, 0.0), XO)
    xe_ref[192:208, :] = jnp.zeros((16, 768), F32)
    xe_ref[0:208, 640:768] = jnp.zeros((208, 128), F32)
    rr = iota((192, 128), 0)
    rows_ok = ((rr >= 32) | top_ok) & ((rr < 160) | bot_ok)
    lf = jnp.where(rows_ok & left_ok, lf_ref[...].astype(F32), 0.0)
    rt = jnp.where(rows_ok & right_ok, rt_ref[...].astype(F32), 0.0)
    shape = (192, 128)
    add = jnp.where(between(shape, 16, 48), lf, 0.0)
    xe_ref[0:192, 0:128] += add + jnp.where(between(shape, 47, 48), lanes(lf, 79), 0.0)
    add = jnp.where(between(shape, 48, 80), rt, 0.0)
    xe_ref[0:192, 512:640] += add + jnp.where(between(shape, 48, 49), lanes(rt, 80), 0.0)
    seen = o_ref[...]
    c_ref[16:144] = widen(y_ref[...] - SIGMA * seen, YO)
    ob_ref[16:144] = widen(seen, YO)
    for ref, span in ((top_ref, slice(0, 16)), (bot_ref, slice(144, 160))):
        c_ref[span] = widen(ref[32:48].astype(F32) + ref[48:64].astype(F32), YO)
        ob_ref[span] = widen(ref[64:80].astype(F32), YO)
    lf = lf_ref[0:160].astype(F32)
    rt = rt_ref[0:160].astype(F32)
    shape = (160, 128)
    at = between(shape, 16, 32)
    c_ref[:, 0:128] = jnp.where(at, lanes(lf, 96) + lanes(lf, 80), c_ref[:, 0:128])
    ob_ref[:, 0:128] = jnp.where(at, lanes(lf, 64), ob_ref[:, 0:128])
    at = between(shape, 32, 48)
    c_ref[:, 512:640] = jnp.where(at, lanes(rt, 32) + lanes(rt, 16), c_ref[:, 512:640])
    ob_ref[:, 512:640] = jnp.where(at, rt, ob_ref[:, 512:640])
    lf = lf_ref[24:168].astype(F32)
    edge = between((144, 128), 47, 48)
    r8 = iota((8, COLS), 0)
    for comp, ref in ((0, q1_ref), (1, q2_ref)):
        line = misc_t[1 + 2 * comp : 2 + 2 * comp] + misc_t[2 + 2 * comp : 3 + 2 * comp]
        ref[0:8] = widen(jnp.where(r8 == 7, line, 0.0), XO)
        ref[8:136] = widen(q_ref[comp], XO)
        ref[136:144] = jnp.zeros((8, WIDE), F32)
        side = lanes(lf, 78 - 2 * comp) + lanes(lf, 77 - 2 * comp)
        ref[:, 0:128] = jnp.where(edge, side, ref[:, 0:128])
    row_ok, col_ok = masks()
    windows(xe_ref, p_ref)
    blur(p_ref, t_ref, a_ref, c_ref, ys_ref, row_ok, col_ok)
    total_variation(xe_ref, q1_ref, q2_ref, q1o_ref, q2o_ref, row0, col0, limit_row, limit_col)
    adjoint(ys_ref, t_ref, l_ref, f_ref, z_ref)
    c2_ref[...] = ys_ref[...] - SIGMA * ob_ref[...]
    for chunk in range(8):
        span = slice(16 * chunk, 16 * chunk + 16)
        ext = slice(32 + 16 * chunk, 48 + 16 * chunk)
        div = divergence(q1o_ref, q2o_ref, chunk, row0, col0, limit_row, limit_col)
        x = xe_ref[ext, 0:WIDE]
        new = x - TAU * (z_ref[ext, 0:WIDE] - div)
        x1_ref[span] = new
        xb_ref[span] = 2.0 * new - x
    row = iota((16, WIDE), 0)
    down_ref[0:32] = xb_ref[96:128].astype(BF16)
    up_ref[0:32] = xb_ref[0:32].astype(BF16)
    down_ref[32:48] = jnp.where(row == 0, split(xb_ref[127:128])[1], 0.0).astype(BF16)
    up_ref[32:48] = jnp.where(row == 0, split(xb_ref[0:1])[1], 0.0).astype(BF16)


def second_kernel(
    x1_ref, xb_ref, c2_ref, q1i_ref, q2i_ref, tab_ref, top_ref, bot_ref, lf_ref, rt_ref,
    x2_ref, y2_ref,
    xe_ref, ys_ref, q1_ref, q2_ref, t_ref, p_ref, a_ref, l_ref, f_ref, z_ref,
):
    top_ok, bot_ok, left_ok, right_ok = flags()
    row0, col0, limit_row, limit_col = places()
    build_taps(tab_ref, t_ref)
    lane = iota((32, WIDE), 1)
    own_lane = (lane >= XO) & (lane < XO + COLS)
    rix = iota((32, WIDE), 0)
    above = top_ref[0:32].astype(F32) + jnp.where(rix == 31, top_ref[32:48].astype(F32)[0:1], 0.0)
    below = bot_ref[0:32].astype(F32) + jnp.where(rix == 0, bot_ref[32:48].astype(F32)[0:1], 0.0)
    xe_ref[0:32, 0:WIDE] = jnp.where(own_lane & top_ok, above, 0.0)
    for chunk in range(4):
        span = slice(32 * chunk, 32 * chunk + 32)
        xe_ref[32 + 32 * chunk : 64 + 32 * chunk, 0:WIDE] = jnp.where(own_lane, xb_ref[span], 0.0)
    xe_ref[160:192, 0:WIDE] = jnp.where(own_lane & bot_ok, below, 0.0)
    xe_ref[192:208, :] = jnp.zeros((16, 768), F32)
    xe_ref[0:208, 640:768] = jnp.zeros((208, 128), F32)
    rr = iota((192, 128), 0)
    rows_ok = ((rr >= 32) | top_ok) & ((rr < 160) | bot_ok)
    lf = jnp.where(rows_ok & left_ok, lf_ref[...].astype(F32), 0.0)
    rt = jnp.where(rows_ok & right_ok, rt_ref[...].astype(F32), 0.0)
    shape = (192, 128)
    add = jnp.where(between(shape, 16, 48), lf, 0.0)
    xe_ref[0:192, 0:128] += add + jnp.where(between(shape, 47, 48), lanes(lf, 79), 0.0)
    add = jnp.where(between(shape, 48, 80), rt, 0.0)
    xe_ref[0:192, 512:640] += add + jnp.where(between(shape, 48, 49), lanes(rt, 80), 0.0)
    row_ok, col_ok = masks()
    windows(xe_ref, p_ref)
    blur(p_ref, t_ref, a_ref, c2_ref, ys_ref, row_ok, col_ok)
    total_variation(xe_ref, q1i_ref, q2i_ref, q1_ref, q2_ref, row0, col0, limit_row, limit_col)
    adjoint(ys_ref, t_ref, l_ref, f_ref, z_ref)
    for chunk in range(8):
        span = slice(16 * chunk, 16 * chunk + 16)
        ext = slice(32 + 16 * chunk, 48 + 16 * chunk)
        div = divergence(q1_ref, q2_ref, chunk, row0, col0, limit_row, limit_col)
        new = x1_ref[span] - TAU * (z_ref[ext, 0:WIDE] - div)
        x2_ref[span] = lanes(new, -XO)[:, :COLS]
        y2_ref[span] = lanes(ys_ref[16 + 16 * chunk : 32 + 16 * chunk], -YO)[:, :COLS]


def work_scratch():
    return [
        pltpu.VMEM((18, 256, 256), BF16),
        pltpu.VMEM((18, 192, 128), BF16),
        pltpu.VMEM((18, 144, 128), F32),
        pltpu.VMEM((18, 144, 256), BF16),
        pltpu.VMEM((18, 160, 128), F32),
        pltpu.VMEM((208, WIDE), F32),
    ]


def field(*shape, dtype=F32):
    return jax.ShapeDtypeStruct(shape, dtype)


def call(kernel, outs, scratch, *args, name, room=4):
    return pl.pallas_call(
        kernel,
        out_shape=outs,
        scratch_shapes=scratch,
        compiler_params=pltpu.CompilerParams(vmem_limit_bytes=room * 1024 * 1024),
        name=name,
    )(*args)


def ring(block, axis, distance):
    count = lax.axis_size(axis)
    return lax.ppermute(block, axis, [(i, (i + distance) % count) for i in range(count)])


def per_device(observed, psf_table, psf_index, start_image, blur_dual, tv_dual):
    table = psf_table.astype(F32)
    normed = (table / jnp.sum(table, axis=(1, 2), keepdims=True)).astype(BF16)
    normed = jnp.pad(normed[:, :, ::-1], ((0, 0), (1, 0), (0, 1))).reshape(64, 1024)
    idx = jnp.pad(psf_index.astype(F32), ((0, 0), (1, COLS - 5)))
    strip = field(96, COLS, dtype=BF16)
    side = field(192, 128, dtype=BF16)
    down, up = call(
        pack_rows_kernel, (strip, strip), [], start_image, blur_dual, observed, tv_dual, idx,
        name="pack_rows",
    )
    top = ring(down, "row", 1)
    bot = ring(up, "row", -1)
    to_right, to_left = call(
        pack_cols_kernel, (side, side), [],
        start_image, blur_dual, observed, tv_dual, idx, top, bot, name="pack_cols",
    )
    lf = ring(to_right, "col", 1)
    rt = ring(to_left, "col", -1)
    q_ext = field(144, WIDE)
    strip2 = field(48, WIDE, dtype=BF16)
    x1, xb, c2, q1, q2, tab, down, up = call(
        first_kernel,
        (
            field(ROWS, WIDE), field(ROWS, WIDE), field(160, WIDE), q_ext, q_ext,
            field(24, 1024), strip2, strip2,
        ),
        [
            pltpu.VMEM((208, 768), F32), pltpu.VMEM((160, WIDE), F32),
            pltpu.VMEM((160, WIDE), F32), pltpu.VMEM((160, WIDE), F32),
            pltpu.VMEM((144, WIDE), F32), pltpu.VMEM((144, WIDE), F32),
        ] + work_scratch(),
        start_image, blur_dual, observed, tv_dual, idx, normed, top, bot, lf, rt,
        name="first", room=24,
    )
    top = ring(down, "row", 1)
    bot = ring(up, "row", -1)
    to_right, to_left = call(pack_cols2_kernel, (side, side), [], xb, top, bot, name="pack_cols2")
    lf = ring(to_right, "col", 1)
    rt = ring(to_left, "col", -1)
    return call(
        second_kernel,
        (field(ROWS, COLS), field(ROWS, COLS)),
        [
            pltpu.VMEM((208, 768), F32), pltpu.VMEM((160, WIDE), F32),
            pltpu.VMEM((144, WIDE), F32), pltpu.VMEM((144, WIDE), F32),
        ] + work_scratch(),
        x1, xb, c2, q1, q2, tab, top, bot, lf, rt, name="second", room=24,
    )


def solution(mesh):
    placed = (
        P("row", "col"),
        P(),
        P("row", "col"),
        P("row", "col"),
        P("row", "col"),
        P(None, "row", "col"),
    )
    return jax.shard_map(
        per_device,
        mesh=mesh,
        in_specs=placed,
        out_specs=(P("row", "col"), P("row", "col")),
        check_vma=False,
    )
```

```python
import jax
import jax.numpy as jnp
from jax import lax
from jax.experimental import pallas as pl
from jax.experimental.pallas import tpu as pltpu
from jax.sharding import PartitionSpec as P

SIGMA = 0.15
TAU = 0.6
TV = 0.5
F32 = jnp.float32
BF16 = jnp.bfloat16

ROWS = 128
COLS = 512
XO = 80
YO = 64
WIDE = 640
FULL = 768
SEGS1 = ((0, 48, 64), (48, 128, 144), (176, 48, 64))
SEGS2 = ((0, 16, 32), (16, 128, 144), (144, 16, 32))
PATCHES1 = ((0, 1), (2, 3, 4, 5), (6, 7, 8, 9), (10, 11, 12, 13), (14, 15, 16, 17), (18, 19))
PATCHES2 = ((1,), (2, 3, 4, 5), (6, 7, 8, 9), (10, 11, 12, 13), (14, 15, 16, 17), (18,))
SX, SXL, SC, SCL, SO, S1, S2, SM, STRIP = 0, 64, 80, 128, 144, 160, 192, 224, 240


def iota(shape, dim):
    return lax.broadcasted_iota(jnp.int32, shape, dim)


def split(value):
    hi = value.astype(BF16).astype(F32)
    return hi, value - hi


def lanes(value, shift):
    shift = shift % value.shape[1]
    return pltpu.roll(value, shift, 1) if shift else value


def rows(value, shift):
    shift = shift % value.shape[0]
    return pltpu.roll(value, shift, 0) if shift else value


def between(shape, lo, hi):
    lane = iota(shape, 1)
    return (lane >= lo) & (lane < hi)


def flags():
    row = lax.axis_index("row")
    col = lax.axis_index("col")
    return (
        row > 0,
        row < lax.axis_size("row") - 1,
        col > 0,
        col < lax.axis_size("col") - 1,
    )


def index_line(idx_ref, width):
    lane = iota((1, width), 1)
    line = jnp.zeros((1, width), F32)
    for j in range(4):
        line = jnp.where(lane == 1 + j, idx_ref[0:1, j : j + 1].astype(F32), line)
    return line


def pack_rows_kernel(x_hbm, y_hbm, o_hbm, q_hbm, idx_ref, down_ref, up_ref, x_ref, y_ref, o_ref, q_ref, sems):
    copies = [
        pltpu.make_async_copy(src, dst, sems.at[i])
        for i, (src, dst) in enumerate(((x_hbm, x_ref), (y_hbm, y_ref), (o_hbm, o_ref), (q_hbm, q_ref)))
    ]
    for copy in copies:
        copy.start()
    line = index_line(idx_ref, COLS)
    copies[0].wait()
    for out, x_at, low in ((down_ref, 64, 112), (up_ref, 0, 0)):
        out[SX : SX + 64] = x_ref[x_at : x_at + 64].astype(BF16)
        out[SXL : SXL + 16] = split(x_ref[low : low + 16])[1].astype(BF16)
    copies[1].wait()
    copies[2].wait()
    for out, c_at, low in ((down_ref, 80, 112), (up_ref, 0, 0)):
        out[SC : SC + 48] = (y_ref[c_at : c_at + 48] - SIGMA * o_ref[c_at : c_at + 48]).astype(BF16)
        c = y_ref[low : low + 16] - SIGMA * o_ref[low : low + 16]
        out[SCL : SCL + 16] = split(c)[1].astype(BF16)
        out[SO : SO + 16] = o_ref[low : low + 16].astype(BF16)
    copies[3].wait()
    row = iota((16, COLS), 0)
    for out, q_at, edge in ((down_ref, 96, 127), (up_ref, 0, 0)):
        out[S1 : S1 + 32] = q_ref[0, q_at : q_at + 32].astype(BF16)
        out[S2 : S2 + 32] = q_ref[1, q_at : q_at + 32].astype(BF16)
        misc = jnp.zeros((16, COLS), F32)
        for place in range(2):
            misc = jnp.where(row == place, split(q_ref[place, edge : edge + 1])[1], misc)
        misc = jnp.where(row == 2, line, misc)
        out[SM : SM + 16] = misc.astype(BF16)


def pack_cols_kernel(x_ref, y_ref, o_ref, q_ref, idx_ref, top_ref, bot_ref, right_ref, left_ref):
    for out, base in ((right_ref, 384), (left_ref, 0)):
        right = base > 0
        own = slice(base, base + 128)

        def strip(ref, at, count):
            return ref[at : at + count, own].astype(F32)

        def column(middle, at, count, shift):
            parts = [strip(top_ref, at, count), middle, strip(bot_ref, at, count)]
            return lanes(jnp.concatenate(parts, axis=0), shift)

        seen = o_ref[:, own]
        x_hi, x_lo = split(x_ref[:, own])
        c_hi, c_lo = split(y_ref[:, own] - SIGMA * seen)
        zeros = jnp.zeros((128, 128), F32)
        buf = column(x_hi, SX, 64, 80)
        part = jnp.concatenate([column(c_hi, SC, 48, 0 if right else 16), zeros[:32]], axis=0)
        at = 80 if right else 16
        buf = jnp.where(between((256, 128), at, at + 48), part, buf)
        part = jnp.concatenate([column(seen, SO, 16, 16 if right else 64), zeros[:96]], axis=0)
        at = 0 if right else 64
        buf = jnp.where(between((256, 128), at, at + 16), part, buf)
        out[0] = buf.astype(BF16)
        buf = jnp.concatenate([column(q_ref[0, :, own], S1, 32, 80), zeros[:64]], axis=0)
        part = jnp.concatenate(
            [column(q_ref[1, :, own], S2, 32, 112 if right else 0), zeros[:64]], axis=0
        )
        at = 80 if right else 0
        buf = jnp.where(between((256, 128), at, at + 32), part, buf)
        shift = 0 if right else 32
        part = jnp.concatenate(
            [
                zeros[:48],
                lanes(strip(top_ref, SXL, 16), shift),
                lanes(x_lo, shift),
                lanes(strip(bot_ref, SXL, 16), shift),
                zeros[:48],
            ],
            axis=0,
        )
        at = 112 if right else 32
        buf = jnp.where(between((256, 128), at, at + 16), part, buf)
        shift = 16 if right else 64
        part = jnp.concatenate(
            [
                zeros[:32],
                lanes(strip(top_ref, SCL, 16), shift),
                lanes(c_lo, shift),
                lanes(strip(bot_ref, SCL, 16), shift),
                zeros[:64],
            ],
            axis=0,
        )
        at = 0 if right else 64
        buf = jnp.where(between((256, 128), at, at + 16), part, buf)
        misc_t = strip(top_ref, SM, 16)
        misc_b = strip(bot_ref, SM, 16)
        if right:
            for comp in range(2):
                low = lanes(split(q_ref[comp, :, own])[1], 17 + comp)
                part = jnp.concatenate([zeros[:32], low, zeros[:96]], axis=0)
                buf = jnp.where(between((256, 128), 16 + comp, 17 + comp), part, buf)
        row = iota((256, 1), 0)
        spot = 4 if right else 1
        first = top_ref[SM : SM + 16, 0:128].astype(F32)[2:3, spot : spot + 1]
        last = bot_ref[SM : SM + 16, 0:128].astype(F32)[2:3, spot : spot + 1]
        mine = idx_ref[0:1, spot - 1 : spot].astype(F32)
        entry = jnp.where(row == 0, first, jnp.where(row == 1, mine, last))
        at = 18 if right else 112
        buf = jnp.where(between((256, 128), at, at + 1), entry, buf)
        out[1] = buf.astype(BF16)


def build_taps(tab_ref, t_ref):
    k = iota((32, 128), 0)
    j = iota((32, 128), 1) % 32
    lower = j <= k
    sub = iota((8, 128), 0)
    bits = [(sub // (1 << n)) % 2 == 1 for n in range(3)]
    for patch in range(18):
        at = 8 * (patch // 6) + patch % 6
        for e in range(8):
            skew = jnp.broadcast_to(tab_ref[at : at + 1, 128 * e : 128 * e + 128], (8, 128))
            for n in range(3):
                skew = jnp.where(bits[n], lanes(skew, 1 << n), skew)
            low = jnp.concatenate([lanes(skew, 8 * v - 31) for v in range(4)], axis=0)
            high = jnp.concatenate([lanes(skew, 8 * v + 1) for v in range(4)], axis=0)
            block = jnp.concatenate(
                [jnp.where(lower, low, 0.0), jnp.where(lower, 0.0, high)], axis=0
            )
            a1, half = e // 2, e % 2
            t_ref[patch, 64 * a1 : 64 * a1 + 64, 128 * half : 128 * half + 128] = block.astype(BF16)


def windows(xe_ref, p_ref, count):
    low = between((count, 128), 0, 64)
    tail = between((count, 128), 96, 128)
    for tile in range(5):
        here = slice(128 * tile, 128 * tile + 128)
        after = slice(128 * tile + 128, 128 * tile + 256)
        x0 = xe_ref[0:count, here]
        x8 = xe_ref[8 : count + 8, here]
        w0 = jnp.where(tail, x0, xe_ref[0:count, after])
        w8 = jnp.where(tail, x8, xe_ref[8 : count + 8, after])
        p_ref[4 * tile, 0:count] = jnp.where(low, x0, lanes(x8, 64)).astype(BF16)
        p_ref[4 * tile + 1, 0:count] = jnp.where(low, lanes(x0, 96), lanes(x8, 32)).astype(BF16)
        p_ref[4 * tile + 2, 0:count] = jnp.where(low, lanes(x0, 64), x8).astype(BF16)
        p_ref[4 * tile + 3, 0:count] = jnp.where(low, lanes(w0, 32), lanes(w8, 96)).astype(BF16)


def blur(segs, patches, p_ref, t_ref, a_ref, c_ref, y_ref, row_ok, col_ok):
    present = [b for blocks in patches for b in blocks]
    for seg, (first, size, padded) in enumerate(segs):
        for patch, blocks in enumerate(patches):
            lhs = jnp.concatenate(
                [
                    jnp.concatenate(
                        [
                            p_ref[b, first : first + padded],
                            p_ref[b, first + 16 : first + 16 + padded],
                        ],
                        axis=1,
                    )
                    for b in blocks
                ],
                axis=0,
            )
            v = jnp.dot(lhs, t_ref[6 * seg + patch], preferred_element_type=F32)
            for place, b in enumerate(blocks):
                part = v[place * padded : place * padded + padded]
                a_ref[b, 0:padded] = part[:, :128] + rows(part[:, 128:], -4)
        low = between((padded, 128), 0, 64)
        even = iota((padded, 128), 1) % 64 < 32
        for tile in range(5):
            a = [
                a_ref[4 * tile + p, 0:padded]
                if 4 * tile + p in present
                else jnp.zeros((padded, 128), F32)
                for p in range(4)
            ]
            e = []
            for p in range(2):
                z = lanes(jnp.where(low, a[p + 2], a[p]), 64)
                e.append(jnp.where(low, a[p], z) + rows(jnp.where(low, z, a[p + 2]), -2))
            m1 = jnp.where(even, e[0], lanes(e[1], 32))
            m2 = jnp.where(even, lanes(e[0], 96), e[1])
            blurred = (m1 + rows(m2, -1))[0:size]
            here = slice(128 * tile, 128 * tile + 128)
            new = (c_ref[first : first + size, here] + SIGMA * blurred) / (1.0 + SIGMA)
            keep = col_ok(tile, size) & row_ok(seg)
            y_ref[first : first + size, here] = jnp.where(keep, new, 0.0)


def adjoint(segs, patches, y_ref, t_ref, l_ref, f_ref, z_ref):
    present = [b for blocks in patches for b in blocks]
    z_ref[...] = jnp.zeros_like(z_ref)
    for seg, (first, size, padded) in enumerate(segs):
        low = between((padded, 128), 0, 64)
        even = iota((padded, 128), 1) % 64 < 32
        for tile in range(5):
            here = slice(128 * tile, 128 * tile + 128)
            o = jnp.concatenate(
                [y_ref[first : first + size, here], jnp.zeros((padded - size, 128), F32)], axis=0
            )
            o1 = rows(o, 1)
            e = [jnp.where(even, o, lanes(o1, 32)), jnp.where(even, lanes(o, 96), o1)]
            for p in range(2):
                s = rows(e[p], 2)
                for place in (p, p + 2):
                    b = 4 * tile + place
                    if b not in present:
                        continue
                    if place < 2:
                        part = jnp.where(low, e[p], lanes(s, 64))
                    else:
                        part = jnp.where(low, lanes(e[p], 64), s)
                    l_ref[b, 0:padded, 0:128] = part.astype(BF16)
                    l_ref[b, 0:padded, 128:256] = rows(part, 4).astype(BF16)
        for patch, blocks in enumerate(patches):
            lhs = jnp.concatenate([l_ref[b, 0:padded] for b in blocks], axis=0)
            g = lax.dot_general(
                lhs, t_ref[6 * seg + patch], (((1,), (1,)), ((), ())), preferred_element_type=F32
            )
            zero = jnp.zeros((16, 128), F32)
            for place, b in enumerate(blocks):
                part = g[place * padded : place * padded + padded]
                f_ref[b, 0 : padded + 16] = jnp.concatenate(
                    [part[:, :128], zero], axis=0
                ) + jnp.concatenate([zero, part[:, 128:]], axis=0)
        tall = padded + 24
        low = between((tall, 128), 0, 64)
        head = between((tall, 128), 0, 32)
        pad8 = jnp.zeros((8, 128), F32)

        def both_ways(b):
            if b not in present:
                zero = jnp.zeros((tall, 128), F32)
                return zero, zero
            f = f_ref[b, 0 : padded + 16]
            return jnp.concatenate([f, pad8], axis=0), jnp.concatenate([pad8, f], axis=0)

        for tile in range(5):
            both = []
            for p in range(2):
                a0, a8 = both_ways(4 * tile + p)
                b0, b8 = both_ways(4 * tile + p + 2)
                both.append(jnp.where(low, a0, b8) + lanes(jnp.where(low, b0, a8), 64))
            turned = lanes(both[1], 32)
            here = slice(128 * tile, 128 * tile + 128)
            after = slice(128 * tile + 128, 128 * tile + 256)
            span = slice(first, first + tall)
            z_ref[span, here] += both[0] + jnp.where(head, 0.0, turned)
            z_ref[span, after] += jnp.where(head, turned, 0.0)


def total_variation(x_ref, x_first, q1i_ref, q2i_ref, q1_ref, q2_ref, chunks, place):
    row0, col0, limit_row, limit_col = place
    for chunk in chunks:
        start = 16 * chunk
        tall = x_ref[x_first + start : x_first + start + 24, 0:WIDE]
        x = tall[0:16]
        below = rows(tall, -1)[0:16]
        right = lanes(x, -1)
        r = row0 - 32 + start + iota((16, WIDE), 0)
        c = col0 - XO + iota((16, WIDE), 1)
        g1 = jnp.where(r < limit_row, below - x, 0.0)
        g2 = jnp.where(c < limit_col, right - x, 0.0)
        span = slice(start, start + 16)
        u1 = q1i_ref[span] + SIGMA * g1
        u2 = q2i_ref[span] + SIGMA * g2
        shrink = jnp.maximum(1.0, jnp.sqrt(u1 * u1 + u2 * u2) / TV)
        inv = 1.0 / shrink
        q1_ref[span] = u1 * inv
        q2_ref[span] = u2 * inv


def divergence(q1_ref, q2_ref, start, place):
    row0, col0, limit_row, limit_col = place
    above = max(start - 8, 0)
    m1 = q1_ref[above : start + 16]
    m2 = q2_ref[start : start + 16]
    r = row0 - 32 + above + iota(m1.shape, 0)
    c = col0 - XO + iota((16, WIDE), 1)
    m1 = jnp.where((r >= 0) & (r < limit_row), m1, 0.0)
    m2 = jnp.where((c >= 0) & (c < limit_col), m2, 0.0)
    return (m1 - rows(m1, 1))[start - above :] + (m2 - lanes(m2, 1))


def places():
    row = lax.axis_index("row")
    col = lax.axis_index("col")
    return (
        row * ROWS,
        col * COLS,
        lax.axis_size("row") * ROWS - 1,
        lax.axis_size("col") * COLS - 1,
    )


def masks():
    top, bot, left, right = flags()

    def row_ok(seg):
        if seg == 1:
            return jnp.bool_(True)
        return top if seg == 0 else bot

    def col_ok(tile, size):
        lane = iota((size, 128), 1)
        if tile == 0:
            return (lane >= YO) | left
        if tile == 4:
            return (lane < YO) | right
        return jnp.ones((size, 128), jnp.bool_)

    return row_ok, col_ok


def widen(value, shift, width=WIDE):
    pad = jnp.zeros((value.shape[0], width - COLS), F32)
    return lanes(jnp.concatenate([value, pad], axis=1), shift)


def select_tables(table_ref, idx_ref, top_ref, bot_ref, lf_ref, rt_ref, tab_ref):
    lane = iota((1, 128), 1)
    total = jnp.full((1, 128), -1.0, F32)
    lines = (
        top_ref[SM : SM + 16, 0:128].astype(F32)[2:3],
        index_line(idx_ref, 128),
        bot_ref[SM : SM + 16, 0:128].astype(F32)[2:3],
    )
    lf = lf_ref[1, 0:16].astype(F32)
    rt = rt_ref[1, 0:16].astype(F32)
    for r in range(3):
        line = jnp.where(lane == 0, lf[r : r + 1, 18:19], lines[r])
        line = jnp.where(lane == 5, rt[r : r + 1, 112:113], line)
        line = lanes(line, 8 * r)
        total = jnp.where((lane >= 8 * r) & (lane < 8 * r + 6), line, total)
    onehot = jnp.where(total == iota((64, 128), 0).astype(F32), 1.0, 0.0).astype(BF16)
    picked = lax.dot_general(
        onehot, table_ref[...], (((0,), (0,)), ((), ())), preferred_element_type=F32
    )
    tab_ref[...] = picked[0:24]


def main_kernel(
    x_ref, y_ref, o_ref, q_ref, idx_ref, table_ref, top_ref, bot_ref, lf_ref, rt_ref,
    x2_ref, y2_ref,
    xe_ref, c_ref, ob_ref, ys_ref, q1_ref, q2_ref, tab_ref, t_ref, p_ref, a_ref, l_ref, f_ref,
    z_ref, xb_ref, x1_ref,
):
    top_ok, bot_ok, left_ok, right_ok = flags()
    place = places()
    select_tables(table_ref, idx_ref, top_ref, bot_ref, lf_ref, rt_ref, tab_ref)
    build_taps(tab_ref, t_ref)

    def f32(ref, at, count):
        return ref[at : at + count].astype(F32)

    zero = jnp.zeros((48, COLS), F32)
    above = f32(top_ref, SX, 64) + jnp.concatenate([zero, f32(top_ref, SXL, 16)], axis=0)
    below = f32(bot_ref, SX, 64) + jnp.concatenate([f32(bot_ref, SXL, 16), zero], axis=0)
    xe_ref[0:64] = widen(jnp.where(top_ok, above, 0.0), XO, FULL)
    xe_ref[64:192] = widen(x_ref[...], XO, FULL)
    xe_ref[192:256] = widen(jnp.where(bot_ok, below, 0.0), XO, FULL)
    xe_ref[256:272] = jnp.zeros((16, FULL), F32)
    rr = iota((256, 128), 0)
    rows_ok = ((rr >= 64) | top_ok) & ((rr < 192) | bot_ok)
    lf0 = lf_ref[0].astype(F32)
    lf1 = lf_ref[1].astype(F32)
    rt0 = rt_ref[0].astype(F32)
    rt1 = rt_ref[1].astype(F32)
    shape = (256, 128)
    side = jnp.where(between(shape, 16, 80), lf0, 0.0)
    side += jnp.where(between(shape, 64, 80), lanes(lf1, 80), 0.0)
    xe_ref[0:256, 0:128] += jnp.where(rows_ok & left_ok, side, 0.0)
    side = jnp.where(between(shape, 80, 128), rt0, 0.0)
    side += jnp.where(between(shape, 80, 96), lanes(rt1, 48), 0.0)
    xe_ref[0:256, 512:640] += jnp.where(rows_ok & right_ok, side, 0.0)
    side = jnp.where(between(shape, 0, 16), rt0, 0.0)
    xe_ref[0:256, 640:768] += jnp.where(rows_ok & right_ok, side, 0.0)
    seen = o_ref[...]
    c_ref[48:176] = widen(y_ref[...] - SIGMA * seen, YO)
    ob_ref[16:144] = widen(seen, YO)
    zero = jnp.zeros((32, COLS), F32)
    above = f32(top_ref, SC, 48) + jnp.concatenate([zero, f32(top_ref, SCL, 16)], axis=0)
    below = f32(bot_ref, SC, 48) + jnp.concatenate([f32(bot_ref, SCL, 16), zero], axis=0)
    c_ref[0:48] = widen(above, YO)
    c_ref[176:224] = widen(below, YO)
    ob_ref[0:16] = widen(f32(top_ref, SO, 16), YO)
    ob_ref[144:160] = widen(f32(bot_ref, SO, 16), YO)
    shape = (224, 128)
    side = lanes(lf0[0:224], 64) + jnp.where(between(shape, 48, 64), lanes(lf1[0:224], 48), 0.0)
    c_ref[:, 0:128] = jnp.where(between(shape, 16, 64), side, c_ref[:, 0:128])
    side = lanes(rt0[0:224], 48) + jnp.where(between(shape, 64, 80), rt1[0:224], 0.0)
    c_ref[:, 512:640] = jnp.where(between(shape, 64, 112), side, c_ref[:, 512:640])
    shape = (160, 128)
    at = between(shape, 48, 64)
    ob_ref[:, 0:128] = jnp.where(at, lanes(lf0[0:160], 48), ob_ref[:, 0:128])
    ob_ref[:, 512:640] = jnp.where(between(shape, 64, 80), rt0[0:160], ob_ref[:, 512:640])
    rix = iota((32, COLS), 0)
    misc = f32(top_ref, SM, 16)
    shape = (192, 128)
    for comp, (ref, section) in enumerate(((q1_ref, S1), (q2_ref, S2))):
        above = f32(top_ref, section, 32) + jnp.where(rix == 31, misc[comp : comp + 1], 0.0)
        ref[0:32] = widen(above, XO)
        ref[32:160] = widen(q_ref[comp], XO)
        ref[160:192] = widen(f32(bot_ref, section, 32), XO)
        side = lanes(lf1[0:192], 96 * comp)
        side += jnp.where(between(shape, 79, 80), lanes(lf1[0:192], 63 - comp), 0.0)
        ref[:, 0:128] = jnp.where(between(shape, 48, 80), side, ref[:, 0:128])
        side = lanes(rt1[0:192], 80 * comp)
        ref[:, 512:640] = jnp.where(between(shape, 80, 112), side, ref[:, 512:640])
    row_ok, col_ok = masks()
    windows(xe_ref, p_ref, 256)
    blur(SEGS1, PATCHES1, p_ref, t_ref, a_ref, c_ref, ys_ref, row_ok, col_ok)
    total_variation(xe_ref, 32, q1_ref, q2_ref, q1_ref, q2_ref, range(12), place)
    adjoint(SEGS1, PATCHES1, ys_ref, t_ref, l_ref, f_ref, z_ref)
    lane = iota((16, WIDE), 1)
    inside = ((lane >= XO) | left_ok) & ((lane < XO + COLS) | right_ok)
    for chunk in range(12):
        start = 16 * chunk
        ext = slice(32 + start, 48 + start)
        x = xe_ref[ext, 0:WIDE]
        new = x - TAU * (z_ref[ext, 0:WIDE] - divergence(q1_ref, q2_ref, start, place))
        keep = inside & (top_ok if chunk < 2 else bot_ok) if chunk < 2 or chunk >= 10 else inside
        xb_ref[start : start + 16, 0:WIDE] = jnp.where(keep, 2.0 * new - x, 0.0)
        if 2 <= chunk < 10:
            x1_ref[start - 32 : start - 16] = new
    xb_ref[192:208, 0:WIDE] = jnp.zeros((16, WIDE), F32)
    xb_ref[:, WIDE:FULL] = jnp.zeros((208, FULL - WIDE), F32)
    c_ref[0:160] = ys_ref[32:192] - SIGMA * ob_ref[...]
    windows(xb_ref, p_ref, 192)
    blur(SEGS2, PATCHES2, p_ref, t_ref, a_ref, c_ref, ys_ref, row_ok, col_ok)
    total_variation(xb_ref, 0, q1_ref, q2_ref, q1_ref, q2_ref, range(1, 10), place)
    adjoint(SEGS2, PATCHES2, ys_ref, t_ref, l_ref, f_ref, z_ref)
    for chunk in range(8):
        span = slice(16 * chunk, 16 * chunk + 16)
        ext = slice(32 + 16 * chunk, 48 + 16 * chunk)
        div = divergence(q1_ref, q2_ref, 32 + 16 * chunk, place)
        new = x1_ref[span] - TAU * (z_ref[ext, 0:WIDE] - div)
        x2_ref[span] = lanes(new, -XO)[:, :COLS]
        y2_ref[span] = lanes(ys_ref[16 + 16 * chunk : 32 + 16 * chunk], -YO)[:, :COLS]


def field(*shape, dtype=F32):
    return jax.ShapeDtypeStruct(shape, dtype)


def call(kernel, outs, scratch, *args, name, room=4, far=0):
    spaces = [pltpu.HBM] * far + [pltpu.VMEM] * (len(args) - far)
    return pl.pallas_call(
        kernel,
        out_shape=outs,
        in_specs=[pl.BlockSpec(memory_space=space) for space in spaces],
        scratch_shapes=scratch,
        compiler_params=pltpu.CompilerParams(vmem_limit_bytes=room * 1024 * 1024),
        name=name,
    )(*args)


def ring(block, axis, distance):
    count = lax.axis_size(axis)
    return lax.ppermute(block, axis, [(i, (i + distance) % count) for i in range(count)])


def per_device(observed, psf_table, psf_index, start_image, blur_dual, tv_dual):
    own = (start_image, blur_dual, observed, tv_dual)
    block = pltpu.VMEM((ROWS, COLS), F32)
    strip = field(STRIP, COLS, dtype=BF16)
    side = field(2, 256, 128, dtype=BF16)
    down, up = call(
        pack_rows_kernel, (strip, strip),
        [block, block, block, pltpu.VMEM((2, ROWS, COLS), F32), pltpu.SemaphoreType.DMA((4,))],
        *own, psf_index, name="pack_rows", far=4, room=60,
    )
    top = ring(down, "row", 1)
    bot = ring(up, "row", -1)
    table = psf_table.astype(F32)
    normed = (table / jnp.sum(table, axis=(1, 2), keepdims=True)).astype(BF16)
    normed = jnp.pad(normed[:, :, ::-1], ((0, 0), (1, 0), (0, 1))).reshape(64, 1024)
    to_right, to_left = call(
        pack_cols_kernel, (side, side), [], *own, psf_index, top, bot, name="pack_cols"
    )
    lf = ring(to_right, "col", 1)
    rt = ring(to_left, "col", -1)
    wide = pltpu.VMEM((192, WIDE), F32)
    return call(
        main_kernel,
        (field(ROWS, COLS), field(ROWS, COLS)),
        [
            pltpu.VMEM((272, FULL), F32), pltpu.VMEM((224, WIDE), F32),
            pltpu.VMEM((160, WIDE), F32), pltpu.VMEM((224, WIDE), F32),
            wide, wide, pltpu.VMEM((24, 1024), F32),
            pltpu.VMEM((18, 256, 256), BF16), pltpu.VMEM((20, 256, 128), BF16),
            pltpu.VMEM((20, 144, 128), F32), pltpu.VMEM((20, 144, 256), BF16),
            pltpu.VMEM((20, 160, 128), F32), pltpu.VMEM((272, FULL), F32),
            pltpu.VMEM((208, FULL), F32), pltpu.VMEM((ROWS, WIDE), F32),
        ],
        *own, psf_index, normed, top, bot, lf, rt, name="main", room=28,
    )


def solution(mesh):
    placed = (
        P("row", "col"),
        P(),
        P("row", "col"),
        P("row", "col"),
        P("row", "col"),
        P(None, "row", "col"),
    )
    return jax.shard_map(
        per_device,
        mesh=mesh,
        in_specs=placed,
        out_specs=(P("row", "col"), P("row", "col")),
        check_vma=False,
    )
```

```python
import jax
import jax.numpy as jnp
from jax import lax
from jax.experimental import pallas as pl
from jax.experimental.pallas import tpu as pltpu
from jax.sharding import PartitionSpec as P

SIGMA = 0.15
TAU = 0.6
TV = 0.5
F32 = jnp.float32
BF16 = jnp.bfloat16

ROWS = 128
COLS = 512
XO = 80
YO = 64
WIDE = 640
FULL = 768
SEGS1 = ((0, 48, 64), (48, 128, 144), (176, 48, 64))
SEGS2 = ((0, 16, 32), (16, 128, 144), (144, 16, 32))
PATCHES1 = ((0, 1), (2, 3, 4, 5), (6, 7, 8, 9), (10, 11, 12, 13), (14, 15, 16, 17), (18, 19))
PATCHES2 = ((1,), (2, 3, 4, 5), (6, 7, 8, 9), (10, 11, 12, 13), (14, 15, 16, 17), (18,))
SX, SXL, SC, SCL, SO, S1, S2, SM, STRIP = 0, 64, 80, 128, 144, 160, 192, 224, 240


def iota(shape, dim):
    return lax.broadcasted_iota(jnp.int32, shape, dim)


def split(value):
    hi = value.astype(BF16).astype(F32)
    return hi, value - hi


def lanes(value, shift):
    shift = shift % value.shape[1]
    return pltpu.roll(value, shift, 1) if shift else value


def rows(value, shift):
    shift = shift % value.shape[0]
    return pltpu.roll(value, shift, 0) if shift else value


def between(shape, lo, hi):
    lane = iota(shape, 1)
    return (lane >= lo) & (lane < hi)


def flags():
    row = lax.axis_index("row")
    col = lax.axis_index("col")
    return (
        row > 0,
        row < lax.axis_size("row") - 1,
        col > 0,
        col < lax.axis_size("col") - 1,
    )


def index_line(idx_ref, width):
    lane = iota((1, width), 1)
    line = jnp.zeros((1, width), F32)
    for j in range(4):
        line = jnp.where(lane == 1 + j, idx_ref[0:1, j : j + 1].astype(F32), line)
    return line


def pack_rows_kernel(x_hbm, y_hbm, o_hbm, q_hbm, idx_ref, down_ref, up_ref, x_ref, y_ref, o_ref, q_ref, sems):
    copies = [
        pltpu.make_async_copy(src, dst, sems.at[i])
        for i, (src, dst) in enumerate(((x_hbm, x_ref), (y_hbm, y_ref), (o_hbm, o_ref), (q_hbm, q_ref)))
    ]
    for copy in copies:
        copy.start()
    line = index_line(idx_ref, COLS)
    copies[0].wait()
    for out, x_at, low in ((down_ref, 64, 112), (up_ref, 0, 0)):
        out[SX : SX + 64] = x_ref[x_at : x_at + 64].astype(BF16)
        out[SXL : SXL + 16] = split(x_ref[low : low + 16])[1].astype(BF16)
    copies[1].wait()
    copies[2].wait()
    for out, c_at, low in ((down_ref, 80, 112), (up_ref, 0, 0)):
        out[SC : SC + 48] = (y_ref[c_at : c_at + 48] - SIGMA * o_ref[c_at : c_at + 48]).astype(BF16)
        c = y_ref[low : low + 16] - SIGMA * o_ref[low : low + 16]
        out[SCL : SCL + 16] = split(c)[1].astype(BF16)
        out[SO : SO + 16] = o_ref[low : low + 16].astype(BF16)
    copies[3].wait()
    row = iota((16, COLS), 0)
    for out, q_at, edge in ((down_ref, 96, 127), (up_ref, 0, 0)):
        out[S1 : S1 + 32] = q_ref[0, q_at : q_at + 32].astype(BF16)
        out[S2 : S2 + 32] = q_ref[1, q_at : q_at + 32].astype(BF16)
        misc = jnp.zeros((16, COLS), F32)
        for place in range(2):
            misc = jnp.where(row == place, split(q_ref[place, edge : edge + 1])[1], misc)
        misc = jnp.where(row == 2, line, misc)
        out[SM : SM + 16] = misc.astype(BF16)


def pack_cols_kernel(x_ref, y_ref, o_ref, q_ref, idx_ref, top_ref, bot_ref, right_ref, left_ref):
    for out, base in ((right_ref, 384), (left_ref, 0)):
        right = base > 0
        own = slice(base, base + 128)

        def strip(ref, at, count):
            return ref[at : at + count, own].astype(F32)

        def column(middle, at, count, shift):
            parts = [strip(top_ref, at, count), middle, strip(bot_ref, at, count)]
            return lanes(jnp.concatenate(parts, axis=0), shift)

        seen = o_ref[:, own]
        x_hi, x_lo = split(x_ref[:, own])
        c_hi, c_lo = split(y_ref[:, own] - SIGMA * seen)
        zeros = jnp.zeros((128, 128), F32)
        buf = column(x_hi, SX, 64, 80)
        part = jnp.concatenate([column(c_hi, SC, 48, 0 if right else 16), zeros[:32]], axis=0)
        at = 80 if right else 16
        buf = jnp.where(between((256, 128), at, at + 48), part, buf)
        part = jnp.concatenate([column(seen, SO, 16, 16 if right else 64), zeros[:96]], axis=0)
        at = 0 if right else 64
        buf = jnp.where(between((256, 128), at, at + 16), part, buf)
        out[0] = buf.astype(BF16)
        buf = jnp.concatenate([column(q_ref[0, :, own], S1, 32, 80), zeros[:64]], axis=0)
        part = jnp.concatenate(
            [column(q_ref[1, :, own], S2, 32, 112 if right else 0), zeros[:64]], axis=0
        )
        at = 80 if right else 0
        buf = jnp.where(between((256, 128), at, at + 32), part, buf)
        shift = 0 if right else 32
        part = jnp.concatenate(
            [
                zeros[:48],
                lanes(strip(top_ref, SXL, 16), shift),
                lanes(x_lo, shift),
                lanes(strip(bot_ref, SXL, 16), shift),
                zeros[:48],
            ],
            axis=0,
        )
        at = 112 if right else 32
        buf = jnp.where(between((256, 128), at, at + 16), part, buf)
        shift = 16 if right else 64
        part = jnp.concatenate(
            [
                zeros[:32],
                lanes(strip(top_ref, SCL, 16), shift),
                lanes(c_lo, shift),
                lanes(strip(bot_ref, SCL, 16), shift),
                zeros[:64],
            ],
            axis=0,
        )
        at = 0 if right else 64
        buf = jnp.where(between((256, 128), at, at + 16), part, buf)
        misc_t = strip(top_ref, SM, 16)
        misc_b = strip(bot_ref, SM, 16)
        if right:
            for comp in range(2):
                low = lanes(split(q_ref[comp, :, own])[1], 17 + comp)
                part = jnp.concatenate([zeros[:32], low, zeros[:96]], axis=0)
                buf = jnp.where(between((256, 128), 16 + comp, 17 + comp), part, buf)
        row = iota((256, 1), 0)
        spot = 4 if right else 1
        first = top_ref[SM : SM + 16, 0:128].astype(F32)[2:3, spot : spot + 1]
        last = bot_ref[SM : SM + 16, 0:128].astype(F32)[2:3, spot : spot + 1]
        mine = idx_ref[0:1, spot - 1 : spot].astype(F32)
        entry = jnp.where(row == 0, first, jnp.where(row == 1, mine, last))
        at = 18 if right else 112
        buf = jnp.where(between((256, 128), at, at + 1), entry, buf)
        out[1] = buf.astype(BF16)


def build_taps(tab_ref, t_ref):
    sub = iota((144, 128), 0)
    bits = [(sub // (1 << n)) % 2 == 1 for n in range(3)]
    for e in range(8):
        a1, half = e // 2, e % 2
        here = slice(128 * half, 128 * half + 128)
        skew = jnp.concatenate(
            [
                jnp.broadcast_to(
                    tab_ref[8 * r + p : 8 * r + p + 1, 128 * e : 128 * e + 128], (8, 128)
                )
                for r in range(3)
                for p in range(6)
            ],
            axis=0,
        )
        for n in range(3):
            skew = jnp.where(bits[n], lanes(skew, 1 << n), skew)
        lower_all = [iota((144, 128), 1) % 32 <= sub % 8 + 8 * v for v in range(4)]
        low = [jnp.where(lower_all[v], lanes(skew, 8 * v - 31), 0.0) for v in range(4)]
        high = [jnp.where(lower_all[v], 0.0, lanes(skew, 8 * v + 1)) for v in range(4)]
        for patch in range(18):
            own = slice(8 * patch, 8 * patch + 8)
            block = jnp.concatenate([part[own] for part in low + high], axis=0)
            t_ref[patch, 64 * a1 : 64 * a1 + 64, here] = block.astype(BF16)


def windows(xe_ref, p_ref, count):
    low = between((count, 128), 0, 64)
    tail = between((count, 128), 96, 128)
    for tile in range(5):
        here = slice(128 * tile, 128 * tile + 128)
        after = slice(128 * tile + 128, 128 * tile + 256)
        x0 = xe_ref[0:count, here]
        x8 = xe_ref[8 : count + 8, here]
        w0 = jnp.where(tail, x0, xe_ref[0:count, after])
        w8 = jnp.where(tail, x8, xe_ref[8 : count + 8, after])
        p_ref[4 * tile, 0:count] = jnp.where(low, x0, lanes(x8, 64)).astype(BF16)
        p_ref[4 * tile + 1, 0:count] = jnp.where(low, lanes(x0, 96), lanes(x8, 32)).astype(BF16)
        p_ref[4 * tile + 2, 0:count] = jnp.where(low, lanes(x0, 64), x8).astype(BF16)
        p_ref[4 * tile + 3, 0:count] = jnp.where(low, lanes(w0, 32), lanes(w8, 96)).astype(BF16)


def blur(segs, patches, p_ref, t_ref, a_ref, c_ref, y_ref, row_ok, col_ok):
    present = [b for blocks in patches for b in blocks]
    for seg, (first, size, padded) in enumerate(segs):
        for patch, blocks in enumerate(patches):
            lhs = jnp.concatenate(
                [
                    jnp.concatenate(
                        [
                            p_ref[b, first : first + padded],
                            p_ref[b, first + 16 : first + 16 + padded],
                        ],
                        axis=1,
                    )
                    for b in blocks
                ],
                axis=0,
            )
            v = jnp.dot(lhs, t_ref[6 * seg + patch], preferred_element_type=F32)
            for place, b in enumerate(blocks):
                part = v[place * padded : place * padded + padded]
                a_ref[b, 0:padded] = part[:, :128] + rows(part[:, 128:], -4)
        low = between((padded, 128), 0, 64)
        even = iota((padded, 128), 1) % 64 < 32
        for tile in range(5):
            a = [
                a_ref[4 * tile + p, 0:padded]
                if 4 * tile + p in present
                else jnp.zeros((padded, 128), F32)
                for p in range(4)
            ]
            e = []
            for p in range(2):
                z = lanes(jnp.where(low, a[p + 2], a[p]), 64)
                e.append(jnp.where(low, a[p], z) + rows(jnp.where(low, z, a[p + 2]), -2))
            m1 = jnp.where(even, e[0], lanes(e[1], 32))
            m2 = jnp.where(even, lanes(e[0], 96), e[1])
            blurred = (m1 + rows(m2, -1))[0:size]
            here = slice(128 * tile, 128 * tile + 128)
            new = (c_ref[first : first + size, here] + SIGMA * blurred) / (1.0 + SIGMA)
            keep = col_ok(tile, size) & row_ok(seg)
            y_ref[first : first + size, here] = jnp.where(keep, new, 0.0)


def adjoint(segs, patches, y_ref, t_ref, l_ref, f_ref, z_ref):
    present = [b for blocks in patches for b in blocks]
    z_ref[...] = jnp.zeros_like(z_ref)
    for seg, (first, size, padded) in enumerate(segs):
        low = between((padded, 128), 0, 64)
        even = iota((padded, 128), 1) % 64 < 32
        for tile in range(5):
            here = slice(128 * tile, 128 * tile + 128)
            o = jnp.concatenate(
                [y_ref[first : first + size, here], jnp.zeros((padded - size, 128), F32)], axis=0
            )
            o1 = rows(o, 1)
            e = [jnp.where(even, o, lanes(o1, 32)), jnp.where(even, lanes(o, 96), o1)]
            for p in range(2):
                s = rows(e[p], 2)
                for place in (p, p + 2):
                    b = 4 * tile + place
                    if b not in present:
                        continue
                    if place < 2:
                        part = jnp.where(low, e[p], lanes(s, 64))
                    else:
                        part = jnp.where(low, lanes(e[p], 64), s)
                    l_ref[b, 0:padded, 0:128] = part.astype(BF16)
                    l_ref[b, 0:padded, 128:256] = rows(part, 4).astype(BF16)
        for patch, blocks in enumerate(patches):
            lhs = jnp.concatenate([l_ref[b, 0:padded] for b in blocks], axis=0)
            g = lax.dot_general(
                lhs, t_ref[6 * seg + patch], (((1,), (1,)), ((), ())), preferred_element_type=F32
            )
            zero = jnp.zeros((16, 128), F32)
            for place, b in enumerate(blocks):
                part = g[place * padded : place * padded + padded]
                f_ref[b, 0 : padded + 16] = jnp.concatenate(
                    [part[:, :128], zero], axis=0
                ) + jnp.concatenate([zero, part[:, 128:]], axis=0)
        tall = padded + 24
        low = between((tall, 128), 0, 64)
        head = between((tall, 128), 0, 32)
        pad8 = jnp.zeros((8, 128), F32)

        def both_ways(b):
            if b not in present:
                zero = jnp.zeros((tall, 128), F32)
                return zero, zero
            f = f_ref[b, 0 : padded + 16]
            return jnp.concatenate([f, pad8], axis=0), jnp.concatenate([pad8, f], axis=0)

        for tile in range(5):
            both = []
            for p in range(2):
                a0, a8 = both_ways(4 * tile + p)
                b0, b8 = both_ways(4 * tile + p + 2)
                both.append(jnp.where(low, a0, b8) + lanes(jnp.where(low, b0, a8), 64))
            turned = lanes(both[1], 32)
            here = slice(128 * tile, 128 * tile + 128)
            after = slice(128 * tile + 128, 128 * tile + 256)
            span = slice(first, first + tall)
            z_ref[span, here] += both[0] + jnp.where(head, 0.0, turned)
            z_ref[span, after] += jnp.where(head, turned, 0.0)


def total_variation(x_ref, x_first, q1i_ref, q2i_ref, q1_ref, q2_ref, chunks, place):
    row0, col0, limit_row, limit_col = place
    for chunk in chunks:
        start = 16 * chunk
        tall = x_ref[x_first + start : x_first + start + 24, 0:WIDE]
        x = tall[0:16]
        below = rows(tall, -1)[0:16]
        right = lanes(x, -1)
        r = row0 - 32 + start + iota((16, WIDE), 0)
        c = col0 - XO + iota((16, WIDE), 1)
        g1 = jnp.where(r < limit_row, below - x, 0.0)
        g2 = jnp.where(c < limit_col, right - x, 0.0)
        span = slice(start, start + 16)
        u1 = q1i_ref[span] + SIGMA * g1
        u2 = q2i_ref[span] + SIGMA * g2
        shrink = jnp.maximum(1.0, jnp.sqrt(u1 * u1 + u2 * u2) / TV)
        inv = 1.0 / shrink
        q1_ref[span] = u1 * inv
        q2_ref[span] = u2 * inv


def divergence(q1_ref, q2_ref, start, place):
    row0, col0, limit_row, limit_col = place
    above = max(start - 8, 0)
    m1 = q1_ref[above : start + 16]
    m2 = q2_ref[start : start + 16]
    r = row0 - 32 + above + iota(m1.shape, 0)
    c = col0 - XO + iota((16, WIDE), 1)
    m1 = jnp.where((r >= 0) & (r < limit_row), m1, 0.0)
    m2 = jnp.where((c >= 0) & (c < limit_col), m2, 0.0)
    return (m1 - rows(m1, 1))[start - above :] + (m2 - lanes(m2, 1))


def places():
    row = lax.axis_index("row")
    col = lax.axis_index("col")
    return (
        row * ROWS,
        col * COLS,
        lax.axis_size("row") * ROWS - 1,
        lax.axis_size("col") * COLS - 1,
    )


def masks():
    top, bot, left, right = flags()

    def row_ok(seg):
        if seg == 1:
            return jnp.bool_(True)
        return top if seg == 0 else bot

    def col_ok(tile, size):
        lane = iota((size, 128), 1)
        if tile == 0:
            return (lane >= YO) | left
        if tile == 4:
            return (lane < YO) | right
        return jnp.ones((size, 128), jnp.bool_)

    return row_ok, col_ok


def widen(value, shift, width=WIDE):
    pad = jnp.zeros((value.shape[0], width - COLS), F32)
    return lanes(jnp.concatenate([value, pad], axis=1), shift)


def select_tables(table_ref, idx_ref, top_ref, bot_ref, lf_ref, rt_ref, tab_ref):
    lane = iota((1, 128), 1)
    total = jnp.full((1, 128), -1.0, F32)
    lines = (
        top_ref[SM : SM + 16, 0:128].astype(F32)[2:3],
        index_line(idx_ref, 128),
        bot_ref[SM : SM + 16, 0:128].astype(F32)[2:3],
    )
    lf = lf_ref[1, 0:16].astype(F32)
    rt = rt_ref[1, 0:16].astype(F32)
    for r in range(3):
        line = jnp.where(lane == 0, lf[r : r + 1, 18:19], lines[r])
        line = jnp.where(lane == 5, rt[r : r + 1, 112:113], line)
        line = lanes(line, 8 * r)
        total = jnp.where((lane >= 8 * r) & (lane < 8 * r + 6), line, total)
    onehot = jnp.where(total == iota((64, 128), 0).astype(F32), 1.0, 0.0).astype(BF16)
    picked = lax.dot_general(
        onehot, table_ref[...], (((0,), (0,)), ((), ())), preferred_element_type=F32
    )
    tab_ref[...] = picked[0:24]


def main_kernel(
    x_ref, y_ref, o_ref, q_ref, idx_ref, table_ref, top_ref, bot_ref, lf_ref, rt_ref,
    x2_ref, y2_ref,
    xe_ref, c_ref, ob_ref, ys_ref, q1_ref, q2_ref, tab_ref, t_ref, p_ref, a_ref, l_ref, f_ref,
    z_ref, xb_ref, x1_ref,
):
    top_ok, bot_ok, left_ok, right_ok = flags()
    place = places()
    select_tables(table_ref, idx_ref, top_ref, bot_ref, lf_ref, rt_ref, tab_ref)
    build_taps(tab_ref, t_ref)

    def f32(ref, at, count):
        return ref[at : at + count].astype(F32)

    zero = jnp.zeros((48, COLS), F32)
    above = f32(top_ref, SX, 64) + jnp.concatenate([zero, f32(top_ref, SXL, 16)], axis=0)
    below = f32(bot_ref, SX, 64) + jnp.concatenate([f32(bot_ref, SXL, 16), zero], axis=0)
    xe_ref[0:64] = widen(jnp.where(top_ok, above, 0.0), XO, FULL)
    xe_ref[64:192] = widen(x_ref[...], XO, FULL)
    xe_ref[192:256] = widen(jnp.where(bot_ok, below, 0.0), XO, FULL)
    xe_ref[256:272] = jnp.zeros((16, FULL), F32)
    rr = iota((256, 128), 0)
    rows_ok = ((rr >= 64) | top_ok) & ((rr < 192) | bot_ok)
    lf0 = lf_ref[0].astype(F32)
    lf1 = lf_ref[1].astype(F32)
    rt0 = rt_ref[0].astype(F32)
    rt1 = rt_ref[1].astype(F32)
    shape = (256, 128)
    side = jnp.where(between(shape, 16, 80), lf0, 0.0)
    side += jnp.where(between(shape, 64, 80), lanes(lf1, 80), 0.0)
    xe_ref[0:256, 0:128] += jnp.where(rows_ok & left_ok, side, 0.0)
    side = jnp.where(between(shape, 80, 128), rt0, 0.0)
    side += jnp.where(between(shape, 80, 96), lanes(rt1, 48), 0.0)
    xe_ref[0:256, 512:640] += jnp.where(rows_ok & right_ok, side, 0.0)
    side = jnp.where(between(shape, 0, 16), rt0, 0.0)
    xe_ref[0:256, 640:768] += jnp.where(rows_ok & right_ok, side, 0.0)
    seen = o_ref[...]
    c_ref[48:176] = widen(y_ref[...] - SIGMA * seen, YO)
    ob_ref[16:144] = widen(seen, YO)
    zero = jnp.zeros((32, COLS), F32)
    above = f32(top_ref, SC, 48) + jnp.concatenate([zero, f32(top_ref, SCL, 16)], axis=0)
    below = f32(bot_ref, SC, 48) + jnp.concatenate([f32(bot_ref, SCL, 16), zero], axis=0)
    c_ref[0:48] = widen(above, YO)
    c_ref[176:224] = widen(below, YO)
    ob_ref[0:16] = widen(f32(top_ref, SO, 16), YO)
    ob_ref[144:160] = widen(f32(bot_ref, SO, 16), YO)
    shape = (224, 128)
    side = lanes(lf0[0:224], 64) + jnp.where(between(shape, 48, 64), lanes(lf1[0:224], 48), 0.0)
    c_ref[:, 0:128] = jnp.where(between(shape, 16, 64), side, c_ref[:, 0:128])
    side = lanes(rt0[0:224], 48) + jnp.where(between(shape, 64, 80), rt1[0:224], 0.0)
    c_ref[:, 512:640] = jnp.where(between(shape, 64, 112), side, c_ref[:, 512:640])
    shape = (160, 128)
    at = between(shape, 48, 64)
    ob_ref[:, 0:128] = jnp.where(at, lanes(lf0[0:160], 48), ob_ref[:, 0:128])
    ob_ref[:, 512:640] = jnp.where(between(shape, 64, 80), rt0[0:160], ob_ref[:, 512:640])
    rix = iota((32, COLS), 0)
    misc = f32(top_ref, SM, 16)
    shape = (192, 128)
    for comp, (ref, section) in enumerate(((q1_ref, S1), (q2_ref, S2))):
        above = f32(top_ref, section, 32) + jnp.where(rix == 31, misc[comp : comp + 1], 0.0)
        ref[0:32] = widen(above, XO)
        ref[32:160] = widen(q_ref[comp], XO)
        ref[160:192] = widen(f32(bot_ref, section, 32), XO)
        side = lanes(lf1[0:192], 96 * comp)
        side += jnp.where(between(shape, 79, 80), lanes(lf1[0:192], 63 - comp), 0.0)
        ref[:, 0:128] = jnp.where(between(shape, 48, 80), side, ref[:, 0:128])
        side = lanes(rt1[0:192], 80 * comp)
        ref[:, 512:640] = jnp.where(between(shape, 80, 112), side, ref[:, 512:640])
    row_ok, col_ok = masks()
    windows(xe_ref, p_ref, 256)
    blur(SEGS1, PATCHES1, p_ref, t_ref, a_ref, c_ref, ys_ref, row_ok, col_ok)
    total_variation(xe_ref, 32, q1_ref, q2_ref, q1_ref, q2_ref, range(12), place)
    adjoint(SEGS1, PATCHES1, ys_ref, t_ref, l_ref, f_ref, z_ref)
    lane = iota((16, WIDE), 1)
    inside = ((lane >= XO) | left_ok) & ((lane < XO + COLS) | right_ok)
    for chunk in range(12):
        start = 16 * chunk
        ext = slice(32 + start, 48 + start)
        x = xe_ref[ext, 0:WIDE]
        new = x - TAU * (z_ref[ext, 0:WIDE] - divergence(q1_ref, q2_ref, start, place))
        keep = inside & (top_ok if chunk < 2 else bot_ok) if chunk < 2 or chunk >= 10 else inside
        xb_ref[start : start + 16, 0:WIDE] = jnp.where(keep, 2.0 * new - x, 0.0)
        if 2 <= chunk < 10:
            x1_ref[start - 32 : start - 16] = new
    xb_ref[192:208, 0:WIDE] = jnp.zeros((16, WIDE), F32)
    xb_ref[:, WIDE:FULL] = jnp.zeros((208, FULL - WIDE), F32)
    c_ref[0:160] = ys_ref[32:192] - SIGMA * ob_ref[...]
    windows(xb_ref, p_ref, 192)
    blur(SEGS2, PATCHES2, p_ref, t_ref, a_ref, c_ref, ys_ref, row_ok, col_ok)
    total_variation(xb_ref, 0, q1_ref, q2_ref, q1_ref, q2_ref, range(1, 10), place)
    adjoint(SEGS2, PATCHES2, ys_ref, t_ref, l_ref, f_ref, z_ref)
    for chunk in range(8):
        span = slice(16 * chunk, 16 * chunk + 16)
        ext = slice(32 + 16 * chunk, 48 + 16 * chunk)
        div = divergence(q1_ref, q2_ref, 32 + 16 * chunk, place)
        new = x1_ref[span] - TAU * (z_ref[ext, 0:WIDE] - div)
        x2_ref[span] = lanes(new, -XO)[:, :COLS]
        y2_ref[span] = lanes(ys_ref[16 + 16 * chunk : 32 + 16 * chunk], -YO)[:, :COLS]


def field(*shape, dtype=F32):
    return jax.ShapeDtypeStruct(shape, dtype)


def call(kernel, outs, scratch, *args, name, room=4, far=0):
    spaces = [pltpu.HBM] * far + [pltpu.VMEM] * (len(args) - far)
    return pl.pallas_call(
        kernel,
        out_shape=outs,
        in_specs=[pl.BlockSpec(memory_space=space) for space in spaces],
        scratch_shapes=scratch,
        compiler_params=pltpu.CompilerParams(vmem_limit_bytes=room * 1024 * 1024),
        name=name,
    )(*args)


def ring(block, axis, distance):
    count = lax.axis_size(axis)
    return lax.ppermute(block, axis, [(i, (i + distance) % count) for i in range(count)])


def per_device(observed, psf_table, psf_index, start_image, blur_dual, tv_dual):
    own = (start_image, blur_dual, observed, tv_dual)
    block = pltpu.VMEM((ROWS, COLS), F32)
    strip = field(STRIP, COLS, dtype=BF16)
    side = field(2, 256, 128, dtype=BF16)
    down, up = call(
        pack_rows_kernel, (strip, strip),
        [block, block, block, pltpu.VMEM((2, ROWS, COLS), F32), pltpu.SemaphoreType.DMA((4,))],
        *own, psf_index, name="pack_rows", far=4, room=60,
    )
    top = ring(down, "row", 1)
    bot = ring(up, "row", -1)
    table = psf_table.astype(F32)
    normed = (table / jnp.sum(table, axis=(1, 2), keepdims=True)).astype(BF16)
    normed = jnp.pad(normed[:, :, ::-1], ((0, 0), (1, 0), (0, 1))).reshape(64, 1024)
    to_right, to_left = call(
        pack_cols_kernel, (side, side), [], *own, psf_index, top, bot, name="pack_cols"
    )
    lf = ring(to_right, "col", 1)
    rt = ring(to_left, "col", -1)
    wide = pltpu.VMEM((192, WIDE), F32)
    return call(
        main_kernel,
        (field(ROWS, COLS), field(ROWS, COLS)),
        [
            pltpu.VMEM((272, FULL), F32), pltpu.VMEM((224, WIDE), F32),
            pltpu.VMEM((160, WIDE), F32), pltpu.VMEM((224, WIDE), F32),
            wide, wide, pltpu.VMEM((24, 1024), F32),
            pltpu.VMEM((18, 256, 256), BF16), pltpu.VMEM((20, 256, 128), BF16),
            pltpu.VMEM((20, 144, 128), F32), pltpu.VMEM((20, 144, 256), BF16),
            pltpu.VMEM((20, 160, 128), F32), pltpu.VMEM((272, FULL), F32),
            pltpu.VMEM((208, FULL), F32), pltpu.VMEM((ROWS, WIDE), F32),
        ],
        *own, psf_index, normed, top, bot, lf, rt, name="main", room=28,
    )


def solution(mesh):
    placed = (
        P("row", "col"),
        P(),
        P("row", "col"),
        P("row", "col"),
        P("row", "col"),
        P(None, "row", "col"),
    )
    return jax.shard_map(
        per_device,
        mesh=mesh,
        in_specs=placed,
        out_specs=(P("row", "col"), P("row", "col")),
        check_vma=False,
    )
```

```python
import jax
import jax.numpy as jnp
from jax import lax
from jax.experimental import pallas as pl
from jax.experimental.pallas import tpu as pltpu
from jax.sharding import PartitionSpec as P

SIGMA = 0.15
TAU = 0.6
TV = 0.5
F32 = jnp.float32
BF16 = jnp.bfloat16

ROWS = 128
COLS = 512
XO = 80
YO = 64
WIDE = 640
FULL = 768
SEGS1 = ((0, 48, 64), (48, 128, 144), (176, 48, 64))
SEGS2 = ((0, 16, 32), (16, 128, 144), (144, 16, 32))
PATCHES2 = ((1,), (2, 3, 4, 5), (6, 7, 8, 9), (10, 11, 12, 13), (14, 15, 16, 17), (18,))
INNER = ((0, (3, 4, 5)), (1, (6, 7, 8, 9)), (2, (10, 11, 12, 13)), (3, (14, 15, 16)))
OUTER = ((-1, (0, 1)), (0, (2,)), (3, (17,)), (4, (18, 19)))
ALL = tuple((patch - 1, blocks) for patch, blocks in enumerate(PATCHES2))
SX, SXL, SC, SCL, SO, S1, S2, SM, STRIP = 0, 64, 80, 128, 144, 160, 192, 224, 240


def iota(shape, dim):
    return lax.broadcasted_iota(jnp.int32, shape, dim)


def split(value):
    hi = value.astype(BF16).astype(F32)
    return hi, value - hi


def lanes(value, shift):
    shift = shift % value.shape[1]
    return pltpu.roll(value, shift, 1) if shift else value


def rows(value, shift):
    shift = shift % value.shape[0]
    return pltpu.roll(value, shift, 0) if shift else value


def between(shape, lo, hi):
    lane = iota(shape, 1)
    return (lane >= lo) & (lane < hi)


def flags():
    row = lax.axis_index("row")
    col = lax.axis_index("col")
    return (
        row > 0,
        row < lax.axis_size("row") - 1,
        col > 0,
        col < lax.axis_size("col") - 1,
    )


def index_line(idx_ref, width):
    lane = iota((1, width), 1)
    line = jnp.zeros((1, width), F32)
    for j in range(4):
        line = jnp.where(lane == 1 + j, idx_ref[0:1, j : j + 1].astype(F32), line)
    return line


def parities():
    return lax.axis_index("row") % 2 == 1, lax.axis_index("col") % 2 == 1


def chosen(flag, one_ref, two_ref):
    def read(at):
        return jnp.where(flag, one_ref[at].astype(F32), two_ref[at].astype(F32))

    return read


def sides(a_ref, b_ref, odd):
    return chosen(odd, a_ref, b_ref), chosen(odd, b_ref, a_ref)


def pack_rows_kernel(x_hbm, y_hbm, o_hbm, q_hbm, idx_ref, a_ref, b_ref, x_ref, y_ref, o_ref, q_ref, sems):
    copies = [
        pltpu.make_async_copy(src, dst, sems.at[i])
        for i, (src, dst) in enumerate(((x_hbm, x_ref), (y_hbm, y_ref), (o_hbm, o_ref), (q_hbm, q_ref)))
    ]
    for copy in copies:
        copy.start()
    line = index_line(idx_ref, COLS)
    odd, _ = parities()

    def put(at, count, down, up):
        a_ref[at : at + count] = jnp.where(odd, up, down).astype(BF16)
        b_ref[at : at + count] = jnp.where(odd, down, up).astype(BF16)

    copies[0].wait()
    put(SX, 64, x_ref[64:128], x_ref[0:64])
    put(SXL, 16, split(x_ref[112:128])[1], split(x_ref[0:16])[1])
    copies[1].wait()
    copies[2].wait()
    up = y_ref[0:48] - SIGMA * o_ref[0:48]
    down = y_ref[80:128] - SIGMA * o_ref[80:128]
    put(SC, 48, down, up)
    put(SCL, 16, split(down[32:48])[1], split(up[0:16])[1])
    put(SO, 16, o_ref[112:128], o_ref[0:16])
    copies[3].wait()
    put(S1, 32, q_ref[0, 96:128], q_ref[0, 0:32])
    put(S2, 32, q_ref[1, 96:128], q_ref[1, 0:32])
    row = iota((16, COLS), 0)
    rest = []
    for edge in (127, 0):
        misc = jnp.zeros((16, COLS), F32)
        for comp in range(2):
            misc = jnp.where(row == comp, split(q_ref[comp, edge : edge + 1])[1], misc)
        rest.append(jnp.where(row == 2, line, misc))
    put(SM, 16, *rest)


def pack_cols_kernel(x_ref, y_ref, o_ref, q_ref, idx_ref, ra_ref, rb_ref, a_ref, b_ref):
    odd_row, odd_col = parities()
    top, bot = sides(ra_ref, rb_ref, odd_row)
    made = []
    for base in (384, 0):
        right = base > 0
        own = slice(base, base + 128)

        def strip(read, at, count, own=own):
            return read((slice(at, at + count), own))

        def column(middle, at, count, shift):
            parts = [strip(top, at, count), middle, strip(bot, at, count)]
            return lanes(jnp.concatenate(parts, axis=0), shift)

        seen = o_ref[:, own]
        x_hi, x_lo = split(x_ref[:, own])
        c_hi, c_lo = split(y_ref[:, own] - SIGMA * seen)
        zeros = jnp.zeros((128, 128), F32)
        buf = column(x_hi, SX, 64, 80)
        part = jnp.concatenate([column(c_hi, SC, 48, 0 if right else 16), zeros[:32]], axis=0)
        at = 80 if right else 16
        buf = jnp.where(between((256, 128), at, at + 48), part, buf)
        part = jnp.concatenate([column(seen, SO, 16, 16 if right else 64), zeros[:96]], axis=0)
        at = 0 if right else 64
        buf = jnp.where(between((256, 128), at, at + 16), part, buf)
        made.append(buf)
        buf = jnp.concatenate([column(q_ref[0, :, own], S1, 32, 80), zeros[:64]], axis=0)
        part = jnp.concatenate(
            [column(q_ref[1, :, own], S2, 32, 112 if right else 0), zeros[:64]], axis=0
        )
        at = 80 if right else 0
        buf = jnp.where(between((256, 128), at, at + 32), part, buf)
        shift = 0 if right else 32
        part = jnp.concatenate(
            [
                zeros[:48],
                lanes(strip(top, SXL, 16), shift),
                lanes(x_lo, shift),
                lanes(strip(bot, SXL, 16), shift),
                zeros[:48],
            ],
            axis=0,
        )
        at = 112 if right else 32
        buf = jnp.where(between((256, 128), at, at + 16), part, buf)
        shift = 16 if right else 64
        part = jnp.concatenate(
            [
                zeros[:32],
                lanes(strip(top, SCL, 16), shift),
                lanes(c_lo, shift),
                lanes(strip(bot, SCL, 16), shift),
                zeros[:64],
            ],
            axis=0,
        )
        at = 0 if right else 64
        buf = jnp.where(between((256, 128), at, at + 16), part, buf)
        if right:
            for comp in range(2):
                low = lanes(split(q_ref[comp, :, own])[1], 17 + comp)
                part = jnp.concatenate([zeros[:32], low, zeros[:96]], axis=0)
                buf = jnp.where(between((256, 128), 16 + comp, 17 + comp), part, buf)
        row = iota((256, 1), 0)
        spot = 4 if right else 1
        first = top((slice(SM, SM + 16), slice(0, 128)))[2:3, spot : spot + 1]
        last = bot((slice(SM, SM + 16), slice(0, 128)))[2:3, spot : spot + 1]
        mine = idx_ref[0:1, spot - 1 : spot].astype(F32)
        entry = jnp.where(row == 0, first, jnp.where(row == 1, mine, last))
        at = 18 if right else 112
        buf = jnp.where(between((256, 128), at, at + 1), entry, buf)
        made.append(buf)
    for tile in range(2):
        a_ref[tile] = jnp.where(odd_col, made[2 + tile], made[tile]).astype(BF16)
        b_ref[tile] = jnp.where(odd_col, made[tile], made[2 + tile]).astype(BF16)


def build_taps(tab_ref, t_ref, places):
    size = 8 * len(places)
    sub = iota((size, 128), 0)
    bits = [(sub // (1 << n)) % 2 == 1 for n in range(3)]
    for e in range(8):
        a1, half = e // 2, e % 2
        here = slice(128 * half, 128 * half + 128)
        skew = jnp.concatenate(
            [
                jnp.broadcast_to(
                    tab_ref[at : at + 1, 128 * e : 128 * e + 128], (8, 128)
                )
                for at in places
            ],
            axis=0,
        )
        for n in range(3):
            skew = jnp.where(bits[n], lanes(skew, 1 << n), skew)
        lower_all = [iota((size, 128), 1) % 32 <= sub % 8 + 8 * v for v in range(4)]
        low = [jnp.where(lower_all[v], lanes(skew, 8 * v - 31), 0.0) for v in range(4)]
        high = [jnp.where(lower_all[v], 0.0, lanes(skew, 8 * v + 1)) for v in range(4)]
        for patch in range(len(places)):
            own = slice(8 * patch, 8 * patch + 8)
            block = jnp.concatenate([part[own] for part in low + high], axis=0)
            t_ref[patch, 64 * a1 : 64 * a1 + 64, here] = block.astype(BF16)


def windows(get, p_ref, blocks, count):
    low = between((count, 128), 0, 64)
    tail = between((count, 128), 96, 128)
    for b in blocks:
        tile, place = b // 4, b % 4
        x0, x8 = get(tile, 0), get(tile, 8)
        if place == 0:
            part = jnp.where(low, x0, lanes(x8, 64))
        elif place == 1:
            part = jnp.where(low, lanes(x0, 96), lanes(x8, 32))
        elif place == 2:
            part = jnp.where(low, lanes(x0, 64), x8)
        else:
            w0 = jnp.where(tail, x0, get(tile + 1, 0))
            w8 = jnp.where(tail, x8, get(tile + 1, 8))
            part = jnp.where(low, lanes(w0, 32), lanes(w8, 96))
        p_ref[b, 0:count] = part.astype(BF16)


def blur(segs, groups, taps, p_ref, a_ref, put):
    present = [b for _, blocks in groups for b in blocks]
    for seg, (first, size, padded) in enumerate(segs):
        for patch, blocks in groups:
            lhs = jnp.concatenate(
                [
                    jnp.concatenate(
                        [
                            p_ref[b, first : first + padded],
                            p_ref[b, first + 16 : first + 16 + padded],
                        ],
                        axis=1,
                    )
                    for b in blocks
                ],
                axis=0,
            )
            v = jnp.dot(lhs, taps(seg, patch), preferred_element_type=F32)
            for place, b in enumerate(blocks):
                part = v[place * padded : place * padded + padded]
                a_ref[b, 0:padded] = part[:, :128] + rows(part[:, 128:], -4)
        low = between((padded, 128), 0, 64)
        even = iota((padded, 128), 1) % 64 < 32
        for tile in sorted({b // 4 for b in present}):
            a = [
                a_ref[4 * tile + p, 0:padded]
                if 4 * tile + p in present
                else jnp.zeros((padded, 128), F32)
                for p in range(4)
            ]
            e = []
            for p in range(2):
                z = lanes(jnp.where(low, a[p + 2], a[p]), 64)
                e.append(jnp.where(low, a[p], z) + rows(jnp.where(low, z, a[p + 2]), -2))
            m1 = jnp.where(even, e[0], lanes(e[1], 32))
            m2 = jnp.where(even, lanes(e[0], 96), e[1])
            blurred = (m1 + rows(m2, -1))[0:size]
            put(seg, first, size, tile, blurred)


def adjoint(segs, groups, taps, get, l_ref, f_ref, z_ref):
    present = [b for _, blocks in groups for b in blocks]
    tiles = sorted({b // 4 for b in present})
    for seg, (first, size, padded) in enumerate(segs):
        low = between((padded, 128), 0, 64)
        even = iota((padded, 128), 1) % 64 < 32
        for tile in tiles:
            o = jnp.concatenate(
                [get(first, size, tile), jnp.zeros((padded - size, 128), F32)], axis=0
            )
            o1 = rows(o, 1)
            e = [jnp.where(even, o, lanes(o1, 32)), jnp.where(even, lanes(o, 96), o1)]
            for p in range(2):
                s = rows(e[p], 2)
                for place in (p, p + 2):
                    b = 4 * tile + place
                    if b not in present:
                        continue
                    if place < 2:
                        part = jnp.where(low, e[p], lanes(s, 64))
                    else:
                        part = jnp.where(low, lanes(e[p], 64), s)
                    l_ref[b, 0:padded, 0:128] = part.astype(BF16)
                    l_ref[b, 0:padded, 128:256] = rows(part, 4).astype(BF16)
        for patch, blocks in groups:
            lhs = jnp.concatenate([l_ref[b, 0:padded] for b in blocks], axis=0)
            g = lax.dot_general(
                lhs, taps(seg, patch), (((1,), (1,)), ((), ())), preferred_element_type=F32
            )
            zero = jnp.zeros((16, 128), F32)
            for place, b in enumerate(blocks):
                part = g[place * padded : place * padded + padded]
                f_ref[b, 0 : padded + 16] = jnp.concatenate(
                    [part[:, :128], zero], axis=0
                ) + jnp.concatenate([zero, part[:, 128:]], axis=0)
        tall = padded + 24
        low = between((tall, 128), 0, 64)
        head = between((tall, 128), 0, 32)
        pad8 = jnp.zeros((8, 128), F32)

        def both_ways(b):
            if b not in present:
                zero = jnp.zeros((tall, 128), F32)
                return zero, zero
            f = f_ref[b, 0 : padded + 16]
            return jnp.concatenate([f, pad8], axis=0), jnp.concatenate([pad8, f], axis=0)

        for tile in tiles:
            both = []
            for p in range(2):
                a0, a8 = both_ways(4 * tile + p)
                b0, b8 = both_ways(4 * tile + p + 2)
                both.append(jnp.where(low, a0, b8) + lanes(jnp.where(low, b0, a8), 64))
            turned = lanes(both[1], 32)
            here = slice(128 * tile, 128 * tile + 128)
            after = slice(128 * tile + 128, 128 * tile + 256)
            span = slice(first, first + tall)
            z_ref[span, here] += both[0] + jnp.where(head, 0.0, turned)
            z_ref[span, after] += jnp.where(head, turned, 0.0)


def total_variation(get_x, get_q, q1_ref, q2_ref, chunks, place):
    row0, col0, limit_row, limit_col = place
    for chunk in chunks:
        start = 16 * chunk
        tall = get_x(start, 24)
        x = tall[0:16]
        below = rows(tall, -1)[0:16]
        right = lanes(x, -1)
        r = row0 - 32 + start + iota((16, WIDE), 0)
        c = col0 - XO + iota((16, WIDE), 1)
        g1 = jnp.where(r < limit_row, below - x, 0.0)
        g2 = jnp.where(c < limit_col, right - x, 0.0)
        span = slice(start, start + 16)
        u1 = get_q(0, start) + SIGMA * g1
        u2 = get_q(1, start) + SIGMA * g2
        shrink = jnp.maximum(1.0, jnp.sqrt(u1 * u1 + u2 * u2) / TV)
        inv = 1.0 / shrink
        q1_ref[span] = u1 * inv
        q2_ref[span] = u2 * inv


def divergence(q1_ref, q2_ref, start, place):
    row0, col0, limit_row, limit_col = place
    above = max(start - 8, 0)
    m1 = q1_ref[above : start + 16]
    m2 = q2_ref[start : start + 16]
    r = row0 - 32 + above + iota(m1.shape, 0)
    c = col0 - XO + iota((16, WIDE), 1)
    m1 = jnp.where((r >= 0) & (r < limit_row), m1, 0.0)
    m2 = jnp.where((c >= 0) & (c < limit_col), m2, 0.0)
    return (m1 - rows(m1, 1))[start - above :] + (m2 - lanes(m2, 1))


def places():
    row = lax.axis_index("row")
    col = lax.axis_index("col")
    return (
        row * ROWS,
        col * COLS,
        lax.axis_size("row") * ROWS - 1,
        lax.axis_size("col") * COLS - 1,
    )


def masks():
    top, bot, left, right = flags()

    def row_ok(seg):
        if seg == 1:
            return jnp.bool_(True)
        return top if seg == 0 else bot

    def col_ok(tile, size):
        lane = iota((size, 128), 1)
        if tile == 0:
            return (lane >= YO) | left
        if tile == 4:
            return (lane < YO) | right
        return jnp.ones((size, 128), jnp.bool_)

    return row_ok, col_ok


def widen(value, shift, width=WIDE):
    pad = jnp.zeros((value.shape[0], width - COLS), F32)
    return lanes(jnp.concatenate([value, pad], axis=1), shift)


def select_tables(table_ref, total, tab_ref):
    onehot = jnp.where(total == iota((64, 128), 0).astype(F32), 1.0, 0.0).astype(BF16)
    picked = lax.dot_general(
        onehot, table_ref[...], (((0,), (0,)), ((), ())), preferred_element_type=F32
    )
    tab_ref[...] = picked[0:24]


def tile_of(value, tile):
    return value[:, 128 * tile : 128 * tile + 128]


def middle_kernel(
    x_ref, y_ref, o_ref, q_ref, idx_ref, table_ref, ra_ref, rb_ref,
    xe_ref, c_ref, ob_ref, ys_ref, q1_ref, q2_ref, z_ref, t_ref,
    tab_ref, p_ref, a_ref, l_ref, f_ref,
):
    top_ok, bot_ok, _, _ = flags()
    odd, _ = parities()
    top, bot = sides(ra_ref, rb_ref, odd)
    misc = slice(SM, SM + 16)
    lane = iota((1, 128), 1)
    lines = (
        top((misc, slice(0, 128)))[2:3], index_line(idx_ref, 128), bot((misc, slice(0, 128)))[2:3],
    )
    total = jnp.full((1, 128), -1.0, F32)
    for r in range(3):
        total = jnp.where((lane >= 8 * r) & (lane < 8 * r + 6), lanes(lines[r], 8 * r), total)
    select_tables(table_ref, total, tab_ref)
    build_taps(tab_ref, t_ref, [8 * r + 1 + p for r in range(3) for p in range(4)])

    def part(read, at, count):
        return read(slice(at, at + count))

    zero = jnp.zeros((48, COLS), F32)
    above = part(top, SX, 64) + jnp.concatenate([zero, part(top, SXL, 16)], axis=0)
    below = part(bot, SX, 64) + jnp.concatenate([part(bot, SXL, 16), zero], axis=0)
    xe_ref[0:64] = widen(jnp.where(top_ok, above, 0.0), XO, FULL)
    xe_ref[64:192] = widen(x_ref[...], XO, FULL)
    xe_ref[192:256] = widen(jnp.where(bot_ok, below, 0.0), XO, FULL)
    xe_ref[256:272] = jnp.zeros((16, FULL), F32)
    seen = o_ref[...]
    c_ref[48:176] = widen(y_ref[...] - SIGMA * seen, YO)
    ob_ref[16:144] = widen(seen, YO)
    zero = jnp.zeros((32, COLS), F32)
    above = part(top, SC, 48) + jnp.concatenate([zero, part(top, SCL, 16)], axis=0)
    below = part(bot, SC, 48) + jnp.concatenate([part(bot, SCL, 16), zero], axis=0)
    c_ref[0:48] = widen(above, YO)
    c_ref[176:224] = widen(below, YO)
    ob_ref[0:16] = widen(part(top, SO, 16), YO)
    ob_ref[144:160] = widen(part(bot, SO, 16), YO)
    rix = iota((32, COLS), 0)
    rest = top(misc)
    for comp, (ref, section) in enumerate(((q1_ref, S1), (q2_ref, S2))):
        above = part(top, section, 32) + jnp.where(rix == 31, rest[comp : comp + 1], 0.0)
        ref[0:32] = widen(above, XO)
        ref[32:160] = widen(q_ref[comp], XO)
        ref[160:192] = widen(part(bot, section, 32), XO)
    row_ok, _ = masks()

    def taps(seg, patch):
        return t_ref[4 * seg + patch]

    def get_x(tile, first):
        return xe_ref[first : first + 256, 128 * tile : 128 * tile + 128]

    def put(seg, first, size, tile, blurred):
        here = slice(128 * tile, 128 * tile + 128)
        new = (c_ref[first : first + size, here] + SIGMA * blurred) / (1.0 + SIGMA)
        ys_ref[first : first + size, here] = jnp.where(row_ok(seg), new, 0.0)

    def get_y(first, size, tile):
        return ys_ref[first : first + size, 128 * tile : 128 * tile + 128]

    windows(get_x, p_ref, range(3, 17), 256)
    blur(SEGS1, INNER, taps, p_ref, a_ref, put)
    z_ref[...] = jnp.zeros_like(z_ref)
    adjoint(SEGS1, INNER, taps, get_y, l_ref, f_ref, z_ref)


def main_kernel(
    idx_ref, table_ref, ra_ref, rb_ref, ca_ref, cb_ref,
    xi_ref, ci_ref, oi_ref, yi_ref, q1i_ref, q2i_ref, zi_ref, ti_ref,
    x2_ref, y2_ref,
    side_ref, qs_ref, ys_ref, c_ref, q1_ref, q2_ref, tab_ref, t_ref, p_ref, a_ref, l_ref, f_ref,
    z_ref, xb_ref, x1_ref,
):
    top_ok, bot_ok, left_ok, right_ok = flags()
    place = places()
    odd_row, odd_col = parities()
    top, bot = sides(ra_ref, rb_ref, odd_row)
    before, after = sides(ca_ref, cb_ref, odd_col)
    lf0, lf1, rt0, rt1 = before(0), before(1), after(0), after(1)
    lane = iota((1, 128), 1)
    total = jnp.full((1, 128), -1.0, F32)
    for r in range(3):
        total = jnp.where(lane == 8 * r, lf1[r : r + 1, 18:19], total)
        total = jnp.where(lane == 8 * r + 5, rt1[r : r + 1, 112:113], total)
    select_tables(table_ref, total, tab_ref)
    build_taps(tab_ref, t_ref, [8 * r + p for r in range(3) for p in (0, 5)])

    def taps(seg, patch):
        if 0 <= patch < 4:
            return ti_ref[4 * seg + patch]
        return t_ref[2 * seg + (patch == 4)]

    rr = iota((256, 128), 0)
    rows_ok = ((rr >= 64) | top_ok) & ((rr < 192) | bot_ok)
    shape = (256, 128)
    part = jnp.where(between(shape, 16, 80), lf0, 0.0)
    part += jnp.where(between(shape, 64, 80), lanes(lf1, 80), 0.0)
    side_ref[0, 0:256] = xi_ref[0:256, 0:128] + jnp.where(rows_ok & left_ok, part, 0.0)
    part = jnp.where(between(shape, 80, 128), rt0, 0.0)
    part += jnp.where(between(shape, 80, 96), lanes(rt1, 48), 0.0)
    side_ref[1, 0:256] = xi_ref[0:256, 512:640] + jnp.where(rows_ok & right_ok, part, 0.0)
    part = jnp.where(between(shape, 0, 16), rt0, 0.0)
    side_ref[2, 0:256] = xi_ref[0:256, 640:768] + jnp.where(rows_ok & right_ok, part, 0.0)
    side_ref[:, 256:272] = jnp.zeros((3, 16, 128), F32)
    shape = (192, 128)
    for comp, ref in enumerate((q1i_ref, q2i_ref)):
        part = lanes(lf1[0:192], 96 * comp)
        part += jnp.where(between(shape, 79, 80), lanes(lf1[0:192], 63 - comp), 0.0)
        qs_ref[comp, 0] = jnp.where(between(shape, 48, 80), part, ref[:, 0:128])
        part = lanes(rt1[0:192], 80 * comp)
        qs_ref[comp, 1] = jnp.where(between(shape, 80, 112), part, ref[:, 512:640])
    shape = (224, 128)
    part = lanes(lf0[0:224], 64) + jnp.where(between(shape, 48, 64), lanes(lf1[0:224], 48), 0.0)
    c_first = jnp.where(between(shape, 16, 64), part, ci_ref[:, 0:128])
    part = lanes(rt0[0:224], 48) + jnp.where(between(shape, 64, 80), rt1[0:224], 0.0)
    c_last = jnp.where(between(shape, 64, 112), part, ci_ref[:, 512:640])
    shape = (160, 128)
    o_first = jnp.where(between(shape, 48, 64), lanes(lf0[0:160], 48), oi_ref[:, 0:128])
    o_last = jnp.where(between(shape, 64, 80), rt0[0:160], oi_ref[:, 512:640])
    row_ok, col_ok = masks()

    def get_side(tile, first):
        which = {0: 0, 4: 1, 5: 2}[tile]
        return side_ref[which, first : first + 256]

    def put_side(seg, first, size, tile, blurred):
        c = (c_first if tile == 0 else c_last)[first : first + size]
        new = (c + SIGMA * blurred) / (1.0 + SIGMA)
        new = jnp.where(col_ok(tile, size) & row_ok(seg), new, 0.0)
        old = yi_ref[first : first + size, 128 * tile : 128 * tile + 128]
        inner = between((size, 128), 96, 128) if tile == 0 else between((size, 128), 0, 32)
        ys_ref[tile // 4, first : first + size] = jnp.where(inner, old, new)

    def get_side_y(first, size, tile):
        return ys_ref[tile // 4, first : first + size]

    windows(get_side, p_ref, (0, 1, 2, 17, 18, 19), 256)
    blur(SEGS1, OUTER, taps, p_ref, a_ref, put_side)

    def get_x(start, count):
        at = slice(32 + start, 32 + start + count)
        return jnp.concatenate([side_ref[0, at], xi_ref[at, 128:512], side_ref[1, at]], axis=1)

    def get_q(comp, start):
        at = slice(start, start + 16)
        ref = q2i_ref if comp else q1i_ref
        return jnp.concatenate([qs_ref[comp, 0, at], ref[at, 128:512], qs_ref[comp, 1, at]], axis=1)

    total_variation(get_x, get_q, q1_ref, q2_ref, range(12), place)
    z_ref[...] = zi_ref[...]
    adjoint(SEGS1, OUTER, taps, get_side_y, l_ref, f_ref, z_ref)
    lane = iota((16, WIDE), 1)
    inside = ((lane >= XO) | left_ok) & ((lane < XO + COLS) | right_ok)
    for chunk in range(12):
        start = 16 * chunk
        ext = slice(32 + start, 48 + start)
        x = get_x(start, 16)
        new = x - TAU * (z_ref[ext, 0:WIDE] - divergence(q1_ref, q2_ref, start, place))
        keep = inside & (top_ok if chunk < 2 else bot_ok) if chunk < 2 or chunk >= 10 else inside
        xb_ref[start : start + 16, 0:WIDE] = jnp.where(keep, 2.0 * new - x, 0.0)
        if 2 <= chunk < 10:
            x1_ref[start - 32 : start - 16] = new
    xb_ref[192:208, 0:WIDE] = jnp.zeros((16, WIDE), F32)
    xb_ref[:, WIDE:FULL] = jnp.zeros((208, FULL - WIDE), F32)
    c_ref[:, 0:128] = ys_ref[0, 32:192] - SIGMA * o_first
    c_ref[:, 128:512] = yi_ref[32:192, 128:512] - SIGMA * oi_ref[:, 128:512]
    c_ref[:, 512:640] = ys_ref[1, 32:192] - SIGMA * o_last

    def get_xb(tile, first):
        return xb_ref[first : first + 192, 128 * tile : 128 * tile + 128]

    def put(seg, first, size, tile, blurred):
        here = slice(128 * tile, 128 * tile + 128)
        new = (c_ref[first : first + size, here] + SIGMA * blurred) / (1.0 + SIGMA)
        c_ref[first : first + size, here] = jnp.where(col_ok(tile, size) & row_ok(seg), new, 0.0)

    def get_y(first, size, tile):
        return c_ref[first : first + size, 128 * tile : 128 * tile + 128]

    windows(get_xb, p_ref, range(1, 19), 192)
    blur(SEGS2, ALL, taps, p_ref, a_ref, put)
    total_variation(
        lambda start, count: xb_ref[start : start + count, 0:WIDE],
        lambda comp, start: (q2_ref if comp else q1_ref)[start : start + 16],
        q1_ref, q2_ref, range(1, 10), place,
    )
    z_ref[...] = jnp.zeros_like(z_ref)
    adjoint(SEGS2, ALL, taps, get_y, l_ref, f_ref, z_ref)
    for chunk in range(8):
        span = slice(16 * chunk, 16 * chunk + 16)
        ext = slice(32 + 16 * chunk, 48 + 16 * chunk)
        div = divergence(q1_ref, q2_ref, 32 + 16 * chunk, place)
        new = x1_ref[span] - TAU * (z_ref[ext, 0:WIDE] - div)
        x2_ref[span] = lanes(new, -XO)[:, :COLS]
        y2_ref[span] = lanes(c_ref[16 + 16 * chunk : 32 + 16 * chunk], -YO)[:, :COLS]


def field(*shape, dtype=F32):
    return jax.ShapeDtypeStruct(shape, dtype)


def call(kernel, outs, scratch, *args, name, room=4, far=0, flops=0):
    spaces = [pltpu.HBM] * far + [pltpu.VMEM] * (len(args) - far)
    return pl.pallas_call(
        kernel,
        out_shape=outs,
        in_specs=[pl.BlockSpec(memory_space=space) for space in spaces],
        scratch_shapes=scratch,
        compiler_params=pltpu.CompilerParams(vmem_limit_bytes=room * 1024 * 1024),
        cost_estimate=pl.CostEstimate(flops=flops, bytes_accessed=0, transcendentals=0)
        if flops
        else None,
        name=name,
    )(*args)


def swap(block, axis, first):
    count = lax.axis_size(axis)
    pairs = [(i % count, (i + 1) % count) for i in range(first, count + first, 2)]
    return lax.ppermute(block, axis, pairs + [(b, a) for a, b in pairs])


def per_device(observed, psf_table, psf_index, start_image, blur_dual, tv_dual):
    own = (start_image, blur_dual, observed, tv_dual)
    block = pltpu.VMEM((ROWS, COLS), F32)
    strip = field(STRIP, COLS, dtype=BF16)
    side = field(2, 256, 128, dtype=BF16)
    a, b = call(
        pack_rows_kernel, (strip, strip),
        [block, block, block, pltpu.VMEM((2, ROWS, COLS), F32), pltpu.SemaphoreType.DMA((4,))],
        *own, psf_index, name="pack_rows", far=4, room=62,
    )
    ra = swap(a, "row", 0)
    rb = swap(b, "row", 1)
    table = psf_table.astype(F32)
    normed = (table / jnp.sum(table, axis=(1, 2), keepdims=True)).astype(BF16)
    normed = jnp.pad(normed[:, :, ::-1], ((0, 0), (1, 0), (0, 1))).reshape(64, 1024)
    a, b = call(
        pack_cols_kernel, (side, side), [], *own, psf_index, ra, rb, name="pack_cols"
    )
    ca = swap(a, "col", 0)
    cb = swap(b, "col", 1)
    work = [
        pltpu.VMEM((20, 256, 128), BF16), pltpu.VMEM((20, 144, 128), F32),
        pltpu.VMEM((20, 144, 256), BF16), pltpu.VMEM((20, 160, 128), F32),
    ]
    wide = field(192, WIDE)
    ready = call(
        middle_kernel,
        (
            field(272, FULL), field(224, WIDE), field(160, WIDE), field(224, WIDE), wide, wide,
            field(272, FULL), field(12, 256, 256, dtype=BF16),
        ),
        [pltpu.VMEM((24, 1024), F32)] + work,
        *own, psf_index, normed, ra, rb, name="middle", room=16, flops=1 << 33,
    )
    return call(
        main_kernel,
        (field(ROWS, COLS), field(ROWS, COLS)),
        [
            pltpu.VMEM((3, 272, 128), F32), pltpu.VMEM((2, 2, 192, 128), F32),
            pltpu.VMEM((2, 224, 128), F32), pltpu.VMEM((160, WIDE), F32),
            pltpu.VMEM((192, WIDE), F32), pltpu.VMEM((192, WIDE), F32),
            pltpu.VMEM((24, 1024), F32), pltpu.VMEM((6, 256, 256), BF16),
        ] + work + [
            pltpu.VMEM((272, FULL), F32), pltpu.VMEM((208, FULL), F32), pltpu.VMEM((ROWS, WIDE), F32),
        ],
        psf_index, normed, ra, rb, ca, cb, *ready, name="main", room=20,
    )


def solution(mesh):
    placed = (
        P("row", "col"),
        P(),
        P("row", "col"),
        P("row", "col"),
        P("row", "col"),
        P(None, "row", "col"),
    )
    return jax.shard_map(
        per_device,
        mesh=mesh,
        in_specs=placed,
        out_specs=(P("row", "col"), P("row", "col")),
        check_vma=False,
    )
```

```python
import jax
import jax.numpy as jnp
from jax import lax
from jax.experimental import pallas as pl
from jax.experimental.pallas import tpu as pltpu
from jax.sharding import PartitionSpec as P

SIGMA = 0.15
TAU = 0.6
TV = 0.5
F32 = jnp.float32
BF16 = jnp.bfloat16

ROWS = 128
COLS = 512
XO = 80
YO = 64
WIDE = 640
FULL = 768
SEGS1 = ((0, 48, 64), (48, 128, 144), (176, 48, 64))
SEGS2 = ((0, 16, 32), (16, 128, 144), (144, 16, 32))
PATCHES2 = ((1,), (2, 3, 4, 5), (6, 7, 8, 9), (10, 11, 12, 13), (14, 15, 16, 17), (18,))
INNER = ((0, (3, 4, 5)), (1, (6, 7, 8, 9)), (2, (10, 11, 12, 13)), (3, (14, 15, 16)))
OUTER = ((-1, (0, 1)), (0, (2,)), (3, (17,)), (4, (18, 19)))
ALL = tuple((patch - 1, blocks) for patch, blocks in enumerate(PATCHES2))
SX, SXL, SC, SCL, SO, S1, S2, SM, STRIP = 0, 64, 80, 128, 144, 160, 192, 224, 240


def iota(shape, dim):
    return lax.broadcasted_iota(jnp.int32, shape, dim)


def split(value):
    hi = value.astype(BF16).astype(F32)
    return hi, value - hi


def lanes(value, shift):
    shift = shift % value.shape[1]
    return pltpu.roll(value, shift, 1) if shift else value


def rows(value, shift):
    shift = shift % value.shape[0]
    return pltpu.roll(value, shift, 0) if shift else value


def between(shape, lo, hi):
    lane = iota(shape, 1)
    return (lane >= lo) & (lane < hi)


def flags():
    row = lax.axis_index("row")
    col = lax.axis_index("col")
    return (
        row > 0,
        row < lax.axis_size("row") - 1,
        col > 0,
        col < lax.axis_size("col") - 1,
    )


def index_line(idx_ref, width):
    lane = iota((1, width), 1)
    line = jnp.zeros((1, width), F32)
    for j in range(4):
        line = jnp.where(lane == 1 + j, idx_ref[0:1, j : j + 1].astype(F32), line)
    return line


def parities():
    return lax.axis_index("row") % 2 == 1, lax.axis_index("col") % 2 == 1


def chosen(flag, one_ref, two_ref):
    def read(at):
        return jnp.where(flag, one_ref[at].astype(F32), two_ref[at].astype(F32))

    return read


def sides(a_ref, b_ref, odd):
    return chosen(odd, a_ref, b_ref), chosen(odd, b_ref, a_ref)


def pack_rows_kernel(x_hbm, y_hbm, o_hbm, q_hbm, idx_ref, a_ref, b_ref, x_ref, y_ref, o_ref, q_ref, sems):
    copies = [
        pltpu.make_async_copy(src, dst, sems.at[i])
        for i, (src, dst) in enumerate(((x_hbm, x_ref), (y_hbm, y_ref), (o_hbm, o_ref), (q_hbm, q_ref)))
    ]
    for copy in copies:
        copy.start()
    line = index_line(idx_ref, COLS)
    odd, _ = parities()

    def put(at, count, down, up):
        a_ref[at : at + count] = jnp.where(odd, up, down).astype(BF16)
        b_ref[at : at + count] = jnp.where(odd, down, up).astype(BF16)

    copies[0].wait()
    put(SX, 64, x_ref[64:128], x_ref[0:64])
    put(SXL, 16, split(x_ref[112:128])[1], split(x_ref[0:16])[1])
    copies[1].wait()
    copies[2].wait()
    up = y_ref[0:48] - SIGMA * o_ref[0:48]
    down = y_ref[80:128] - SIGMA * o_ref[80:128]
    put(SC, 48, down, up)
    put(SCL, 16, split(down[32:48])[1], split(up[0:16])[1])
    put(SO, 16, o_ref[112:128], o_ref[0:16])
    copies[3].wait()
    put(S1, 32, q_ref[0, 96:128], q_ref[0, 0:32])
    put(S2, 32, q_ref[1, 96:128], q_ref[1, 0:32])
    row = iota((16, COLS), 0)
    rest = []
    for edge in (127, 0):
        misc = jnp.zeros((16, COLS), F32)
        for comp in range(2):
            misc = jnp.where(row == comp, split(q_ref[comp, edge : edge + 1])[1], misc)
        rest.append(jnp.where(row == 2, line, misc))
    put(SM, 16, *rest)


def pack_cols_kernel(x_ref, y_ref, o_ref, q_ref, idx_ref, ra_ref, rb_ref, a_ref, b_ref):
    odd_row, odd_col = parities()
    top, bot = sides(ra_ref, rb_ref, odd_row)
    made = []
    for base in (384, 0):
        right = base > 0
        own = slice(base, base + 128)

        def strip(read, at, count, own=own):
            return read((slice(at, at + count), own))

        def column(middle, at, count, shift):
            parts = [strip(top, at, count), middle, strip(bot, at, count)]
            return lanes(jnp.concatenate(parts, axis=0), shift)

        seen = o_ref[:, own]
        x_hi, x_lo = split(x_ref[:, own])
        c_hi, c_lo = split(y_ref[:, own] - SIGMA * seen)
        zeros = jnp.zeros((128, 128), F32)
        buf = column(x_hi, SX, 64, 80)
        part = jnp.concatenate([column(c_hi, SC, 48, 0 if right else 16), zeros[:32]], axis=0)
        at = 80 if right else 16
        buf = jnp.where(between((256, 128), at, at + 48), part, buf)
        part = jnp.concatenate([column(seen, SO, 16, 16 if right else 64), zeros[:96]], axis=0)
        at = 0 if right else 64
        buf = jnp.where(between((256, 128), at, at + 16), part, buf)
        made.append(buf)
        buf = jnp.concatenate([column(q_ref[0, :, own], S1, 32, 80), zeros[:64]], axis=0)
        part = jnp.concatenate(
            [column(q_ref[1, :, own], S2, 32, 112 if right else 0), zeros[:64]], axis=0
        )
        at = 80 if right else 0
        buf = jnp.where(between((256, 128), at, at + 32), part, buf)
        shift = 0 if right else 32
        part = jnp.concatenate(
            [
                zeros[:48],
                lanes(strip(top, SXL, 16), shift),
                lanes(x_lo, shift),
                lanes(strip(bot, SXL, 16), shift),
                zeros[:48],
            ],
            axis=0,
        )
        at = 112 if right else 32
        buf = jnp.where(between((256, 128), at, at + 16), part, buf)
        shift = 16 if right else 64
        part = jnp.concatenate(
            [
                zeros[:32],
                lanes(strip(top, SCL, 16), shift),
                lanes(c_lo, shift),
                lanes(strip(bot, SCL, 16), shift),
                zeros[:64],
            ],
            axis=0,
        )
        at = 0 if right else 64
        buf = jnp.where(between((256, 128), at, at + 16), part, buf)
        if right:
            for comp in range(2):
                low = lanes(split(q_ref[comp, :, own])[1], 17 + comp)
                part = jnp.concatenate([zeros[:32], low, zeros[:96]], axis=0)
                buf = jnp.where(between((256, 128), 16 + comp, 17 + comp), part, buf)
        row = iota((256, 1), 0)
        spot = 4 if right else 1
        first = top((slice(SM, SM + 16), slice(0, 128)))[2:3, spot : spot + 1]
        last = bot((slice(SM, SM + 16), slice(0, 128)))[2:3, spot : spot + 1]
        mine = idx_ref[0:1, spot - 1 : spot].astype(F32)
        entry = jnp.where(row == 0, first, jnp.where(row == 1, mine, last))
        at = 18 if right else 112
        buf = jnp.where(between((256, 128), at, at + 1), entry, buf)
        made.append(buf)
    for tile in range(2):
        a_ref[tile] = jnp.where(odd_col, made[2 + tile], made[tile]).astype(BF16)
        b_ref[tile] = jnp.where(odd_col, made[tile], made[2 + tile]).astype(BF16)


def build_taps(tab_ref, t_ref, places):
    size = 8 * len(places)
    sub = iota((size, 128), 0)
    bits = [(sub // (1 << n)) % 2 == 1 for n in range(3)]
    for e in range(8):
        a1, half = e // 2, e % 2
        here = slice(128 * half, 128 * half + 128)
        skew = jnp.concatenate(
            [
                jnp.broadcast_to(
                    tab_ref[at : at + 1, 128 * e : 128 * e + 128], (8, 128)
                )
                for at in places
            ],
            axis=0,
        )
        for n in range(3):
            skew = jnp.where(bits[n], lanes(skew, 1 << n), skew)
        lower_all = [iota((size, 128), 1) % 32 <= sub % 8 + 8 * v for v in range(4)]
        low = [jnp.where(lower_all[v], lanes(skew, 8 * v - 31), 0.0) for v in range(4)]
        high = [jnp.where(lower_all[v], 0.0, lanes(skew, 8 * v + 1)) for v in range(4)]
        for patch in range(len(places)):
            own = slice(8 * patch, 8 * patch + 8)
            block = jnp.concatenate([part[own] for part in low + high], axis=0)
            t_ref[patch, 64 * a1 : 64 * a1 + 64, here] = block.astype(BF16)


def windows(get, p_ref, blocks, count):
    low = between((count, 128), 0, 64)
    tail = between((count, 128), 96, 128)
    for b in blocks:
        tile, place = b // 4, b % 4
        x0, x8 = get(tile, 0), get(tile, 8)
        if place == 0:
            part = jnp.where(low, x0, lanes(x8, 64))
        elif place == 1:
            part = jnp.where(low, lanes(x0, 96), lanes(x8, 32))
        elif place == 2:
            part = jnp.where(low, lanes(x0, 64), x8)
        else:
            w0 = jnp.where(tail, x0, get(tile + 1, 0))
            w8 = jnp.where(tail, x8, get(tile + 1, 8))
            part = jnp.where(low, lanes(w0, 32), lanes(w8, 96))
        p_ref[b, 0:count] = part.astype(BF16)


def blur(segs, groups, taps, p_ref, a_ref, put):
    present = [b for _, blocks in groups for b in blocks]
    for seg, (first, size, padded) in enumerate(segs):
        for patch, blocks in groups:
            lhs = jnp.concatenate(
                [
                    jnp.concatenate(
                        [
                            p_ref[b, first : first + padded],
                            p_ref[b, first + 16 : first + 16 + padded],
                        ],
                        axis=1,
                    )
                    for b in blocks
                ],
                axis=0,
            )
            v = jnp.dot(lhs, taps(seg, patch), preferred_element_type=F32)
            for place, b in enumerate(blocks):
                part = v[place * padded : place * padded + padded]
                a_ref[b, 0:padded] = part[:, :128] + rows(part[:, 128:], -4)
        low = between((padded, 128), 0, 64)
        even = iota((padded, 128), 1) % 64 < 32
        for tile in sorted({b // 4 for b in present}):
            a = [
                a_ref[4 * tile + p, 0:padded]
                if 4 * tile + p in present
                else jnp.zeros((padded, 128), F32)
                for p in range(4)
            ]
            e = []
            for p in range(2):
                z = lanes(jnp.where(low, a[p + 2], a[p]), 64)
                e.append(jnp.where(low, a[p], z) + rows(jnp.where(low, z, a[p + 2]), -2))
            m1 = jnp.where(even, e[0], lanes(e[1], 32))
            m2 = jnp.where(even, lanes(e[0], 96), e[1])
            blurred = (m1 + rows(m2, -1))[0:size]
            put(seg, first, size, tile, blurred)


def adjoint(segs, groups, taps, get, l_ref, f_ref, z_ref):
    present = [b for _, blocks in groups for b in blocks]
    tiles = sorted({b // 4 for b in present})
    for seg, (first, size, padded) in enumerate(segs):
        low = between((padded, 128), 0, 64)
        even = iota((padded, 128), 1) % 64 < 32
        for tile in tiles:
            o = jnp.concatenate(
                [get(first, size, tile), jnp.zeros((padded - size, 128), F32)], axis=0
            )
            o1 = rows(o, 1)
            e = [jnp.where(even, o, lanes(o1, 32)), jnp.where(even, lanes(o, 96), o1)]
            for p in range(2):
                s = rows(e[p], 2)
                for place in (p, p + 2):
                    b = 4 * tile + place
                    if b not in present:
                        continue
                    if place < 2:
                        part = jnp.where(low, e[p], lanes(s, 64))
                    else:
                        part = jnp.where(low, lanes(e[p], 64), s)
                    l_ref[b, 0:padded, 0:128] = part.astype(BF16)
                    l_ref[b, 0:padded, 128:256] = rows(part, 4).astype(BF16)
        for patch, blocks in groups:
            lhs = jnp.concatenate([l_ref[b, 0:padded] for b in blocks], axis=0)
            g = lax.dot_general(
                lhs, taps(seg, patch), (((1,), (1,)), ((), ())), preferred_element_type=F32
            )
            zero = jnp.zeros((16, 128), F32)
            for place, b in enumerate(blocks):
                part = g[place * padded : place * padded + padded]
                f_ref[b, 0 : padded + 16] = jnp.concatenate(
                    [part[:, :128], zero], axis=0
                ) + jnp.concatenate([zero, part[:, 128:]], axis=0)
        tall = padded + 24
        low = between((tall, 128), 0, 64)
        head = between((tall, 128), 0, 32)
        pad8 = jnp.zeros((8, 128), F32)

        def both_ways(b):
            if b not in present:
                zero = jnp.zeros((tall, 128), F32)
                return zero, zero
            f = f_ref[b, 0 : padded + 16]
            return jnp.concatenate([f, pad8], axis=0), jnp.concatenate([pad8, f], axis=0)

        for tile in tiles:
            both = []
            for p in range(2):
                a0, a8 = both_ways(4 * tile + p)
                b0, b8 = both_ways(4 * tile + p + 2)
                both.append(jnp.where(low, a0, b8) + lanes(jnp.where(low, b0, a8), 64))
            turned = lanes(both[1], 32)
            here = slice(128 * tile, 128 * tile + 128)
            after = slice(128 * tile + 128, 128 * tile + 256)
            span = slice(first, first + tall)
            z_ref[span, here] += both[0] + jnp.where(head, 0.0, turned)
            z_ref[span, after] += jnp.where(head, turned, 0.0)


def total_variation(get_x, get_q, q1_ref, q2_ref, chunks, place):
    row0, col0, limit_row, limit_col = place
    for chunk in chunks:
        start = 16 * chunk
        tall = get_x(start, 24)
        x = tall[0:16]
        below = rows(tall, -1)[0:16]
        right = lanes(x, -1)
        r = row0 - 32 + start + iota((16, WIDE), 0)
        c = col0 - XO + iota((16, WIDE), 1)
        g1 = jnp.where(r < limit_row, below - x, 0.0)
        g2 = jnp.where(c < limit_col, right - x, 0.0)
        span = slice(start, start + 16)
        u1 = get_q(0, start) + SIGMA * g1
        u2 = get_q(1, start) + SIGMA * g2
        shrink = jnp.maximum(1.0, jnp.sqrt(u1 * u1 + u2 * u2) / TV)
        inv = 1.0 / shrink
        q1_ref[span] = u1 * inv
        q2_ref[span] = u2 * inv


def divergence(q1_ref, q2_ref, start, place):
    row0, col0, limit_row, limit_col = place
    above = max(start - 8, 0)
    m1 = q1_ref[above : start + 16]
    m2 = q2_ref[start : start + 16]
    r = row0 - 32 + above + iota(m1.shape, 0)
    c = col0 - XO + iota((16, WIDE), 1)
    m1 = jnp.where((r >= 0) & (r < limit_row), m1, 0.0)
    m2 = jnp.where((c >= 0) & (c < limit_col), m2, 0.0)
    return (m1 - rows(m1, 1))[start - above :] + (m2 - lanes(m2, 1))


def places():
    row = lax.axis_index("row")
    col = lax.axis_index("col")
    return (
        row * ROWS,
        col * COLS,
        lax.axis_size("row") * ROWS - 1,
        lax.axis_size("col") * COLS - 1,
    )


def masks():
    top, bot, left, right = flags()

    def row_ok(seg):
        if seg == 1:
            return jnp.bool_(True)
        return top if seg == 0 else bot

    def col_ok(tile, size):
        lane = iota((size, 128), 1)
        if tile == 0:
            return (lane >= YO) | left
        if tile == 4:
            return (lane < YO) | right
        return jnp.ones((size, 128), jnp.bool_)

    return row_ok, col_ok


def widen(value, shift, width=WIDE):
    pad = jnp.zeros((value.shape[0], width - COLS), F32)
    return lanes(jnp.concatenate([value, pad], axis=1), shift)


def select_tables(table_ref, total, tab_ref):
    onehot = jnp.where(total == iota((64, 128), 0).astype(F32), 1.0, 0.0).astype(BF16)
    picked = lax.dot_general(
        onehot, table_ref[...], (((0,), (0,)), ((), ())), preferred_element_type=F32
    )
    tab_ref[...] = picked[0:24]


def tile_of(value, tile):
    return value[:, 128 * tile : 128 * tile + 128]


def local_kernel(
    x_ref, y_ref, o_ref, q_ref, idx_ref, table_ref,
    xw_ref, cw_ref, ow_ref, q1w_ref, q2w_ref, t_ref,
    tab_ref,
):
    select_tables(table_ref, index_line(idx_ref, 128), tab_ref)
    build_taps(tab_ref, t_ref, range(1, 5))
    xw_ref[...] = widen(x_ref[...], XO, FULL)
    seen = o_ref[...]
    cw_ref[...] = widen(y_ref[...] - SIGMA * seen, YO)
    ow_ref[...] = widen(seen, YO)
    q1w_ref[...] = widen(q_ref[0], XO)
    q2w_ref[...] = widen(q_ref[1], XO)


def middle_kernel(
    xw_ref, cw_ref, ow_ref, q1w_ref, q2w_ref, own_ref, table_ref, ra_ref, rb_ref,
    xe_ref, c_ref, ob_ref, ys_ref, q1_ref, q2_ref, z_ref, t_ref,
    tab_ref, p_ref, a_ref, l_ref, f_ref,
):
    top_ok, bot_ok, _, _ = flags()
    odd, _ = parities()
    top, bot = sides(ra_ref, rb_ref, odd)
    misc = slice(SM, SM + 16)
    lane = iota((1, 128), 1)
    upper = top((misc, slice(0, 128)))[2:3]
    lower = bot((misc, slice(0, 128)))[2:3]
    select_tables(table_ref, jnp.where(lane < 8, upper, lanes(lower, 8)), tab_ref)
    build_taps(tab_ref, t_ref, [1, 2, 3, 4, 9, 10, 11, 12])

    def part(read, at, count):
        return read(slice(at, at + count))

    zero = jnp.zeros((48, COLS), F32)
    above = part(top, SX, 64) + jnp.concatenate([zero, part(top, SXL, 16)], axis=0)
    below = part(bot, SX, 64) + jnp.concatenate([part(bot, SXL, 16), zero], axis=0)
    xe_ref[0:64] = widen(jnp.where(top_ok, above, 0.0), XO, FULL)
    xe_ref[64:192] = xw_ref[...]
    xe_ref[192:256] = widen(jnp.where(bot_ok, below, 0.0), XO, FULL)
    xe_ref[256:272] = jnp.zeros((16, FULL), F32)
    c_ref[48:176] = cw_ref[...]
    ob_ref[16:144] = ow_ref[...]
    zero = jnp.zeros((32, COLS), F32)
    above = part(top, SC, 48) + jnp.concatenate([zero, part(top, SCL, 16)], axis=0)
    below = part(bot, SC, 48) + jnp.concatenate([part(bot, SCL, 16), zero], axis=0)
    c_ref[0:48] = widen(above, YO)
    c_ref[176:224] = widen(below, YO)
    ob_ref[0:16] = widen(part(top, SO, 16), YO)
    ob_ref[144:160] = widen(part(bot, SO, 16), YO)
    rix = iota((32, COLS), 0)
    rest = top(misc)
    for comp, (ref, section, own) in enumerate(((q1_ref, S1, q1w_ref), (q2_ref, S2, q2w_ref))):
        above = part(top, section, 32) + jnp.where(rix == 31, rest[comp : comp + 1], 0.0)
        ref[0:32] = widen(above, XO)
        ref[32:160] = own[...]
        ref[160:192] = widen(part(bot, section, 32), XO)
    row_ok, _ = masks()

    def taps(seg, patch):
        return own_ref[patch] if seg == 1 else t_ref[2 * seg + patch]

    def get_x(tile, first):
        return xe_ref[first : first + 256, 128 * tile : 128 * tile + 128]

    def put(seg, first, size, tile, blurred):
        here = slice(128 * tile, 128 * tile + 128)
        new = (c_ref[first : first + size, here] + SIGMA * blurred) / (1.0 + SIGMA)
        ys_ref[first : first + size, here] = jnp.where(row_ok(seg), new, 0.0)

    def get_y(first, size, tile):
        return ys_ref[first : first + size, 128 * tile : 128 * tile + 128]

    windows(get_x, p_ref, range(3, 17), 256)
    blur(SEGS1, INNER, taps, p_ref, a_ref, put)
    z_ref[...] = jnp.zeros_like(z_ref)
    adjoint(SEGS1, INNER, taps, get_y, l_ref, f_ref, z_ref)


def main_kernel(
    table_ref, ca_ref, cb_ref,
    xi_ref, ci_ref, oi_ref, yi_ref, q1i_ref, q2i_ref, zi_ref, ti_ref, own_ref,
    x2_ref, y2_ref,
    side_ref, qs_ref, ys_ref, c_ref, q1_ref, q2_ref, tab_ref, t_ref, p_ref, a_ref, l_ref, f_ref,
    z_ref, xb_ref, x1_ref,
):
    top_ok, bot_ok, left_ok, right_ok = flags()
    place = places()
    _, odd_col = parities()
    before, after = sides(ca_ref, cb_ref, odd_col)
    lf0, lf1, rt0, rt1 = before(0), before(1), after(0), after(1)
    lane = iota((1, 128), 1)
    total = jnp.full((1, 128), -1.0, F32)
    for r in range(3):
        total = jnp.where(lane == 8 * r, lf1[r : r + 1, 18:19], total)
        total = jnp.where(lane == 8 * r + 5, rt1[r : r + 1, 112:113], total)
    select_tables(table_ref, total, tab_ref)
    build_taps(tab_ref, t_ref, [8 * r + p for r in range(3) for p in (0, 5)])

    def taps(seg, patch):
        if 0 <= patch < 4:
            return own_ref[patch] if seg == 1 else ti_ref[2 * seg + patch]
        return t_ref[2 * seg + (patch == 4)]

    rr = iota((256, 128), 0)
    rows_ok = ((rr >= 64) | top_ok) & ((rr < 192) | bot_ok)
    shape = (256, 128)
    part = jnp.where(between(shape, 16, 80), lf0, 0.0)
    part += jnp.where(between(shape, 64, 80), lanes(lf1, 80), 0.0)
    side_ref[0, 0:256] = xi_ref[0:256, 0:128] + jnp.where(rows_ok & left_ok, part, 0.0)
    part = jnp.where(between(shape, 80, 128), rt0, 0.0)
    part += jnp.where(between(shape, 80, 96), lanes(rt1, 48), 0.0)
    side_ref[1, 0:256] = xi_ref[0:256, 512:640] + jnp.where(rows_ok & right_ok, part, 0.0)
    part = jnp.where(between(shape, 0, 16), rt0, 0.0)
    side_ref[2, 0:256] = xi_ref[0:256, 640:768] + jnp.where(rows_ok & right_ok, part, 0.0)
    side_ref[:, 256:272] = jnp.zeros((3, 16, 128), F32)
    shape = (192, 128)
    for comp, ref in enumerate((q1i_ref, q2i_ref)):
        part = lanes(lf1[0:192], 96 * comp)
        part += jnp.where(between(shape, 79, 80), lanes(lf1[0:192], 63 - comp), 0.0)
        qs_ref[comp, 0] = jnp.where(between(shape, 48, 80), part, ref[:, 0:128])
        part = lanes(rt1[0:192], 80 * comp)
        qs_ref[comp, 1] = jnp.where(between(shape, 80, 112), part, ref[:, 512:640])
    shape = (224, 128)
    part = lanes(lf0[0:224], 64) + jnp.where(between(shape, 48, 64), lanes(lf1[0:224], 48), 0.0)
    c_first = jnp.where(between(shape, 16, 64), part, ci_ref[:, 0:128])
    part = lanes(rt0[0:224], 48) + jnp.where(between(shape, 64, 80), rt1[0:224], 0.0)
    c_last = jnp.where(between(shape, 64, 112), part, ci_ref[:, 512:640])
    shape = (160, 128)
    o_first = jnp.where(between(shape, 48, 64), lanes(lf0[0:160], 48), oi_ref[:, 0:128])
    o_last = jnp.where(between(shape, 64, 80), rt0[0:160], oi_ref[:, 512:640])
    row_ok, col_ok = masks()

    def get_side(tile, first):
        which = {0: 0, 4: 1, 5: 2}[tile]
        return side_ref[which, first : first + 256]

    def put_side(seg, first, size, tile, blurred):
        c = (c_first if tile == 0 else c_last)[first : first + size]
        new = (c + SIGMA * blurred) / (1.0 + SIGMA)
        new = jnp.where(col_ok(tile, size) & row_ok(seg), new, 0.0)
        old = yi_ref[first : first + size, 128 * tile : 128 * tile + 128]
        inner = between((size, 128), 96, 128) if tile == 0 else between((size, 128), 0, 32)
        ys_ref[tile // 4, first : first + size] = jnp.where(inner, old, new)

    def get_side_y(first, size, tile):
        return ys_ref[tile // 4, first : first + size]

    windows(get_side, p_ref, (0, 1, 2, 17, 18, 19), 256)
    blur(SEGS1, OUTER, taps, p_ref, a_ref, put_side)

    def get_x(start, count):
        at = slice(32 + start, 32 + start + count)
        return jnp.concatenate([side_ref[0, at], xi_ref[at, 128:512], side_ref[1, at]], axis=1)

    def get_q(comp, start):
        at = slice(start, start + 16)
        ref = q2i_ref if comp else q1i_ref
        return jnp.concatenate([qs_ref[comp, 0, at], ref[at, 128:512], qs_ref[comp, 1, at]], axis=1)

    total_variation(get_x, get_q, q1_ref, q2_ref, range(12), place)
    z_ref[...] = zi_ref[...]
    adjoint(SEGS1, OUTER, taps, get_side_y, l_ref, f_ref, z_ref)
    lane = iota((16, WIDE), 1)
    inside = ((lane >= XO) | left_ok) & ((lane < XO + COLS) | right_ok)
    for chunk in range(12):
        start = 16 * chunk
        ext = slice(32 + start, 48 + start)
        x = get_x(start, 16)
        new = x - TAU * (z_ref[ext, 0:WIDE] - divergence(q1_ref, q2_ref, start, place))
        keep = inside & (top_ok if chunk < 2 else bot_ok) if chunk < 2 or chunk >= 10 else inside
        xb_ref[start : start + 16, 0:WIDE] = jnp.where(keep, 2.0 * new - x, 0.0)
        if 2 <= chunk < 10:
            x1_ref[start - 32 : start - 16] = new
    xb_ref[192:208, 0:WIDE] = jnp.zeros((16, WIDE), F32)
    xb_ref[:, WIDE:FULL] = jnp.zeros((208, FULL - WIDE), F32)
    c_ref[:, 0:128] = ys_ref[0, 32:192] - SIGMA * o_first
    c_ref[:, 128:512] = yi_ref[32:192, 128:512] - SIGMA * oi_ref[:, 128:512]
    c_ref[:, 512:640] = ys_ref[1, 32:192] - SIGMA * o_last

    def get_xb(tile, first):
        return xb_ref[first : first + 192, 128 * tile : 128 * tile + 128]

    def put(seg, first, size, tile, blurred):
        here = slice(128 * tile, 128 * tile + 128)
        new = (c_ref[first : first + size, here] + SIGMA * blurred) / (1.0 + SIGMA)
        c_ref[first : first + size, here] = jnp.where(col_ok(tile, size) & row_ok(seg), new, 0.0)

    def get_y(first, size, tile):
        return c_ref[first : first + size, 128 * tile : 128 * tile + 128]

    windows(get_xb, p_ref, range(1, 19), 192)
    blur(SEGS2, ALL, taps, p_ref, a_ref, put)
    total_variation(
        lambda start, count: xb_ref[start : start + count, 0:WIDE],
        lambda comp, start: (q2_ref if comp else q1_ref)[start : start + 16],
        q1_ref, q2_ref, range(1, 10), place,
    )
    z_ref[...] = jnp.zeros_like(z_ref)
    adjoint(SEGS2, ALL, taps, get_y, l_ref, f_ref, z_ref)
    for chunk in range(8):
        span = slice(16 * chunk, 16 * chunk + 16)
        ext = slice(32 + 16 * chunk, 48 + 16 * chunk)
        div = divergence(q1_ref, q2_ref, 32 + 16 * chunk, place)
        new = x1_ref[span] - TAU * (z_ref[ext, 0:WIDE] - div)
        x2_ref[span] = lanes(new, -XO)[:, :COLS]
        y2_ref[span] = lanes(c_ref[16 + 16 * chunk : 32 + 16 * chunk], -YO)[:, :COLS]


def field(*shape, dtype=F32):
    return jax.ShapeDtypeStruct(shape, dtype)


def call(kernel, outs, scratch, *args, name, room=4, far=0, flops=0):
    spaces = [pltpu.HBM] * far + [pltpu.VMEM] * (len(args) - far)
    return pl.pallas_call(
        kernel,
        out_shape=outs,
        in_specs=[pl.BlockSpec(memory_space=space) for space in spaces],
        scratch_shapes=scratch,
        compiler_params=pltpu.CompilerParams(vmem_limit_bytes=room * 1024 * 1024),
        cost_estimate=pl.CostEstimate(flops=flops, bytes_accessed=0, transcendentals=0)
        if flops
        else None,
        name=name,
    )(*args)


def swap(block, axis, first):
    high, wide = lax.axis_size("row"), lax.axis_size("col")

    def partner(row, col):
        if axis == "row":
            to = ((row - first) ^ 1) + first
            return (to, col) if 0 <= to < high else (row, col ^ 2 if wide > 2 else col ^ 1)
        to = ((col - first) ^ 1) + first
        return (row, to) if 0 <= to < wide else (row ^ 1, col)

    pairs = []
    for row in range(high):
        for col in range(wide):
            to_row, to_col = partner(row, col)
            pairs.append((row * wide + col, to_row * wide + to_col))
    return lax.ppermute(block, ("row", "col"), pairs)


def per_device(observed, psf_table, psf_index, start_image, blur_dual, tv_dual):
    own = (start_image, blur_dual, observed, tv_dual)
    block = pltpu.VMEM((ROWS, COLS), F32)
    strip = field(STRIP, COLS, dtype=BF16)
    side = field(2, 256, 128, dtype=BF16)
    a, b = call(
        pack_rows_kernel, (strip, strip),
        [block, block, block, pltpu.VMEM((2, ROWS, COLS), F32), pltpu.SemaphoreType.DMA((4,))],
        *own, psf_index, name="pack_rows", far=4, room=62,
    )
    ra = swap(a, "row", 0)
    rb = swap(b, "row", 1)
    table = psf_table.astype(F32)
    normed = (table / jnp.sum(table, axis=(1, 2), keepdims=True)).astype(BF16)
    normed = jnp.pad(normed[:, :, ::-1], ((0, 0), (1, 0), (0, 1))).reshape(64, 1024)
    a, b = call(
        pack_cols_kernel, (side, side), [], *own, psf_index, ra, rb, name="pack_cols"
    )
    ca = swap(a, "col", 0)
    cb = swap(b, "col", 1)
    work = [
        pltpu.VMEM((20, 256, 128), BF16), pltpu.VMEM((20, 144, 128), F32),
        pltpu.VMEM((20, 144, 256), BF16), pltpu.VMEM((20, 160, 128), F32),
    ]
    wide = field(192, WIDE)
    local = field(ROWS, WIDE)
    *fields, taps = call(
        local_kernel,
        (field(ROWS, FULL), local, local, local, local, field(4, 256, 256, dtype=BF16)),
        [pltpu.VMEM((24, 1024), F32)],
        *own, psf_index, normed, name="local", room=4, flops=1 << 32,
    )
    ready = call(
        middle_kernel,
        (
            field(272, FULL), field(224, WIDE), field(160, WIDE), field(224, WIDE), wide, wide,
            field(272, FULL), field(8, 256, 256, dtype=BF16),
        ),
        [pltpu.VMEM((24, 1024), F32)] + work,
        *fields, taps, normed, ra, rb, name="middle", room=16, flops=1 << 33,
    )
    return call(
        main_kernel,
        (field(ROWS, COLS), field(ROWS, COLS)),
        [
            pltpu.VMEM((3, 272, 128), F32), pltpu.VMEM((2, 2, 192, 128), F32),
            pltpu.VMEM((2, 224, 128), F32), pltpu.VMEM((160, WIDE), F32),
            pltpu.VMEM((192, WIDE), F32), pltpu.VMEM((192, WIDE), F32),
            pltpu.VMEM((24, 1024), F32), pltpu.VMEM((6, 256, 256), BF16),
        ] + work + [
            pltpu.VMEM((272, FULL), F32), pltpu.VMEM((208, FULL), F32), pltpu.VMEM((ROWS, WIDE), F32),
        ],
        normed, ca, cb, *ready, taps, name="main", room=20,
    )


def solution(mesh):
    placed = (
        P("row", "col"),
        P(),
        P("row", "col"),
        P("row", "col"),
        P("row", "col"),
        P(None, "row", "col"),
    )
    return jax.shard_map(
        per_device,
        mesh=mesh,
        in_specs=placed,
        out_specs=(P("row", "col"), P("row", "col")),
        check_vma=False,
    )
```

```python
import jax
import jax.numpy as jnp
from jax import lax
from jax.experimental import pallas as pl
from jax.experimental.pallas import tpu as pltpu
from jax.sharding import PartitionSpec as P

SIGMA = 0.15
TAU = 0.6
TV = 0.5
F32 = jnp.float32
BF16 = jnp.bfloat16

ROWS = 128
COLS = 512
XO = 80
YO = 64
WIDE = 640
FULL = 768
SEGS1 = ((0, 48, 64), (48, 128, 144), (176, 48, 64))
SEGS2 = ((0, 16, 32), (16, 128, 144), (144, 16, 32))
PATCHES2 = ((1,), (2, 3, 4, 5), (6, 7, 8, 9), (10, 11, 12, 13), (14, 15, 16, 17), (18,))
INNER = ((0, (3, 4, 5)), (1, (6, 7, 8, 9)), (2, (10, 11, 12, 13)), (3, (14, 15, 16)))
OUTER = ((-1, (0, 1)), (0, (2,)), (3, (17,)), (4, (18, 19)))
ALL = tuple((patch - 1, blocks) for patch, blocks in enumerate(PATCHES2))
SX, SXL, SC, SCL, SO, S1, S2, SM, STRIP = 0, 64, 80, 128, 144, 160, 192, 224, 240


def iota(shape, dim):
    return lax.broadcasted_iota(jnp.int32, shape, dim)


def split(value):
    hi = value.astype(BF16).astype(F32)
    return hi, value - hi


def lanes(value, shift):
    shift = shift % value.shape[1]
    return pltpu.roll(value, shift, 1) if shift else value


def rows(value, shift):
    shift = shift % value.shape[0]
    return pltpu.roll(value, shift, 0) if shift else value


def between(shape, lo, hi):
    lane = iota(shape, 1)
    return (lane >= lo) & (lane < hi)


def flags():
    row = lax.axis_index("row")
    col = lax.axis_index("col")
    return (
        row > 0,
        row < lax.axis_size("row") - 1,
        col > 0,
        col < lax.axis_size("col") - 1,
    )


def index_line(idx_ref, width):
    lane = iota((1, width), 1)
    line = jnp.zeros((1, width), F32)
    for j in range(4):
        line = jnp.where(lane == 1 + j, idx_ref[0:1, j : j + 1].astype(F32), line)
    return line


def parities():
    return lax.axis_index("row") % 2 == 1, lax.axis_index("col") % 2 == 1


def chosen(flag, one_ref, two_ref):
    def read(at):
        return jnp.where(flag, one_ref[at].astype(F32), two_ref[at].astype(F32))

    return read


def sides(a_ref, b_ref, odd):
    return chosen(odd, a_ref, b_ref), chosen(odd, b_ref, a_ref)


def pack_rows_kernel(x_hbm, y_hbm, o_hbm, q_hbm, idx_ref, a_ref, b_ref, x_ref, y_ref, o_ref, q_ref, sems):
    copies = [
        pltpu.make_async_copy(src, dst, sems.at[i])
        for i, (src, dst) in enumerate(((x_hbm, x_ref), (y_hbm, y_ref), (o_hbm, o_ref), (q_hbm, q_ref)))
    ]
    for copy in copies:
        copy.start()
    line = index_line(idx_ref, COLS)
    odd, _ = parities()

    def put(at, count, down, up):
        a_ref[at : at + count] = jnp.where(odd, up, down).astype(BF16)
        b_ref[at : at + count] = jnp.where(odd, down, up).astype(BF16)

    copies[0].wait()
    put(SX, 64, x_ref[64:128], x_ref[0:64])
    put(SXL, 16, split(x_ref[112:128])[1], split(x_ref[0:16])[1])
    copies[1].wait()
    copies[2].wait()
    up = y_ref[0:48] - SIGMA * o_ref[0:48]
    down = y_ref[80:128] - SIGMA * o_ref[80:128]
    put(SC, 48, down, up)
    put(SCL, 16, split(down[32:48])[1], split(up[0:16])[1])
    put(SO, 16, o_ref[112:128], o_ref[0:16])
    copies[3].wait()
    put(S1, 32, q_ref[0, 96:128], q_ref[0, 0:32])
    put(S2, 32, q_ref[1, 96:128], q_ref[1, 0:32])
    row = iota((16, COLS), 0)
    rest = []
    for edge in (127, 0):
        misc = jnp.zeros((16, COLS), F32)
        for comp in range(2):
            misc = jnp.where(row == comp, split(q_ref[comp, edge : edge + 1])[1], misc)
        rest.append(jnp.where(row == 2, line, misc))
    put(SM, 16, *rest)


def pack_cols_kernel(x_ref, y_ref, o_ref, q_ref, idx_ref, ra_ref, rb_ref, a_ref, b_ref):
    odd_row, odd_col = parities()
    top, bot = sides(ra_ref, rb_ref, odd_row)
    made = []
    for base in (384, 0):
        right = base > 0
        own = slice(base, base + 128)

        def strip(read, at, count, own=own):
            return read((slice(at, at + count), own))

        def column(middle, at, count, shift):
            parts = [strip(top, at, count), middle, strip(bot, at, count)]
            return lanes(jnp.concatenate(parts, axis=0), shift)

        seen = o_ref[:, own]
        x_hi, x_lo = split(x_ref[:, own])
        c_hi, c_lo = split(y_ref[:, own] - SIGMA * seen)
        zeros = jnp.zeros((128, 128), F32)
        buf = column(x_hi, SX, 64, 80)
        part = jnp.concatenate([column(c_hi, SC, 48, 0 if right else 16), zeros[:32]], axis=0)
        at = 80 if right else 16
        buf = jnp.where(between((256, 128), at, at + 48), part, buf)
        part = jnp.concatenate([column(seen, SO, 16, 16 if right else 64), zeros[:96]], axis=0)
        at = 0 if right else 64
        buf = jnp.where(between((256, 128), at, at + 16), part, buf)
        made.append(buf)
        buf = jnp.concatenate([column(q_ref[0, :, own], S1, 32, 80), zeros[:64]], axis=0)
        part = jnp.concatenate(
            [column(q_ref[1, :, own], S2, 32, 112 if right else 0), zeros[:64]], axis=0
        )
        at = 80 if right else 0
        buf = jnp.where(between((256, 128), at, at + 32), part, buf)
        shift = 0 if right else 32
        part = jnp.concatenate(
            [
                zeros[:48],
                lanes(strip(top, SXL, 16), shift),
                lanes(x_lo, shift),
                lanes(strip(bot, SXL, 16), shift),
                zeros[:48],
            ],
            axis=0,
        )
        at = 112 if right else 32
        buf = jnp.where(between((256, 128), at, at + 16), part, buf)
        shift = 16 if right else 64
        part = jnp.concatenate(
            [
                zeros[:32],
                lanes(strip(top, SCL, 16), shift),
                lanes(c_lo, shift),
                lanes(strip(bot, SCL, 16), shift),
                zeros[:64],
            ],
            axis=0,
        )
        at = 0 if right else 64
        buf = jnp.where(between((256, 128), at, at + 16), part, buf)
        if right:
            for comp in range(2):
                low = lanes(split(q_ref[comp, :, own])[1], 17 + comp)
                part = jnp.concatenate([zeros[:32], low, zeros[:96]], axis=0)
                buf = jnp.where(between((256, 128), 16 + comp, 17 + comp), part, buf)
        row = iota((256, 1), 0)
        spot = 4 if right else 1
        first = top((slice(SM, SM + 16), slice(0, 128)))[2:3, spot : spot + 1]
        last = bot((slice(SM, SM + 16), slice(0, 128)))[2:3, spot : spot + 1]
        mine = idx_ref[0:1, spot - 1 : spot].astype(F32)
        entry = jnp.where(row == 0, first, jnp.where(row == 1, mine, last))
        at = 18 if right else 112
        buf = jnp.where(between((256, 128), at, at + 1), entry, buf)
        made.append(buf)
    for tile in range(2):
        a_ref[tile] = jnp.where(odd_col, made[2 + tile], made[tile]).astype(BF16)
        b_ref[tile] = jnp.where(odd_col, made[tile], made[2 + tile]).astype(BF16)


def build_taps(tab_ref, t_ref, places):
    size = 8 * len(places)
    sub = iota((size, 128), 0)
    bits = [(sub // (1 << n)) % 2 == 1 for n in range(3)]
    for e in range(8):
        a1, half = 2 * (e // 4) + e % 2, e // 2 % 2
        here = slice(128 * half, 128 * half + 128)
        skew = jnp.concatenate(
            [
                jnp.broadcast_to(
                    tab_ref[at : at + 1, 128 * e : 128 * e + 128], (8, 128)
                )
                for at in places
            ],
            axis=0,
        )
        for n in range(3):
            skew = jnp.where(bits[n], lanes(skew, 1 << n), skew)
        lower_all = [iota((size, 128), 1) % 32 <= sub % 8 + 8 * v for v in range(4)]
        low = [jnp.where(lower_all[v], lanes(skew, 8 * v - 31), 0.0) for v in range(4)]
        high = [jnp.where(lower_all[v], 0.0, lanes(skew, 8 * v + 1)) for v in range(4)]
        for patch in range(len(places)):
            own = slice(8 * patch, 8 * patch + 8)
            block = jnp.concatenate([part[own] for part in low + high], axis=0)
            t_ref[patch, 64 * a1 : 64 * a1 + 64, here] = block.astype(BF16)


def windows(get, p_ref, blocks, count):
    low = between((count, 128), 0, 64)
    tail = between((count, 128), 96, 128)
    for b in blocks:
        tile, place = b // 4, b % 4
        x0, x4 = get(tile, 0), get(tile, 4)
        if place == 0:
            part = jnp.where(low, x0, lanes(x4, 64))
        elif place == 1:
            part = jnp.where(low, lanes(x0, 96), lanes(x4, 32))
        elif place == 2:
            part = jnp.where(low, lanes(x0, 64), x4)
        else:
            w0 = jnp.where(tail, x0, get(tile + 1, 0))
            w4 = jnp.where(tail, x4, get(tile + 1, 4))
            part = jnp.where(low, lanes(w0, 32), lanes(w4, 96))
        p_ref[b, 0:count] = part.astype(BF16)


def blur(segs, groups, taps, p_ref, a_ref, put):
    present = [b for _, blocks in groups for b in blocks]
    for seg, (first, size, padded) in enumerate(segs):
        for patch, blocks in groups:
            lhs = jnp.concatenate(
                [
                    jnp.concatenate(
                        [
                            p_ref[b, first : first + padded],
                            p_ref[b, first + 16 : first + 16 + padded],
                        ],
                        axis=1,
                    )
                    for b in blocks
                ],
                axis=0,
            )
            v = jnp.dot(lhs, taps(seg, patch), preferred_element_type=F32)
            for place, b in enumerate(blocks):
                part = v[place * padded : place * padded + padded]
                a_ref[b, 0:padded] = part[:, :128] + rows(part[:, 128:], -8)
        low = between((padded, 128), 0, 64)
        even = iota((padded, 128), 1) % 64 < 32
        for tile in sorted({b // 4 for b in present}):
            a = [
                a_ref[4 * tile + p, 0:padded]
                if 4 * tile + p in present
                else jnp.zeros((padded, 128), F32)
                for p in range(4)
            ]
            e = []
            for p in range(2):
                z = lanes(jnp.where(low, a[p + 2], a[p]), 64)
                e.append(jnp.where(low, a[p], z) + rows(jnp.where(low, z, a[p + 2]), -2))
            m1 = jnp.where(even, e[0], lanes(e[1], 32))
            m2 = jnp.where(even, lanes(e[0], 96), e[1])
            blurred = (m1 + rows(m2, -1))[0:size]
            put(seg, first, size, tile, blurred)


def adjoint(segs, groups, taps, get, l_ref, f_ref, z_ref):
    present = [b for _, blocks in groups for b in blocks]
    tiles = sorted({b // 4 for b in present})
    for seg, (first, size, padded) in enumerate(segs):
        low = between((padded, 128), 0, 64)
        even = iota((padded, 128), 1) % 64 < 32
        for tile in tiles:
            o = jnp.concatenate(
                [get(first, size, tile), jnp.zeros((padded - size, 128), F32)], axis=0
            )
            o1 = rows(o, 1)
            e = [jnp.where(even, o, lanes(o1, 32)), jnp.where(even, lanes(o, 96), o1)]
            for p in range(2):
                s = rows(e[p], 2)
                for place in (p, p + 2):
                    b = 4 * tile + place
                    if b not in present:
                        continue
                    if place < 2:
                        part = jnp.where(low, e[p], lanes(s, 64))
                    else:
                        part = jnp.where(low, lanes(e[p], 64), s)
                    l_ref[b, 0:padded, 0:128] = part.astype(BF16)
                    l_ref[b, 0:padded, 128:256] = rows(part, 8).astype(BF16)
        for patch, blocks in groups:
            lhs = jnp.concatenate([l_ref[b, 0:padded] for b in blocks], axis=0)
            g = lax.dot_general(
                lhs, taps(seg, patch), (((1,), (1,)), ((), ())), preferred_element_type=F32
            )
            zero = jnp.zeros((16, 128), F32)
            for place, b in enumerate(blocks):
                part = g[place * padded : place * padded + padded]
                f_ref[b, 0:8] = zero[0:8]
                f_ref[b, 8 : padded + 24] = jnp.concatenate(
                    [part[:, :128], zero], axis=0
                ) + jnp.concatenate([zero, part[:, 128:]], axis=0)
                f_ref[b, padded + 24 : padded + 32] = zero[0:8]
        tall = padded + 24
        low = between((tall, 128), 0, 64)
        head = between((tall, 128), 0, 32)

        def both_ways(b):
            if b not in present:
                zero = jnp.zeros((tall, 128), F32)
                return zero, zero
            return f_ref[b, 8 : 8 + tall], f_ref[b, 4 : 4 + tall]

        for tile in tiles:
            both = []
            for p in range(2):
                a0, a8 = both_ways(4 * tile + p)
                b0, b8 = both_ways(4 * tile + p + 2)
                both.append(jnp.where(low, a0, b8) + lanes(jnp.where(low, b0, a8), 64))
            turned = lanes(both[1], 32)
            here = slice(128 * tile, 128 * tile + 128)
            after = slice(128 * tile + 128, 128 * tile + 256)
            span = slice(first, first + tall)
            z_ref[span, here] += both[0] + jnp.where(head, 0.0, turned)
            z_ref[span, after] += jnp.where(head, turned, 0.0)


def on_tile(value, tile, change):
    parts = [value[:, 128 * k : 128 * k + 128] for k in range(5)]
    parts[tile] = change(parts[tile])
    return jnp.concatenate(parts, axis=1)


def unless(bad, value):
    return jnp.where(bad, 0.0, value)


def total_variation(get_x, get_q, q1_ref, q2_ref, chunks):
    _, bot_ok, _, right_ok = flags()
    lane = iota((16, 128), 1)
    past = (lane + 512 - XO >= COLS - 1) & jnp.logical_not(right_ok)
    for chunk in chunks:
        start = 16 * chunk
        tall = get_x(start, 24)
        x = tall[0:16]
        g1 = rows(tall, -1)[0:16] - x
        g2 = on_tile(lanes(x, -1) - x, 4, lambda part: unless(past, part))
        if start + 16 > 31 + ROWS:
            row = start - 32 + iota((16, WIDE), 0)
            g1 = unless((row >= ROWS - 1) & jnp.logical_not(bot_ok), g1)
        span = slice(start, start + 16)
        u1 = get_q(0, start) + SIGMA * g1
        u2 = get_q(1, start) + SIGMA * g2
        scale = jnp.minimum(1.0, TV * lax.rsqrt(u1 * u1 + u2 * u2))
        q1_ref[span] = u1 * scale
        q2_ref[span] = u2 * scale


def divergence(q1_ref, q2_ref, start):
    top_ok, bot_ok, left_ok, right_ok = flags()
    above = max(start - 8, 0)
    m1 = q1_ref[above : start + 16]
    m2 = q2_ref[start : start + 16]
    row = above - 32 + iota(m1.shape, 0)
    if above < 32:
        m1 = unless((row < 0) & jnp.logical_not(top_ok), m1)
    if start + 16 > 31 + ROWS:
        m1 = unless((row >= ROWS - 1) & jnp.logical_not(bot_ok), m1)
    lane = iota((16, 128), 1)
    m2 = on_tile(m2, 0, lambda part: unless((lane < XO) & jnp.logical_not(left_ok), part))
    past = (lane + 512 - XO >= COLS - 1) & jnp.logical_not(right_ok)
    m2 = on_tile(m2, 4, lambda part: unless(past, part))
    return (m1 - rows(m1, 1))[start - above :] + (m2 - lanes(m2, 1))


def masks():
    top, bot, left, right = flags()

    def row_ok(seg):
        if seg == 1:
            return jnp.bool_(True)
        return top if seg == 0 else bot

    def col_ok(tile, size):
        lane = iota((size, 128), 1)
        if tile == 0:
            return (lane >= YO) | left
        if tile == 4:
            return (lane < YO) | right
        return jnp.ones((size, 128), jnp.bool_)

    return row_ok, col_ok


def widen(value, shift, width=WIDE):
    pad = jnp.zeros((value.shape[0], width - COLS), F32)
    return lanes(jnp.concatenate([value, pad], axis=1), shift)


def select_tables(table_ref, total, tab_ref):
    onehot = jnp.where(total == iota((64, 128), 0).astype(F32), 1.0, 0.0).astype(BF16)
    picked = lax.dot_general(
        onehot, table_ref[...], (((0,), (0,)), ((), ())), preferred_element_type=F32
    )
    tab_ref[...] = picked[0:24]


def tile_of(value, tile):
    return value[:, 128 * tile : 128 * tile + 128]


def local_kernel(
    x_ref, y_ref, o_ref, q_ref, idx_ref, table_ref,
    xw_ref, cw_ref, ow_ref, q1w_ref, q2w_ref, t_ref,
    tab_ref,
):
    select_tables(table_ref, index_line(idx_ref, 128), tab_ref)
    build_taps(tab_ref, t_ref, range(1, 5))
    xw_ref[...] = widen(x_ref[...], XO, FULL)
    seen = o_ref[...]
    cw_ref[...] = widen(y_ref[...] - SIGMA * seen, YO)
    ow_ref[...] = widen(seen, YO)
    q1w_ref[...] = widen(q_ref[0], XO)
    q2w_ref[...] = widen(q_ref[1], XO)


def middle_kernel(
    xw_ref, cw_ref, ow_ref, q1w_ref, q2w_ref, own_ref, table_ref, ra_ref, rb_ref,
    xe_ref, c_ref, ob_ref, ys_ref, q1_ref, q2_ref, z_ref, t_ref,
    tab_ref, p_ref, a_ref, l_ref, f_ref,
):
    top_ok, bot_ok, _, _ = flags()
    odd, _ = parities()
    top, bot = sides(ra_ref, rb_ref, odd)
    misc = slice(SM, SM + 16)
    lane = iota((1, 128), 1)
    upper = top((misc, slice(0, 128)))[2:3]
    lower = bot((misc, slice(0, 128)))[2:3]
    select_tables(table_ref, jnp.where(lane < 8, upper, lanes(lower, 8)), tab_ref)
    build_taps(tab_ref, t_ref, [1, 2, 3, 4, 9, 10, 11, 12])

    def part(read, at, count):
        return read(slice(at, at + count))

    zero = jnp.zeros((48, COLS), F32)
    above = part(top, SX, 64) + jnp.concatenate([zero, part(top, SXL, 16)], axis=0)
    below = part(bot, SX, 64) + jnp.concatenate([part(bot, SXL, 16), zero], axis=0)
    xe_ref[0:64] = widen(jnp.where(top_ok, above, 0.0), XO, FULL)
    xe_ref[64:192] = xw_ref[...]
    xe_ref[192:256] = widen(jnp.where(bot_ok, below, 0.0), XO, FULL)
    xe_ref[256:272] = jnp.zeros((16, FULL), F32)
    c_ref[48:176] = cw_ref[...]
    ob_ref[16:144] = ow_ref[...]
    zero = jnp.zeros((32, COLS), F32)
    above = part(top, SC, 48) + jnp.concatenate([zero, part(top, SCL, 16)], axis=0)
    below = part(bot, SC, 48) + jnp.concatenate([part(bot, SCL, 16), zero], axis=0)
    c_ref[0:48] = widen(above, YO)
    c_ref[176:224] = widen(below, YO)
    ob_ref[0:16] = widen(part(top, SO, 16), YO)
    ob_ref[144:160] = widen(part(bot, SO, 16), YO)
    rix = iota((32, COLS), 0)
    rest = top(misc)
    for comp, (ref, section, own) in enumerate(((q1_ref, S1, q1w_ref), (q2_ref, S2, q2w_ref))):
        above = part(top, section, 32) + jnp.where(rix == 31, rest[comp : comp + 1], 0.0)
        ref[0:32] = widen(above, XO)
        ref[32:160] = own[...]
        ref[160:192] = widen(part(bot, section, 32), XO)
    row_ok, _ = masks()

    def taps(seg, patch):
        return own_ref[patch] if seg == 1 else t_ref[2 * seg + patch]

    def get_x(tile, first):
        return xe_ref[first : first + 256, 128 * tile : 128 * tile + 128]

    def put(seg, first, size, tile, blurred):
        here = slice(128 * tile, 128 * tile + 128)
        new = (c_ref[first : first + size, here] + SIGMA * blurred) * (1.0 / (1.0 + SIGMA))
        ys_ref[first : first + size, here] = new if seg == 1 else jnp.where(row_ok(seg), new, 0.0)

    def get_y(first, size, tile):
        return ys_ref[first : first + size, 128 * tile : 128 * tile + 128]

    windows(get_x, p_ref, range(3, 17), 256)
    blur(SEGS1, INNER, taps, p_ref, a_ref, put)
    z_ref[...] = jnp.zeros_like(z_ref)
    adjoint(SEGS1, INNER, taps, get_y, l_ref, f_ref, z_ref)


def main_kernel(
    table_ref, ca_ref, cb_ref,
    xi_ref, ci_ref, oi_ref, yi_ref, q1i_ref, q2i_ref, zi_ref, ti_ref, own_ref,
    x2_ref, y2_hbm,
    side_ref, qs_ref, ys_ref, c_ref, q1_ref, q2_ref, tab_ref, t_ref, p_ref, a_ref, l_ref, f_ref,
    z_ref, xb_ref, x1_ref, y2_ref, sem,
):
    top_ok, bot_ok, left_ok, right_ok = flags()
    _, odd_col = parities()
    before, after = sides(ca_ref, cb_ref, odd_col)
    lf0, lf1, rt0, rt1 = before(0), before(1), after(0), after(1)
    lane = iota((1, 128), 1)
    total = jnp.full((1, 128), -1.0, F32)
    for r in range(3):
        total = jnp.where(lane == 8 * r, lf1[r : r + 1, 18:19], total)
        total = jnp.where(lane == 8 * r + 5, rt1[r : r + 1, 112:113], total)
    select_tables(table_ref, total, tab_ref)
    build_taps(tab_ref, t_ref, [8 * r + p for r in range(3) for p in (0, 5)])

    def taps(seg, patch):
        if 0 <= patch < 4:
            return own_ref[patch] if seg == 1 else ti_ref[2 * seg + patch]
        return t_ref[2 * seg + (patch == 4)]

    rr = iota((256, 128), 0)
    rows_ok = ((rr >= 64) | top_ok) & ((rr < 192) | bot_ok)
    shape = (256, 128)
    part = jnp.where(between(shape, 16, 80), lf0, 0.0)
    part += jnp.where(between(shape, 64, 80), lanes(lf1, 80), 0.0)
    side_ref[0, 0:256] = xi_ref[0:256, 0:128] + jnp.where(rows_ok & left_ok, part, 0.0)
    part = jnp.where(between(shape, 80, 128), rt0, 0.0)
    part += jnp.where(between(shape, 80, 96), lanes(rt1, 48), 0.0)
    side_ref[1, 0:256] = xi_ref[0:256, 512:640] + jnp.where(rows_ok & right_ok, part, 0.0)
    part = jnp.where(between(shape, 0, 16), rt0, 0.0)
    side_ref[2, 0:256] = xi_ref[0:256, 640:768] + jnp.where(rows_ok & right_ok, part, 0.0)
    side_ref[:, 256:272] = jnp.zeros((3, 16, 128), F32)
    shape = (192, 128)
    for comp, ref in enumerate((q1i_ref, q2i_ref)):
        part = lanes(lf1[0:192], 96 * comp)
        part += jnp.where(between(shape, 79, 80), lanes(lf1[0:192], 63 - comp), 0.0)
        qs_ref[comp, 0] = jnp.where(between(shape, 48, 80), part, ref[:, 0:128])
        part = lanes(rt1[0:192], 80 * comp)
        qs_ref[comp, 1] = jnp.where(between(shape, 80, 112), part, ref[:, 512:640])
    shape = (224, 128)
    part = lanes(lf0[0:224], 64) + jnp.where(between(shape, 48, 64), lanes(lf1[0:224], 48), 0.0)
    c_first = jnp.where(between(shape, 16, 64), part, ci_ref[:, 0:128])
    part = lanes(rt0[0:224], 48) + jnp.where(between(shape, 64, 80), rt1[0:224], 0.0)
    c_last = jnp.where(between(shape, 64, 112), part, ci_ref[:, 512:640])
    shape = (160, 128)
    o_first = jnp.where(between(shape, 48, 64), lanes(lf0[0:160], 48), oi_ref[:, 0:128])
    o_last = jnp.where(between(shape, 64, 80), rt0[0:160], oi_ref[:, 512:640])
    row_ok, col_ok = masks()

    def get_side(tile, first):
        which = {0: 0, 4: 1, 5: 2}[tile]
        return side_ref[which, first : first + 256]

    def put_side(seg, first, size, tile, blurred):
        c = (c_first if tile == 0 else c_last)[first : first + size]
        new = (c + SIGMA * blurred) * (1.0 / (1.0 + SIGMA))
        new = jnp.where(col_ok(tile, size) & row_ok(seg), new, 0.0)
        old = yi_ref[first : first + size, 128 * tile : 128 * tile + 128]
        inner = between((size, 128), 96, 128) if tile == 0 else between((size, 128), 0, 32)
        ys_ref[tile // 4, first : first + size] = jnp.where(inner, old, new)

    def get_side_y(first, size, tile):
        return ys_ref[tile // 4, first : first + size]

    windows(get_side, p_ref, (0, 1, 2, 17, 18, 19), 256)
    blur(SEGS1, OUTER, taps, p_ref, a_ref, put_side)

    def get_x(start, count):
        at = slice(32 + start, 32 + start + count)
        return jnp.concatenate([side_ref[0, at], xi_ref[at, 128:512], side_ref[1, at]], axis=1)

    def get_q(comp, start):
        at = slice(start, start + 16)
        ref = q2i_ref if comp else q1i_ref
        return jnp.concatenate([qs_ref[comp, 0, at], ref[at, 128:512], qs_ref[comp, 1, at]], axis=1)

    total_variation(get_x, get_q, q1_ref, q2_ref, range(12))
    z_ref[...] = zi_ref[...]
    adjoint(SEGS1, OUTER, taps, get_side_y, l_ref, f_ref, z_ref)
    lane = iota((16, 128), 1)
    for chunk in range(12):
        start = 16 * chunk
        ext = slice(32 + start, 48 + start)
        x = get_x(start, 16)
        new = x - TAU * (z_ref[ext, 0:WIDE] - divergence(q1_ref, q2_ref, start))
        ahead = 2.0 * new - x
        ahead = on_tile(ahead, 0, lambda part: unless((lane < XO) & jnp.logical_not(left_ok), part))
        past = (lane + 512 - XO >= COLS) & jnp.logical_not(right_ok)
        ahead = on_tile(ahead, 4, lambda part: unless(past, part))
        if chunk < 2 or chunk >= 10:
            ahead = jnp.where(top_ok if chunk < 2 else bot_ok, ahead, 0.0)
        xb_ref[start : start + 16, 0:WIDE] = ahead
        if 2 <= chunk < 10:
            x1_ref[start - 32 : start - 16] = new
    xb_ref[192:208, 0:WIDE] = jnp.zeros((16, WIDE), F32)
    xb_ref[:, WIDE:FULL] = jnp.zeros((208, FULL - WIDE), F32)
    c_ref[:, 0:128] = ys_ref[0, 32:192] - SIGMA * o_first
    c_ref[:, 128:512] = yi_ref[32:192, 128:512] - SIGMA * oi_ref[:, 128:512]
    c_ref[:, 512:640] = ys_ref[1, 32:192] - SIGMA * o_last

    def get_xb(tile, first):
        return xb_ref[first : first + 192, 128 * tile : 128 * tile + 128]

    def put(seg, first, size, tile, blurred):
        here = slice(128 * tile, 128 * tile + 128)
        new = (c_ref[first : first + size, here] + SIGMA * blurred) * (1.0 / (1.0 + SIGMA))
        if seg != 1 or tile in (0, 4):
            new = jnp.where(col_ok(tile, size) & row_ok(seg), new, 0.0)
        c_ref[first : first + size, here] = new

    def get_y(first, size, tile):
        return c_ref[first : first + size, 128 * tile : 128 * tile + 128]

    windows(get_xb, p_ref, range(1, 19), 192)
    blur(SEGS2, ALL, taps, p_ref, a_ref, put)
    for chunk in range(8):
        span = slice(16 * chunk, 16 * chunk + 16)
        y2_ref[span] = lanes(c_ref[16 + 16 * chunk : 32 + 16 * chunk], -YO)[:, :COLS]
    total_variation(
        lambda start, count: xb_ref[start : start + count, 0:WIDE],
        lambda comp, start: (q2_ref if comp else q1_ref)[start : start + 16],
        q1_ref, q2_ref, range(1, 10),
    )
    done = pltpu.make_async_copy(y2_ref, y2_hbm, sem.at[0])
    done.start()
    z_ref[...] = jnp.zeros_like(z_ref)
    adjoint(SEGS2, ALL, taps, get_y, l_ref, f_ref, z_ref)
    for chunk in range(8):
        span = slice(16 * chunk, 16 * chunk + 16)
        ext = slice(32 + 16 * chunk, 48 + 16 * chunk)
        div = divergence(q1_ref, q2_ref, 32 + 16 * chunk)
        new = x1_ref[span] - TAU * (z_ref[ext, 0:WIDE] - div)
        x2_ref[span] = lanes(new, -XO)[:, :COLS]
    done.wait()


def field(*shape, dtype=F32):
    return jax.ShapeDtypeStruct(shape, dtype)


def call(kernel, outs, scratch, *args, name, room=4, far=0, flops=0, out_far=0):
    spaces = [pltpu.HBM] * far + [pltpu.VMEM] * (len(args) - far)
    return pl.pallas_call(
        kernel,
        out_shape=outs,
        out_specs=tuple(
            pl.BlockSpec(memory_space=pltpu.HBM if i >= len(outs) - out_far else pltpu.VMEM)
            for i in range(len(outs))
        ),
        in_specs=[pl.BlockSpec(memory_space=space) for space in spaces],
        scratch_shapes=scratch,
        compiler_params=pltpu.CompilerParams(vmem_limit_bytes=int(room * 1024 * 1024)),
        cost_estimate=pl.CostEstimate(flops=flops, bytes_accessed=0, transcendentals=0)
        if flops
        else None,
        name=name,
    )(*args)


def swap(block, axis, first):
    high, wide = lax.axis_size("row"), lax.axis_size("col")

    def partner(row, col):
        if axis == "row":
            to = ((row - first) ^ 1) + first
            return (to, col) if 0 <= to < high else (row, col ^ 2 if wide > 2 else col ^ 1)
        to = ((col - first) ^ 1) + first
        return (row, to) if 0 <= to < wide else (row ^ 1, col)

    pairs = []
    for row in range(high):
        for col in range(wide):
            to_row, to_col = partner(row, col)
            pairs.append((row * wide + col, to_row * wide + to_col))
    return lax.ppermute(block, ("row", "col"), pairs)


def per_device(observed, psf_table, psf_index, start_image, blur_dual, tv_dual):
    own = (start_image, blur_dual, observed, tv_dual)
    block = pltpu.VMEM((ROWS, COLS), F32)
    strip = field(STRIP, COLS, dtype=BF16)
    side = field(2, 256, 128, dtype=BF16)
    a, b = call(
        pack_rows_kernel, (strip, strip),
        [block, block, block, pltpu.VMEM((2, ROWS, COLS), F32), pltpu.SemaphoreType.DMA((4,))],
        *own, psf_index, name="pack_rows", far=4, room=53.3,
    )
    ra = swap(a, "row", 0)
    rb = swap(b, "row", 1)
    table = psf_table.astype(F32)
    normed = (table / jnp.sum(table, axis=(1, 2), keepdims=True)).astype(BF16)
    normed = jnp.pad(normed[:, :, ::-1], ((0, 0), (1, 0), (0, 1))).reshape(64, 1024)
    a, b = call(
        pack_cols_kernel, (side, side), [], *own, psf_index, ra, rb, name="pack_cols"
    )
    ca = swap(a, "col", 0)
    cb = swap(b, "col", 1)
    work = [
        pltpu.VMEM((20, 256, 128), BF16), pltpu.VMEM((20, 144, 128), F32),
        pltpu.VMEM((20, 144, 256), BF16), pltpu.VMEM((20, 176, 128), F32),
    ]
    wide = field(192, WIDE)
    local = field(ROWS, WIDE)
    *fields, taps = call(
        local_kernel,
        (field(ROWS, FULL), local, local, local, local, field(4, 256, 256, dtype=BF16)),
        [pltpu.VMEM((24, 1024), F32)],
        *own, psf_index, normed, name="local", room=4, flops=1 << 32,
    )
    ready = call(
        middle_kernel,
        (
            field(272, FULL), field(224, WIDE), field(160, WIDE), field(224, WIDE), wide, wide,
            field(272, FULL), field(8, 256, 256, dtype=BF16),
        ),
        [pltpu.VMEM((24, 1024), F32)] + work,
        *fields, taps, normed, ra, rb, name="middle", room=16, flops=1 << 33,
    )
    return call(
        main_kernel,
        (field(ROWS, COLS), field(ROWS, COLS)),
        [
            pltpu.VMEM((3, 272, 128), F32), pltpu.VMEM((2, 2, 192, 128), F32),
            pltpu.VMEM((2, 224, 128), F32), pltpu.VMEM((160, WIDE), F32),
            pltpu.VMEM((192, WIDE), F32), pltpu.VMEM((192, WIDE), F32),
            pltpu.VMEM((24, 1024), F32), pltpu.VMEM((6, 256, 256), BF16),
        ] + work + [
            pltpu.VMEM((272, FULL), F32), pltpu.VMEM((208, FULL), F32), pltpu.VMEM((ROWS, WIDE), F32),
            pltpu.VMEM((ROWS, COLS), F32), pltpu.SemaphoreType.DMA((1,)),
        ],
        normed, ca, cb, *ready, taps, name="main", room=20, out_far=1,
    )


def solution(mesh):
    placed = (
        P("row", "col"),
        P(),
        P("row", "col"),
        P("row", "col"),
        P("row", "col"),
        P(None, "row", "col"),
    )
    return jax.shard_map(
        per_device,
        mesh=mesh,
        in_specs=placed,
        out_specs=(P("row", "col"), P("row", "col")),
        check_vma=False,
    )
```

```python
import jax
import jax.numpy as jnp
from jax import lax
from jax.experimental import pallas as pl
from jax.experimental.pallas import tpu as pltpu
from jax.sharding import PartitionSpec as P

SIGMA = 0.15
TAU = 0.6
TV = 0.5
F32 = jnp.float32
BF16 = jnp.bfloat16

ROWS = 128
COLS = 512
XO = 80
YO = 64
WIDE = 640
FULL = 768
SEGS1 = ((0, 48, 64), (48, 128, 144), (176, 48, 64))
SEGS2 = ((0, 16, 32), (16, 128, 144), (144, 16, 32))
PATCHES2 = ((1,), (2, 3, 4, 5), (6, 7, 8, 9), (10, 11, 12, 13), (14, 15, 16, 17), (18,))
INNER = ((0, (3, 4, 5)), (1, (6, 7, 8, 9)), (2, (10, 11, 12, 13)), (3, (14, 15, 16)))
OUTER = ((-1, (0, 1)), (0, (2,)), (3, (17,)), (4, (18, 19)))
ALL = tuple((patch - 1, blocks) for patch, blocks in enumerate(PATCHES2))
SX, SXL, SC, SCL, SO, S1, S2, SM, STRIP = 0, 64, 80, 128, 144, 160, 192, 224, 240


def iota(shape, dim):
    return lax.broadcasted_iota(jnp.int32, shape, dim)


def split(value):
    hi = value.astype(BF16).astype(F32)
    return hi, value - hi


def lanes(value, shift):
    shift = shift % value.shape[1]
    return pltpu.roll(value, shift, 1) if shift else value


def rows(value, shift):
    shift = shift % value.shape[0]
    return pltpu.roll(value, shift, 0) if shift else value


def between(shape, lo, hi):
    lane = iota(shape, 1)
    return (lane >= lo) & (lane < hi)


def flags():
    row = lax.axis_index("row")
    col = lax.axis_index("col")
    return (
        row > 0,
        row < lax.axis_size("row") - 1,
        col > 0,
        col < lax.axis_size("col") - 1,
    )


def index_line(idx_ref, width):
    lane = iota((1, width), 1)
    line = jnp.zeros((1, width), F32)
    for j in range(4):
        line = jnp.where(lane == 1 + j, idx_ref[0:1, j : j + 1].astype(F32), line)
    return line


def parities():
    return lax.axis_index("row") % 2 == 1, lax.axis_index("col") % 2 == 1


def chosen(flag, one_ref, two_ref):
    def read(at):
        return jnp.where(flag, one_ref[at].astype(F32), two_ref[at].astype(F32))

    return read


def sides(a_ref, b_ref, odd):
    return chosen(odd, a_ref, b_ref), chosen(odd, b_ref, a_ref)


def pack_rows_kernel(x_hbm, y_hbm, o_hbm, q_hbm, idx_ref, a_ref, b_ref, x_ref, y_ref, o_ref, q_ref, sems):
    copies = [
        pltpu.make_async_copy(src, dst, sems.at[i])
        for i, (src, dst) in enumerate(((x_hbm, x_ref), (y_hbm, y_ref), (o_hbm, o_ref), (q_hbm, q_ref)))
    ]
    for copy in copies:
        copy.start()
    line = index_line(idx_ref, COLS)
    odd, _ = parities()

    def put(at, count, down, up):
        a_ref[at : at + count] = jnp.where(odd, up, down).astype(BF16)
        b_ref[at : at + count] = jnp.where(odd, down, up).astype(BF16)

    copies[0].wait()
    put(SX, 64, x_ref[64:128], x_ref[0:64])
    put(SXL, 16, split(x_ref[112:128])[1], split(x_ref[0:16])[1])
    copies[1].wait()
    copies[2].wait()
    up = y_ref[0:48] - SIGMA * o_ref[0:48]
    down = y_ref[80:128] - SIGMA * o_ref[80:128]
    put(SC, 48, down, up)
    put(SCL, 16, split(down[32:48])[1], split(up[0:16])[1])
    put(SO, 16, o_ref[112:128], o_ref[0:16])
    copies[3].wait()
    put(S1, 32, q_ref[0, 96:128], q_ref[0, 0:32])
    put(S2, 32, q_ref[1, 96:128], q_ref[1, 0:32])
    row = iota((16, COLS), 0)
    rest = []
    for edge in (127, 0):
        misc = jnp.zeros((16, COLS), F32)
        for comp in range(2):
            misc = jnp.where(row == comp, split(q_ref[comp, edge : edge + 1])[1], misc)
        rest.append(jnp.where(row == 2, line, misc))
    put(SM, 16, *rest)


def pack_cols_kernel(x_ref, y_ref, o_ref, q_ref, idx_ref, ra_ref, rb_ref, a_ref, b_ref):
    odd_row, odd_col = parities()
    top, bot = sides(ra_ref, rb_ref, odd_row)
    made = []
    for base in (384, 0):
        right = base > 0
        own = slice(base, base + 128)

        def strip(read, at, count, own=own):
            return read((slice(at, at + count), own))

        def column(middle, at, count, shift):
            parts = [strip(top, at, count), middle, strip(bot, at, count)]
            return lanes(jnp.concatenate(parts, axis=0), shift)

        seen = o_ref[:, own]
        x_hi, x_lo = split(x_ref[:, own])
        c_hi, c_lo = split(y_ref[:, own] - SIGMA * seen)
        zeros = jnp.zeros((128, 128), F32)
        buf = column(x_hi, SX, 64, 80)
        part = jnp.concatenate([column(c_hi, SC, 48, 0 if right else 16), zeros[:32]], axis=0)
        at = 80 if right else 16
        buf = jnp.where(between((256, 128), at, at + 48), part, buf)
        part = jnp.concatenate([column(seen, SO, 16, 16 if right else 64), zeros[:96]], axis=0)
        at = 0 if right else 64
        buf = jnp.where(between((256, 128), at, at + 16), part, buf)
        made.append(buf)
        buf = jnp.concatenate([column(q_ref[0, :, own], S1, 32, 80)], axis=0)
        part = jnp.concatenate(
            [column(q_ref[1, :, own], S2, 32, 112 if right else 0)], axis=0
        )
        at = 80 if right else 0
        buf = jnp.where(between((192, 128), at, at + 32), part, buf)
        shift = 0 if right else 32
        part = jnp.concatenate(
            [
                lanes(strip(top, SXL, 16), shift),
                lanes(x_lo, shift),
                lanes(strip(bot, SXL, 16), shift),
                zeros[:32],
            ],
            axis=0,
        )
        at = 112 if right else 32
        buf = jnp.where(between((192, 128), at, at + 16), part, buf)
        shift = 16 if right else 64
        part = jnp.concatenate(
            [
                lanes(strip(top, SCL, 16), shift),
                lanes(c_lo, shift),
                lanes(strip(bot, SCL, 16), shift),
                zeros[:32],
            ],
            axis=0,
        )
        at = 0 if right else 64
        buf = jnp.where(between((192, 128), at, at + 16), part, buf)
        if right:
            for comp in range(2):
                low = lanes(split(q_ref[comp, :, own])[1], 17 + comp)
                part = jnp.concatenate([zeros[:32], low, zeros[:32]], axis=0)
                buf = jnp.where(between((192, 128), 16 + comp, 17 + comp), part, buf)
        row = iota((192, 1), 0)
        spot = 4 if right else 1
        first = top((slice(SM, SM + 16), slice(0, 128)))[2:3, spot : spot + 1]
        last = bot((slice(SM, SM + 16), slice(0, 128)))[2:3, spot : spot + 1]
        mine = idx_ref[0:1, spot - 1 : spot].astype(F32)
        entry = jnp.where(row == 0, first, jnp.where(row == 1, mine, last))
        at = 18 if right else 112
        buf = jnp.where(between((192, 128), at, at + 1), entry, buf)
        made.append(buf)
    for tile, span in enumerate((slice(0, 256), slice(256, 448))):
        a_ref[span] = jnp.where(odd_col, made[2 + tile], made[tile]).astype(BF16)
        b_ref[span] = jnp.where(odd_col, made[tile], made[2 + tile]).astype(BF16)


def build_taps(tab_ref, t_ref, places):
    size = 8 * len(places)
    sub = iota((size, 128), 0)
    bits = [(sub // (1 << n)) % 2 == 1 for n in range(3)]
    for e in range(8):
        a1, half = 2 * (e // 4) + e % 2, e // 2 % 2
        here = slice(128 * half, 128 * half + 128)
        skew = jnp.concatenate(
            [
                jnp.broadcast_to(
                    tab_ref[at : at + 1, 128 * e : 128 * e + 128], (8, 128)
                )
                for at in places
            ],
            axis=0,
        )
        for n in range(3):
            skew = jnp.where(bits[n], lanes(skew, 1 << n), skew)
        lower_all = [iota((size, 128), 1) % 32 <= sub % 8 + 8 * v for v in range(4)]
        low = [jnp.where(lower_all[v], lanes(skew, 8 * v - 31), 0.0) for v in range(4)]
        high = [jnp.where(lower_all[v], 0.0, lanes(skew, 8 * v + 1)) for v in range(4)]
        for patch in range(len(places)):
            own = slice(8 * patch, 8 * patch + 8)
            block = jnp.concatenate([part[own] for part in low + high], axis=0)
            t_ref[patch, 64 * a1 : 64 * a1 + 64, here] = block.astype(BF16)


def windows(get, p_ref, blocks, count):
    low = between((count, 128), 0, 64)
    tail = between((count, 128), 96, 128)
    for b in blocks:
        tile, place = b // 4, b % 4
        x0, x4 = get(tile, 0), get(tile, 4)
        if place == 0:
            part = jnp.where(low, x0, lanes(x4, 64))
        elif place == 1:
            part = jnp.where(low, lanes(x0, 96), lanes(x4, 32))
        elif place == 2:
            part = jnp.where(low, lanes(x0, 64), x4)
        else:
            w0 = jnp.where(tail, x0, get(tile + 1, 0))
            w4 = jnp.where(tail, x4, get(tile + 1, 4))
            part = jnp.where(low, lanes(w0, 32), lanes(w4, 96))
        p_ref[b, 0:count] = part.astype(BF16)


def blur(segs, groups, taps, p_ref, a_ref, put):
    present = [b for _, blocks in groups for b in blocks]
    for seg, (first, size, padded) in enumerate(segs):
        for patch, blocks in groups:
            lhs = jnp.concatenate(
                [
                    jnp.concatenate(
                        [
                            p_ref[b, first : first + padded],
                            p_ref[b, first + 16 : first + 16 + padded],
                        ],
                        axis=1,
                    )
                    for b in blocks
                ],
                axis=0,
            )
            v = jnp.dot(lhs, taps(seg, patch), preferred_element_type=F32)
            for place, b in enumerate(blocks):
                part = v[place * padded : place * padded + padded]
                a_ref[b, 0:padded] = part[:, :128] + rows(part[:, 128:], -8)
        low = between((padded, 128), 0, 64)
        even = iota((padded, 128), 1) % 64 < 32
        for tile in sorted({b // 4 for b in present}):
            a = [
                a_ref[4 * tile + p, 0:padded]
                if 4 * tile + p in present
                else jnp.zeros((padded, 128), F32)
                for p in range(4)
            ]
            e = []
            for p in range(2):
                z = lanes(jnp.where(low, a[p + 2], a[p]), 64)
                e.append(jnp.where(low, a[p], z) + rows(jnp.where(low, z, a[p + 2]), -2))
            m1 = jnp.where(even, e[0], lanes(e[1], 32))
            m2 = jnp.where(even, lanes(e[0], 96), e[1])
            blurred = (m1 + rows(m2, -1))[0:size]
            put(seg, first, size, tile, blurred)


def adjoint(segs, groups, taps, get, l_ref, f_ref, z_ref):
    present = [b for _, blocks in groups for b in blocks]
    tiles = sorted({b // 4 for b in present})
    for seg, (first, size, padded) in enumerate(segs):
        low = between((padded, 128), 0, 64)
        even = iota((padded, 128), 1) % 64 < 32
        for tile in tiles:
            o = jnp.concatenate(
                [get(first, size, tile), jnp.zeros((padded - size, 128), F32)], axis=0
            )
            o1 = rows(o, 1)
            e = [jnp.where(even, o, lanes(o1, 32)), jnp.where(even, lanes(o, 96), o1)]
            for p in range(2):
                s = rows(e[p], 2)
                for place in (p, p + 2):
                    b = 4 * tile + place
                    if b not in present:
                        continue
                    if place < 2:
                        part = jnp.where(low, e[p], lanes(s, 64))
                    else:
                        part = jnp.where(low, lanes(e[p], 64), s)
                    l_ref[b, 0:padded, 0:128] = part.astype(BF16)
                    l_ref[b, 0:padded, 128:256] = rows(part, 8).astype(BF16)
        for patch, blocks in groups:
            lhs = jnp.concatenate([l_ref[b, 0:padded] for b in blocks], axis=0)
            g = lax.dot_general(
                lhs, taps(seg, patch), (((1,), (1,)), ((), ())), preferred_element_type=F32
            )
            zero = jnp.zeros((16, 128), F32)
            for place, b in enumerate(blocks):
                part = g[place * padded : place * padded + padded]
                f_ref[b, 0:8] = zero[0:8]
                f_ref[b, 8 : padded + 24] = jnp.concatenate(
                    [part[:, :128], zero], axis=0
                ) + jnp.concatenate([zero, part[:, 128:]], axis=0)
                f_ref[b, padded + 24 : padded + 32] = zero[0:8]
        tall = padded + 24
        low = between((tall, 128), 0, 64)
        head = between((tall, 128), 0, 32)

        def both_ways(b):
            if b not in present:
                zero = jnp.zeros((tall, 128), F32)
                return zero, zero
            return f_ref[b, 8 : 8 + tall], f_ref[b, 4 : 4 + tall]

        spill = None
        for tile in tiles:
            both = []
            for p in range(2):
                a0, a8 = both_ways(4 * tile + p)
                b0, b8 = both_ways(4 * tile + p + 2)
                both.append(jnp.where(low, a0, b8) + lanes(jnp.where(low, b0, a8), 64))
            turned = lanes(both[1], 32)
            here = slice(128 * tile, 128 * tile + 128)
            after = slice(128 * tile + 128, 128 * tile + 256)
            span = slice(first, first + tall)
            if spill is None:
                turned_here = jnp.where(head, 0.0, turned)
            else:
                turned_here = jnp.where(head, spill, turned)
            z_ref[span, here] += both[0] + turned_here
            spill = turned
            if tile + 1 not in tiles:
                z_ref[span, after] += jnp.where(head, turned, 0.0)
                spill = None


def on_tile(value, tile, change):
    parts = [value[:, 128 * k : 128 * k + 128] for k in range(5)]
    parts[tile] = change(parts[tile])
    return jnp.concatenate(parts, axis=1)


def unless(bad, value):
    return jnp.where(bad, 0.0, value)


def total_variation(get_x, get_q, q1_ref, q2_ref, chunks):
    _, bot_ok, _, right_ok = flags()
    lane = iota((16, 128), 1)
    past = (lane + 512 - XO >= COLS - 1) & jnp.logical_not(right_ok)
    for chunk in chunks:
        start = 16 * chunk
        tall = get_x(start, 24)
        x = tall[0:16]
        g1 = rows(tall, -1)[0:16] - x
        g2 = on_tile(lanes(x, -1) - x, 4, lambda part: unless(past, part))
        if start + 16 > 31 + ROWS:
            row = start - 32 + iota((16, WIDE), 0)
            g1 = unless((row >= ROWS - 1) & jnp.logical_not(bot_ok), g1)
        span = slice(start, start + 16)
        u1 = get_q(0, start) + SIGMA * g1
        u2 = get_q(1, start) + SIGMA * g2
        scale = jnp.minimum(1.0, TV * lax.rsqrt(u1 * u1 + u2 * u2))
        q1_ref[span] = u1 * scale
        q2_ref[span] = u2 * scale


def divergence(q1_ref, q2_ref, start):
    top_ok, bot_ok, left_ok, right_ok = flags()
    above = max(start - 8, 0)
    m1 = q1_ref[above : start + 16]
    m2 = q2_ref[start : start + 16]
    row = above - 32 + iota(m1.shape, 0)
    if above < 32:
        m1 = unless((row < 0) & jnp.logical_not(top_ok), m1)
    if start + 16 > 31 + ROWS:
        m1 = unless((row >= ROWS - 1) & jnp.logical_not(bot_ok), m1)
    lane = iota((16, 128), 1)
    m2 = on_tile(m2, 0, lambda part: unless((lane < XO) & jnp.logical_not(left_ok), part))
    past = (lane + 512 - XO >= COLS - 1) & jnp.logical_not(right_ok)
    m2 = on_tile(m2, 4, lambda part: unless(past, part))
    return (m1 - rows(m1, 1))[start - above :] + (m2 - lanes(m2, 1))


def masks():
    top, bot, left, right = flags()

    def row_ok(seg):
        if seg == 1:
            return jnp.bool_(True)
        return top if seg == 0 else bot

    def col_ok(tile, size):
        lane = iota((size, 128), 1)
        if tile == 0:
            return (lane >= YO) | left
        if tile == 4:
            return (lane < YO) | right
        return jnp.ones((size, 128), jnp.bool_)

    return row_ok, col_ok


def widen(value, shift, width=WIDE):
    pad = jnp.zeros((value.shape[0], width - COLS), F32)
    return lanes(jnp.concatenate([value, pad], axis=1), shift)


def select_tables(table_ref, total, tab_ref):
    onehot = jnp.where(total == iota((64, 128), 0).astype(F32), 1.0, 0.0).astype(BF16)
    picked = lax.dot_general(
        onehot, table_ref[...], (((0,), (0,)), ((), ())), preferred_element_type=F32
    )
    tab_ref[...] = picked[0:24]


def tile_of(value, tile):
    return value[:, 128 * tile : 128 * tile + 128]


def local_kernel(
    x_ref, y_ref, o_ref, q_ref, idx_ref, table_ref,
    xw_ref, cw_ref, ow_ref, q1w_ref, q2w_ref, t_ref,
    tab_ref,
):
    select_tables(table_ref, index_line(idx_ref, 128), tab_ref)
    build_taps(tab_ref, t_ref, range(1, 5))
    xw_ref[...] = widen(x_ref[...], XO, FULL)
    seen = o_ref[...]
    cw_ref[...] = widen(y_ref[...] - SIGMA * seen, YO)
    ow_ref[...] = widen(seen, YO)
    q1w_ref[...] = widen(q_ref[0], XO)
    q2w_ref[...] = widen(q_ref[1], XO)


def middle_kernel(
    xw_ref, cw_ref, ow_ref, q1w_ref, q2w_ref, own_ref, table_ref, ra_ref, rb_ref,
    xe_ref, c_ref, ob_ref, ys_ref, q1_ref, q2_ref, z_ref, t_ref,
    tab_ref, p_ref, a_ref, l_ref, f_ref,
):
    top_ok, bot_ok, _, _ = flags()
    odd, _ = parities()
    top, bot = sides(ra_ref, rb_ref, odd)
    misc = slice(SM, SM + 16)
    lane = iota((1, 128), 1)
    upper = top((misc, slice(0, 128)))[2:3]
    lower = bot((misc, slice(0, 128)))[2:3]
    select_tables(table_ref, jnp.where(lane < 8, upper, lanes(lower, 8)), tab_ref)
    build_taps(tab_ref, t_ref, [1, 2, 3, 4, 9, 10, 11, 12])

    def part(read, at, count):
        return read(slice(at, at + count))

    zero = jnp.zeros((48, COLS), F32)
    above = part(top, SX, 64) + jnp.concatenate([zero, part(top, SXL, 16)], axis=0)
    below = part(bot, SX, 64) + jnp.concatenate([part(bot, SXL, 16), zero], axis=0)
    xe_ref[0:64] = widen(jnp.where(top_ok, above, 0.0), XO, FULL)
    xe_ref[64:192] = xw_ref[...]
    xe_ref[192:256] = widen(jnp.where(bot_ok, below, 0.0), XO, FULL)
    xe_ref[256:272] = jnp.zeros((16, FULL), F32)
    c_ref[48:176] = cw_ref[...]
    ob_ref[16:144] = ow_ref[...]
    zero = jnp.zeros((32, COLS), F32)
    above = part(top, SC, 48) + jnp.concatenate([zero, part(top, SCL, 16)], axis=0)
    below = part(bot, SC, 48) + jnp.concatenate([part(bot, SCL, 16), zero], axis=0)
    c_ref[0:48] = widen(above, YO)
    c_ref[176:224] = widen(below, YO)
    ob_ref[0:16] = widen(part(top, SO, 16), YO)
    ob_ref[144:160] = widen(part(bot, SO, 16), YO)
    rix = iota((32, COLS), 0)
    rest = top(misc)
    for comp, (ref, section, own) in enumerate(((q1_ref, S1, q1w_ref), (q2_ref, S2, q2w_ref))):
        above = part(top, section, 32) + jnp.where(rix == 31, rest[comp : comp + 1], 0.0)
        ref[0:32] = widen(above, XO)
        ref[32:160] = own[...]
        ref[160:192] = widen(part(bot, section, 32), XO)
    row_ok, _ = masks()

    def taps(seg, patch):
        return own_ref[patch] if seg == 1 else t_ref[2 * seg + patch]

    def get_x(tile, first):
        return xe_ref[first : first + 256, 128 * tile : 128 * tile + 128]

    def put(seg, first, size, tile, blurred):
        here = slice(128 * tile, 128 * tile + 128)
        new = (c_ref[first : first + size, here] + SIGMA * blurred) * (1.0 / (1.0 + SIGMA))
        ys_ref[first : first + size, here] = new if seg == 1 else jnp.where(row_ok(seg), new, 0.0)

    def get_y(first, size, tile):
        return ys_ref[first : first + size, 128 * tile : 128 * tile + 128]

    windows(get_x, p_ref, range(3, 17), 256)
    blur(SEGS1, INNER, taps, p_ref, a_ref, put)
    z_ref[...] = jnp.zeros_like(z_ref)
    adjoint(SEGS1, INNER, taps, get_y, l_ref, f_ref, z_ref)


def main_kernel(
    table_ref, ca_ref, cb_ref,
    xi_ref, ci_ref, oi_ref, yi_ref, q1i_ref, q2i_ref, zi_ref, ti_ref, own_ref,
    x2_ref, y2_hbm,
    side_ref, qs_ref, ys_ref, c_ref, q1_ref, q2_ref, tab_ref, t_ref, p_ref, a_ref, l_ref, f_ref,
    z_ref, xb_ref, x1_ref, y2_ref, sem,
):
    top_ok, bot_ok, left_ok, right_ok = flags()
    _, odd_col = parities()
    before, after = sides(ca_ref, cb_ref, odd_col)
    first, second = slice(0, 256), slice(256, 448)
    lf0, lf1, rt0, rt1 = before(first), before(second), after(first), after(second)
    gap = jnp.zeros((48, 128), F32)

    def from_row(value, count):
        return jnp.concatenate([gap[: count // 2 - 80], value[0:160], gap[: count // 2 - 80]], axis=0)

    lane = iota((1, 128), 1)
    total = jnp.full((1, 128), -1.0, F32)
    for r in range(3):
        total = jnp.where(lane == 8 * r, lf1[r : r + 1, 18:19], total)
        total = jnp.where(lane == 8 * r + 5, rt1[r : r + 1, 112:113], total)
    select_tables(table_ref, total, tab_ref)
    build_taps(tab_ref, t_ref, [8 * r + p for r in range(3) for p in (0, 5)])

    def taps(seg, patch):
        if 0 <= patch < 4:
            return own_ref[patch] if seg == 1 else ti_ref[2 * seg + patch]
        return t_ref[2 * seg + (patch == 4)]

    rr = iota((256, 128), 0)
    rows_ok = ((rr >= 64) | top_ok) & ((rr < 192) | bot_ok)
    shape = (256, 128)
    part = jnp.where(between(shape, 16, 80), lf0, 0.0)
    part += jnp.where(between(shape, 64, 80), lanes(from_row(lf1, 256), 80), 0.0)
    side_ref[0, 0:256] = xi_ref[0:256, 0:128] + jnp.where(rows_ok & left_ok, part, 0.0)
    part = jnp.where(between(shape, 80, 128), rt0, 0.0)
    part += jnp.where(between(shape, 80, 96), lanes(from_row(rt1, 256), 48), 0.0)
    side_ref[1, 0:256] = xi_ref[0:256, 512:640] + jnp.where(rows_ok & right_ok, part, 0.0)
    part = jnp.where(between(shape, 0, 16), rt0, 0.0)
    side_ref[2, 0:256] = xi_ref[0:256, 640:768] + jnp.where(rows_ok & right_ok, part, 0.0)
    side_ref[:, 256:272] = jnp.zeros((3, 16, 128), F32)
    shape = (192, 128)
    for comp, ref in enumerate((q1i_ref, q2i_ref)):
        part = lanes(lf1[0:192], 96 * comp)
        part += jnp.where(between(shape, 79, 80), lanes(lf1[0:192], 63 - comp), 0.0)
        qs_ref[comp, 0] = jnp.where(between(shape, 48, 80), part, ref[:, 0:128])
        part = lanes(rt1[0:192], 80 * comp)
        qs_ref[comp, 1] = jnp.where(between(shape, 80, 112), part, ref[:, 512:640])
    shape = (224, 128)
    part = lanes(lf0[0:224], 64) + jnp.where(between(shape, 48, 64), lanes(from_row(lf1, 224), 48), 0.0)
    c_first = jnp.where(between(shape, 16, 64), part, ci_ref[:, 0:128])
    part = lanes(rt0[0:224], 48) + jnp.where(between(shape, 64, 80), from_row(rt1, 224), 0.0)
    c_last = jnp.where(between(shape, 64, 112), part, ci_ref[:, 512:640])
    shape = (160, 128)
    o_first = jnp.where(between(shape, 48, 64), lanes(lf0[0:160], 48), oi_ref[:, 0:128])
    o_last = jnp.where(between(shape, 64, 80), rt0[0:160], oi_ref[:, 512:640])
    row_ok, col_ok = masks()

    def get_side(tile, first):
        which = {0: 0, 4: 1, 5: 2}[tile]
        return side_ref[which, first : first + 256]

    def put_side(seg, first, size, tile, blurred):
        c = (c_first if tile == 0 else c_last)[first : first + size]
        new = (c + SIGMA * blurred) * (1.0 / (1.0 + SIGMA))
        new = jnp.where(col_ok(tile, size) & row_ok(seg), new, 0.0)
        old = yi_ref[first : first + size, 128 * tile : 128 * tile + 128]
        inner = between((size, 128), 96, 128) if tile == 0 else between((size, 128), 0, 32)
        ys_ref[tile // 4, first : first + size] = jnp.where(inner, old, new)

    def get_side_y(first, size, tile):
        return ys_ref[tile // 4, first : first + size]

    windows(get_side, p_ref, (0, 1, 2, 17, 18, 19), 256)
    blur(SEGS1, OUTER, taps, p_ref, a_ref, put_side)

    def get_x(start, count):
        at = slice(32 + start, 32 + start + count)
        return jnp.concatenate([side_ref[0, at], xi_ref[at, 128:512], side_ref[1, at]], axis=1)

    def get_q(comp, start):
        at = slice(start, start + 16)
        ref = q2i_ref if comp else q1i_ref
        return jnp.concatenate([qs_ref[comp, 0, at], ref[at, 128:512], qs_ref[comp, 1, at]], axis=1)

    total_variation(get_x, get_q, q1_ref, q2_ref, range(12))
    z_ref[...] = zi_ref[...]
    adjoint(SEGS1, OUTER, taps, get_side_y, l_ref, f_ref, z_ref)
    lane = iota((16, 128), 1)
    for chunk in range(12):
        start = 16 * chunk
        ext = slice(32 + start, 48 + start)
        x = get_x(start, 16)
        new = x - TAU * (z_ref[ext, 0:WIDE] - divergence(q1_ref, q2_ref, start))
        ahead = 2.0 * new - x
        ahead = on_tile(ahead, 0, lambda part: unless((lane < XO) & jnp.logical_not(left_ok), part))
        past = (lane + 512 - XO >= COLS) & jnp.logical_not(right_ok)
        ahead = on_tile(ahead, 4, lambda part: unless(past, part))
        if chunk < 2 or chunk >= 10:
            ahead = jnp.where(top_ok if chunk < 2 else bot_ok, ahead, 0.0)
        xb_ref[start : start + 16, 0:WIDE] = ahead
        if 2 <= chunk < 10:
            x1_ref[start - 32 : start - 16] = new
    xb_ref[192:208, 0:WIDE] = jnp.zeros((16, WIDE), F32)
    xb_ref[:, WIDE:FULL] = jnp.zeros((208, FULL - WIDE), F32)
    c_ref[:, 0:128] = ys_ref[0, 32:192] - SIGMA * o_first
    c_ref[:, 128:512] = yi_ref[32:192, 128:512] - SIGMA * oi_ref[:, 128:512]
    c_ref[:, 512:640] = ys_ref[1, 32:192] - SIGMA * o_last

    def get_xb(tile, first):
        return xb_ref[first : first + 192, 128 * tile : 128 * tile + 128]

    def put(seg, first, size, tile, blurred):
        here = slice(128 * tile, 128 * tile + 128)
        new = (c_ref[first : first + size, here] + SIGMA * blurred) * (1.0 / (1.0 + SIGMA))
        if seg != 1 or tile in (0, 4):
            new = jnp.where(col_ok(tile, size) & row_ok(seg), new, 0.0)
        c_ref[first : first + size, here] = new

    def get_y(first, size, tile):
        return c_ref[first : first + size, 128 * tile : 128 * tile + 128]

    windows(get_xb, p_ref, range(1, 19), 192)
    blur(SEGS2, ALL, taps, p_ref, a_ref, put)
    for chunk in range(8):
        span = slice(16 * chunk, 16 * chunk + 16)
        y2_ref[span] = lanes(c_ref[16 + 16 * chunk : 32 + 16 * chunk], -YO)[:, :COLS]
    total_variation(
        lambda start, count: xb_ref[start : start + count, 0:WIDE],
        lambda comp, start: (q2_ref if comp else q1_ref)[start : start + 16],
        q1_ref, q2_ref, range(1, 10),
    )
    done = pltpu.make_async_copy(y2_ref, y2_hbm, sem.at[0])
    done.start()
    z_ref[...] = jnp.zeros_like(z_ref)
    adjoint(SEGS2, ALL, taps, get_y, l_ref, f_ref, z_ref)
    for chunk in range(8):
        span = slice(16 * chunk, 16 * chunk + 16)
        ext = slice(32 + 16 * chunk, 48 + 16 * chunk)
        div = divergence(q1_ref, q2_ref, 32 + 16 * chunk)
        new = x1_ref[span] - TAU * (z_ref[ext, 0:WIDE] - div)
        x2_ref[span] = lanes(new, -XO)[:, :COLS]
    done.wait()


def field(*shape, dtype=F32):
    return jax.ShapeDtypeStruct(shape, dtype)


def call(kernel, outs, scratch, *args, name, room=4, far=0, flops=0, out_far=0):
    spaces = [pltpu.HBM] * far + [pltpu.VMEM] * (len(args) - far)
    return pl.pallas_call(
        kernel,
        out_shape=outs,
        out_specs=tuple(
            pl.BlockSpec(memory_space=pltpu.HBM if i >= len(outs) - out_far else pltpu.VMEM)
            for i in range(len(outs))
        ),
        in_specs=[pl.BlockSpec(memory_space=space) for space in spaces],
        scratch_shapes=scratch,
        compiler_params=pltpu.CompilerParams(vmem_limit_bytes=int(room * 1024 * 1024)),
        cost_estimate=pl.CostEstimate(flops=flops, bytes_accessed=0, transcendentals=0)
        if flops
        else None,
        name=name,
    )(*args)


def swap(block, axis, first):
    high, wide = lax.axis_size("row"), lax.axis_size("col")

    def partner(row, col):
        if axis == "row":
            to = ((row - first) ^ 1) + first
            return (to, col) if 0 <= to < high else (row, col ^ 2 if wide > 2 else col ^ 1)
        to = ((col - first) ^ 1) + first
        return (row, to) if 0 <= to < wide else (row ^ 1, col)

    pairs = []
    for row in range(high):
        for col in range(wide):
            to_row, to_col = partner(row, col)
            pairs.append((row * wide + col, to_row * wide + to_col))
    return lax.ppermute(block, ("row", "col"), pairs)


def per_device(observed, psf_table, psf_index, start_image, blur_dual, tv_dual):
    own = (start_image, blur_dual, observed, tv_dual)
    block = pltpu.VMEM((ROWS, COLS), F32)
    strip = field(STRIP, COLS, dtype=BF16)
    side = field(448, 128, dtype=BF16)
    a, b = call(
        pack_rows_kernel, (strip, strip),
        [block, block, block, pltpu.VMEM((2, ROWS, COLS), F32), pltpu.SemaphoreType.DMA((4,))],
        *own, psf_index, name="pack_rows", far=4, room=53.3,
    )
    ra = swap(a, "row", 0)
    rb = swap(b, "row", 1)
    table = psf_table.astype(F32)
    normed = (table / jnp.sum(table, axis=(1, 2), keepdims=True)).astype(BF16)
    normed = jnp.pad(normed[:, :, ::-1], ((0, 0), (1, 0), (0, 1))).reshape(64, 1024)
    a, b = call(
        pack_cols_kernel, (side, side), [], *own, psf_index, ra, rb, name="pack_cols"
    )
    ca = swap(a, "col", 0)
    cb = swap(b, "col", 1)
    work = [
        pltpu.VMEM((20, 256, 128), BF16), pltpu.VMEM((20, 144, 128), F32),
        pltpu.VMEM((20, 144, 256), BF16), pltpu.VMEM((20, 176, 128), F32),
    ]
    wide = field(192, WIDE)
    local = field(ROWS, WIDE)
    *fields, taps = call(
        local_kernel,
        (field(ROWS, FULL), local, local, local, local, field(4, 256, 256, dtype=BF16)),
        [pltpu.VMEM((24, 1024), F32)],
        *own, psf_index, normed, name="local", room=4, flops=1 << 32,
    )
    ready = call(
        middle_kernel,
        (
            field(272, FULL), field(224, WIDE), field(160, WIDE), field(224, WIDE), wide, wide,
            field(272, FULL), field(8, 256, 256, dtype=BF16),
        ),
        [pltpu.VMEM((24, 1024), F32)] + work,
        *fields, taps, normed, ra, rb, name="middle", room=16, flops=1 << 33,
    )
    return call(
        main_kernel,
        (field(ROWS, COLS), field(ROWS, COLS)),
        [
            pltpu.VMEM((3, 272, 128), F32), pltpu.VMEM((2, 2, 192, 128), F32),
            pltpu.VMEM((2, 224, 128), F32), pltpu.VMEM((160, WIDE), F32),
            pltpu.VMEM((192, WIDE), F32), pltpu.VMEM((192, WIDE), F32),
            pltpu.VMEM((24, 1024), F32), pltpu.VMEM((6, 256, 256), BF16),
        ] + work + [
            pltpu.VMEM((272, FULL), F32), pltpu.VMEM((208, FULL), F32), pltpu.VMEM((ROWS, WIDE), F32),
            pltpu.VMEM((ROWS, COLS), F32), pltpu.SemaphoreType.DMA((1,)),
        ],
        normed, ca, cb, *ready, taps, name="main", room=20, out_far=1,
    )


def solution(mesh):
    placed = (
        P("row", "col"),
        P(),
        P("row", "col"),
        P("row", "col"),
        P("row", "col"),
        P(None, "row", "col"),
    )
    return jax.shard_map(
        per_device,
        mesh=mesh,
        in_specs=placed,
        out_specs=(P("row", "col"), P("row", "col")),
        check_vma=False,
    )
```

```python
import jax
import jax.numpy as jnp
from jax import lax
from jax.experimental import pallas as pl
from jax.experimental.pallas import tpu as pltpu
from jax.sharding import PartitionSpec as P

SIGMA = 0.15
TAU = 0.6
TV = 0.5
F32 = jnp.float32
BF16 = jnp.bfloat16

ROWS = 128
COLS = 512
XO = 80
YO = 64
WIDE = 640
FULL = 768
SEGS1 = ((0, 48, 64), (48, 128, 144), (176, 48, 64))
SEGS2 = ((0, 16, 32), (16, 128, 144), (144, 16, 32))
PATCHES2 = ((1,), (2, 3, 4, 5), (6, 7, 8, 9), (10, 11, 12, 13), (14, 15, 16, 17), (18,))
INNER = ((0, (3, 4, 5)), (1, (6, 7, 8, 9)), (2, (10, 11, 12, 13)), (3, (14, 15, 16)))
OUTER = ((-1, (0, 1)), (0, (2,)), (3, (17,)), (4, (18, 19)))
ALL = tuple((patch - 1, blocks) for patch, blocks in enumerate(PATCHES2))
SX, SXL, SC, SCL, SO, S1, S2, SM, STRIP = 0, 64, 80, 128, 144, 160, 192, 224, 240


def iota(shape, dim):
    return lax.broadcasted_iota(jnp.int32, shape, dim)


def split(value):
    hi = value.astype(BF16).astype(F32)
    return hi, value - hi


def lanes(value, shift):
    shift = shift % value.shape[1]
    return pltpu.roll(value, shift, 1) if shift else value


def rows(value, shift):
    shift = shift % value.shape[0]
    return pltpu.roll(value, shift, 0) if shift else value


def between(shape, lo, hi):
    lane = iota(shape, 1)
    return (lane >= lo) & (lane < hi)


def flags():
    row = lax.axis_index("row")
    col = lax.axis_index("col")
    return (
        row > 0,
        row < lax.axis_size("row") - 1,
        col > 0,
        col < lax.axis_size("col") - 1,
    )


def index_line(idx_ref, width):
    lane = iota((1, width), 1)
    line = jnp.zeros((1, width), F32)
    for j in range(4):
        line = jnp.where(lane == 1 + j, idx_ref[0:1, j : j + 1].astype(F32), line)
    return line


def parities():
    return lax.axis_index("row") % 2 == 1, lax.axis_index("col") % 2 == 1


def chosen(flag, one_ref, two_ref):
    def read(at):
        return jnp.where(flag, one_ref[at].astype(F32), two_ref[at].astype(F32))

    return read


def sides(a_ref, b_ref, odd):
    return chosen(odd, a_ref, b_ref), chosen(odd, b_ref, a_ref)


def pack_rows_kernel(x_hbm, y_hbm, o_hbm, q_hbm, idx_ref, a_ref, b_ref, x_ref, y_ref, o_ref, q_ref, sems):
    copies = [
        pltpu.make_async_copy(src, dst, sems.at[i])
        for i, (src, dst) in enumerate(((x_hbm, x_ref), (y_hbm, y_ref), (o_hbm, o_ref), (q_hbm, q_ref)))
    ]
    for copy in copies:
        copy.start()
    line = index_line(idx_ref, COLS)
    odd, _ = parities()

    def put(at, count, down, up):
        a_ref[at : at + count] = jnp.where(odd, up, down).astype(BF16)
        b_ref[at : at + count] = jnp.where(odd, down, up).astype(BF16)

    copies[0].wait()
    put(SX, 64, x_ref[64:128], x_ref[0:64])
    put(SXL, 16, split(x_ref[112:128])[1], split(x_ref[0:16])[1])
    copies[1].wait()
    copies[2].wait()
    up = y_ref[0:48] - SIGMA * o_ref[0:48]
    down = y_ref[80:128] - SIGMA * o_ref[80:128]
    put(SC, 48, down, up)
    put(SCL, 16, split(down[32:48])[1], split(up[0:16])[1])
    put(SO, 16, o_ref[112:128], o_ref[0:16])
    copies[3].wait()
    put(S1, 32, q_ref[0, 96:128], q_ref[0, 0:32])
    put(S2, 32, q_ref[1, 96:128], q_ref[1, 0:32])
    row = iota((16, COLS), 0)
    rest = []
    for edge in (127, 0):
        misc = jnp.zeros((16, COLS), F32)
        for comp in range(2):
            misc = jnp.where(row == comp, split(q_ref[comp, edge : edge + 1])[1], misc)
        rest.append(jnp.where(row == 2, line, misc))
    put(SM, 16, *rest)


def pack_cols_kernel(x_ref, y_ref, o_ref, q_ref, idx_ref, ra_ref, rb_ref, a_ref, b_ref):
    odd_row, odd_col = parities()
    top, bot = sides(ra_ref, rb_ref, odd_row)
    made = []
    for base in (384, 0):
        right = base > 0
        own = slice(base, base + 128)

        def strip(read, at, count, own=own):
            return read((slice(at, at + count), own))

        def column(middle, at, count, shift):
            parts = [strip(top, at, count), middle, strip(bot, at, count)]
            return lanes(jnp.concatenate(parts, axis=0), shift)

        seen = o_ref[:, own]
        x_hi, x_lo = split(x_ref[:, own])
        c_hi, c_lo = split(y_ref[:, own] - SIGMA * seen)
        zeros = jnp.zeros((128, 128), F32)
        buf = column(x_hi, SX, 64, 80)
        part = jnp.concatenate([column(c_hi, SC, 48, 0 if right else 16), zeros[:32]], axis=0)
        at = 80 if right else 16
        buf = jnp.where(between((256, 128), at, at + 48), part, buf)
        part = jnp.concatenate([column(seen, SO, 16, 16 if right else 64), zeros[:96]], axis=0)
        at = 0 if right else 64
        buf = jnp.where(between((256, 128), at, at + 16), part, buf)
        made.append(buf)
        buf = jnp.concatenate([column(q_ref[0, :, own], S1, 32, 80)], axis=0)
        part = jnp.concatenate(
            [column(q_ref[1, :, own], S2, 32, 112 if right else 0)], axis=0
        )
        at = 80 if right else 0
        buf = jnp.where(between((192, 128), at, at + 32), part, buf)
        shift = 0 if right else 32
        part = jnp.concatenate(
            [
                lanes(strip(top, SXL, 16), shift),
                lanes(x_lo, shift),
                lanes(strip(bot, SXL, 16), shift),
                zeros[:32],
            ],
            axis=0,
        )
        at = 112 if right else 32
        buf = jnp.where(between((192, 128), at, at + 16), part, buf)
        shift = 16 if right else 64
        part = jnp.concatenate(
            [
                lanes(strip(top, SCL, 16), shift),
                lanes(c_lo, shift),
                lanes(strip(bot, SCL, 16), shift),
                zeros[:32],
            ],
            axis=0,
        )
        at = 0 if right else 64
        buf = jnp.where(between((192, 128), at, at + 16), part, buf)
        if right:
            for comp in range(2):
                low = lanes(split(q_ref[comp, :, own])[1], 17 + comp)
                part = jnp.concatenate([zeros[:32], low, zeros[:32]], axis=0)
                buf = jnp.where(between((192, 128), 16 + comp, 17 + comp), part, buf)
        row = iota((192, 1), 0)
        spot = 4 if right else 1
        first = top((slice(SM, SM + 16), slice(0, 128)))[2:3, spot : spot + 1]
        last = bot((slice(SM, SM + 16), slice(0, 128)))[2:3, spot : spot + 1]
        mine = idx_ref[0:1, spot - 1 : spot].astype(F32)
        entry = jnp.where(row == 0, first, jnp.where(row == 1, mine, last))
        at = 18 if right else 112
        buf = jnp.where(between((192, 128), at, at + 1), entry, buf)
        made.append(buf)
    for tile, span in enumerate((slice(0, 256), slice(256, 448))):
        a_ref[span] = jnp.where(odd_col, made[2 + tile], made[tile]).astype(BF16)
        b_ref[span] = jnp.where(odd_col, made[tile], made[2 + tile]).astype(BF16)


def build_taps(tab_ref, t_ref, places):
    size = 8 * len(places)
    sub = iota((size, 128), 0)
    bits = [(sub // (1 << n)) % 2 == 1 for n in range(3)]
    for e in range(8):
        a1, half = 2 * (e // 4) + e % 2, e // 2 % 2
        here = slice(128 * half, 128 * half + 128)
        skew = jnp.concatenate(
            [
                jnp.broadcast_to(
                    tab_ref[at : at + 1, 128 * e : 128 * e + 128], (8, 128)
                )
                for at in places
            ],
            axis=0,
        )
        for n in range(3):
            skew = jnp.where(bits[n], lanes(skew, 1 << n), skew)
        lower_all = [iota((size, 128), 1) % 32 <= sub % 8 + 8 * v for v in range(4)]
        low = [jnp.where(lower_all[v], lanes(skew, 8 * v - 31), 0.0) for v in range(4)]
        high = [jnp.where(lower_all[v], 0.0, lanes(skew, 8 * v + 1)) for v in range(4)]
        for patch in range(len(places)):
            own = slice(8 * patch, 8 * patch + 8)
            block = jnp.concatenate([part[own] for part in low + high], axis=0)
            t_ref[patch, 64 * a1 : 64 * a1 + 64, here] = block.astype(BF16)


def windows(get, p_ref, blocks, count):
    low = between((count, 128), 0, 64)
    tail = between((count, 128), 96, 128)
    for b in blocks:
        tile, place = b // 4, b % 4
        x0, x4 = get(tile, 0), get(tile, 4)
        if place == 0:
            part = jnp.where(low, x0, lanes(x4, 64))
        elif place == 1:
            part = jnp.where(low, lanes(x0, 96), lanes(x4, 32))
        elif place == 2:
            part = jnp.where(low, lanes(x0, 64), x4)
        else:
            w0 = jnp.where(tail, x0, get(tile + 1, 0))
            w4 = jnp.where(tail, x4, get(tile + 1, 4))
            part = jnp.where(low, lanes(w0, 32), lanes(w4, 96))
        p_ref[b, 0:count] = part.astype(BF16)


def blur(segs, groups, taps, p_ref, a_ref, put):
    present = [b for _, blocks in groups for b in blocks]
    for seg, (first, size, padded) in enumerate(segs):
        for patch, blocks in groups:
            lhs = jnp.concatenate(
                [
                    jnp.concatenate(
                        [
                            p_ref[b, first : first + padded],
                            p_ref[b, first + 16 : first + 16 + padded],
                        ],
                        axis=1,
                    )
                    for b in blocks
                ],
                axis=0,
            )
            v = jnp.dot(lhs, taps(seg, patch), preferred_element_type=F32)
            for place, b in enumerate(blocks):
                part = v[place * padded : place * padded + padded]
                a_ref[b, 0:padded] = part[:, :128] + rows(part[:, 128:], -8)
        low = between((padded, 128), 0, 64)
        even = iota((padded, 128), 1) % 64 < 32
        for tile in sorted({b // 4 for b in present}):
            a = [
                a_ref[4 * tile + p, 0:padded]
                if 4 * tile + p in present
                else jnp.zeros((padded, 128), F32)
                for p in range(4)
            ]
            e = []
            for p in range(2):
                z = lanes(jnp.where(low, a[p + 2], a[p]), 64)
                e.append(jnp.where(low, a[p], z) + rows(jnp.where(low, z, a[p + 2]), -2))
            m1 = jnp.where(even, e[0], lanes(e[1], 32))
            m2 = jnp.where(even, lanes(e[0], 96), e[1])
            blurred = (m1 + rows(m2, -1))[0:size]
            put(seg, first, size, tile, blurred)


def adjoint(segs, groups, taps, get, l_ref, f_ref, z_ref, keep):
    present = [b for _, blocks in groups for b in blocks]
    tiles = sorted({b // 4 for b in present})
    for seg, (first, size, padded) in enumerate(segs):
        low = between((padded, 128), 0, 64)
        even = iota((padded, 128), 1) % 64 < 32
        for tile in tiles:
            o = jnp.concatenate(
                [get(first, size, tile), jnp.zeros((padded - size, 128), F32)], axis=0
            )
            o1 = rows(o, 1)
            e = [jnp.where(even, o, lanes(o1, 32)), jnp.where(even, lanes(o, 96), o1)]
            for p in range(2):
                s = rows(e[p], 2)
                for place in (p, p + 2):
                    b = 4 * tile + place
                    if b not in present:
                        continue
                    if place < 2:
                        part = jnp.where(low, e[p], lanes(s, 64))
                    else:
                        part = jnp.where(low, lanes(e[p], 64), s)
                    l_ref[b, 0:padded, 0:128] = part.astype(BF16)
                    l_ref[b, 0:padded, 128:256] = rows(part, 8).astype(BF16)
        for patch, blocks in groups:
            lhs = jnp.concatenate([l_ref[b, 0:padded] for b in blocks], axis=0)
            g = lax.dot_general(
                lhs, taps(seg, patch), (((1,), (1,)), ((), ())), preferred_element_type=F32
            )
            zero = jnp.zeros((16, 128), F32)
            for place, b in enumerate(blocks):
                part = g[place * padded : place * padded + padded]
                f_ref[b, 0:8] = zero[0:8]
                f_ref[b, 8 : padded + 24] = jnp.concatenate(
                    [part[:, :128], zero], axis=0
                ) + jnp.concatenate([zero, part[:, 128:]], axis=0)
                f_ref[b, padded + 24 : padded + 32] = zero[0:8]
        begin, end = max(first, keep[0]), min(first + padded + 24, keep[1])
        tall, skip = end - begin, begin - first
        low = between((tall, 128), 0, 64)
        head = between((tall, 128), 0, 32)

        def both_ways(b):
            if b not in present:
                zero = jnp.zeros((tall, 128), F32)
                return zero, zero
            return f_ref[b, 8 + skip : 8 + skip + tall], f_ref[b, 4 + skip : 4 + skip + tall]

        spill = None
        for tile in tiles:
            both = []
            for p in range(2):
                a0, a8 = both_ways(4 * tile + p)
                b0, b8 = both_ways(4 * tile + p + 2)
                both.append(jnp.where(low, a0, b8) + lanes(jnp.where(low, b0, a8), 64))
            turned = lanes(both[1], 32)
            here = slice(128 * tile, 128 * tile + 128)
            after = slice(128 * tile + 128, 128 * tile + 256)
            span = slice(begin, end)
            if spill is None:
                turned_here = jnp.where(head, 0.0, turned)
            else:
                turned_here = jnp.where(head, spill, turned)
            z_ref[span, here] += both[0] + turned_here
            spill = turned
            if tile < 4 and tile + 1 not in tiles:
                z_ref[span, after] += jnp.where(head, turned, 0.0)
                spill = None


def on_tile(value, tile, change):
    parts = [value[:, 128 * k : 128 * k + 128] for k in range(5)]
    parts[tile] = change(parts[tile])
    return jnp.concatenate(parts, axis=1)


def unless(bad, value):
    return jnp.where(bad, 0.0, value)


def total_variation(get_x, get_q, q1_ref, q2_ref, chunks):
    _, bot_ok, _, right_ok = flags()
    lane = iota((16, 128), 1)
    past = (lane + 512 - XO >= COLS - 1) & jnp.logical_not(right_ok)
    for chunk in chunks:
        start = 16 * chunk
        tall = get_x(start, 24)
        x = tall[0:16]
        g1 = rows(tall, -1)[0:16] - x
        g2 = on_tile(lanes(x, -1) - x, 4, lambda part: unless(past, part))
        if start + 16 > 31 + ROWS:
            row = start - 32 + iota((16, WIDE), 0)
            g1 = unless((row >= ROWS - 1) & jnp.logical_not(bot_ok), g1)
        span = slice(start, start + 16)
        u1 = get_q(0, start) + SIGMA * g1
        u2 = get_q(1, start) + SIGMA * g2
        scale = jnp.minimum(1.0, TV * lax.rsqrt(u1 * u1 + u2 * u2))
        q1_ref[span] = u1 * scale
        q2_ref[span] = u2 * scale


def divergence(q1_ref, q2_ref, start):
    top_ok, bot_ok, left_ok, right_ok = flags()
    above = max(start - 8, 0)
    m1 = q1_ref[above : start + 16]
    m2 = q2_ref[start : start + 16]
    row = above - 32 + iota(m1.shape, 0)
    if above < 32:
        m1 = unless((row < 0) & jnp.logical_not(top_ok), m1)
    if start + 16 > 31 + ROWS:
        m1 = unless((row >= ROWS - 1) & jnp.logical_not(bot_ok), m1)
    lane = iota((16, 128), 1)
    m2 = on_tile(m2, 0, lambda part: unless((lane < XO) & jnp.logical_not(left_ok), part))
    past = (lane + 512 - XO >= COLS - 1) & jnp.logical_not(right_ok)
    m2 = on_tile(m2, 4, lambda part: unless(past, part))
    return (m1 - rows(m1, 1))[start - above :] + (m2 - lanes(m2, 1))


def masks():
    top, bot, left, right = flags()

    def row_ok(seg):
        if seg == 1:
            return jnp.bool_(True)
        return top if seg == 0 else bot

    def col_ok(tile, size):
        lane = iota((size, 128), 1)
        if tile == 0:
            return (lane >= YO) | left
        if tile == 4:
            return (lane < YO) | right
        return jnp.ones((size, 128), jnp.bool_)

    return row_ok, col_ok


def widen(value, shift, width=WIDE):
    pad = jnp.zeros((value.shape[0], width - COLS), F32)
    return lanes(jnp.concatenate([value, pad], axis=1), shift)


def select_tables(table_ref, total, tab_ref):
    onehot = jnp.where(total == iota((64, 128), 0).astype(F32), 1.0, 0.0).astype(BF16)
    picked = lax.dot_general(
        onehot, table_ref[...], (((0,), (0,)), ((), ())), preferred_element_type=F32
    )
    tab_ref[...] = picked[0:24]


def tile_of(value, tile):
    return value[:, 128 * tile : 128 * tile + 128]


def local_kernel(
    x_ref, y_ref, o_ref, q_ref, idx_ref, table_ref,
    xw_ref, cw_ref, ow_ref, q1w_ref, q2w_ref, t_ref,
    tab_ref,
):
    select_tables(table_ref, index_line(idx_ref, 128), tab_ref)
    build_taps(tab_ref, t_ref, range(1, 5))
    xw_ref[...] = widen(x_ref[...], XO, FULL)
    seen = o_ref[...]
    cw_ref[...] = widen(y_ref[...] - SIGMA * seen, YO)
    ow_ref[...] = widen(seen, YO)
    q1w_ref[...] = widen(q_ref[0], XO)
    q2w_ref[...] = widen(q_ref[1], XO)


def middle_kernel(
    xw_ref, cw_ref, ow_ref, q1w_ref, q2w_ref, own_ref, table_ref, ra_ref, rb_ref,
    xe_ref, c_ref, ob_ref, ys_ref, q1_ref, q2_ref, z_ref, t_ref,
    tab_ref, p_ref, a_ref, l_ref, f_ref,
):
    top_ok, bot_ok, _, _ = flags()
    odd, _ = parities()
    top, bot = sides(ra_ref, rb_ref, odd)
    misc = slice(SM, SM + 16)
    lane = iota((1, 128), 1)
    upper = top((misc, slice(0, 128)))[2:3]
    lower = bot((misc, slice(0, 128)))[2:3]
    select_tables(table_ref, jnp.where(lane < 8, upper, lanes(lower, 8)), tab_ref)
    build_taps(tab_ref, t_ref, [1, 2, 3, 4, 9, 10, 11, 12])

    def part(read, at, count):
        return read(slice(at, at + count))

    zero = jnp.zeros((48, COLS), F32)
    above = part(top, SX, 64) + jnp.concatenate([zero, part(top, SXL, 16)], axis=0)
    below = part(bot, SX, 64) + jnp.concatenate([part(bot, SXL, 16), zero], axis=0)
    xe_ref[0:64] = widen(jnp.where(top_ok, above, 0.0), XO, FULL)
    xe_ref[64:192] = xw_ref[...]
    xe_ref[192:256] = widen(jnp.where(bot_ok, below, 0.0), XO, FULL)
    xe_ref[256:272] = jnp.zeros((16, FULL), F32)
    c_ref[48:176] = cw_ref[...]
    ob_ref[16:144] = ow_ref[...]
    zero = jnp.zeros((32, COLS), F32)
    above = part(top, SC, 48) + jnp.concatenate([zero, part(top, SCL, 16)], axis=0)
    below = part(bot, SC, 48) + jnp.concatenate([part(bot, SCL, 16), zero], axis=0)
    c_ref[0:48] = widen(above, YO)
    c_ref[176:224] = widen(below, YO)
    ob_ref[0:16] = widen(part(top, SO, 16), YO)
    ob_ref[144:160] = widen(part(bot, SO, 16), YO)
    rix = iota((32, COLS), 0)
    rest = top(misc)
    for comp, (ref, section, own) in enumerate(((q1_ref, S1, q1w_ref), (q2_ref, S2, q2w_ref))):
        above = part(top, section, 32) + jnp.where(rix == 31, rest[comp : comp + 1], 0.0)
        ref[0:32] = widen(above, XO)
        ref[32:160] = own[...]
        ref[160:192] = widen(part(bot, section, 32), XO)
    row_ok, _ = masks()

    def taps(seg, patch):
        return own_ref[patch] if seg == 1 else t_ref[2 * seg + patch]

    def get_x(tile, first):
        return xe_ref[first : first + 256, 128 * tile : 128 * tile + 128]

    def put(seg, first, size, tile, blurred):
        here = slice(128 * tile, 128 * tile + 128)
        new = (c_ref[first : first + size, here] + SIGMA * blurred) * (1.0 / (1.0 + SIGMA))
        ys_ref[first : first + size, here] = new if seg == 1 else jnp.where(row_ok(seg), new, 0.0)

    def get_y(first, size, tile):
        return ys_ref[first : first + size, 128 * tile : 128 * tile + 128]

    windows(get_x, p_ref, range(3, 17), 256)
    blur(SEGS1, INNER, taps, p_ref, a_ref, put)
    z_ref[...] = jnp.zeros_like(z_ref)
    adjoint(SEGS1, INNER, taps, get_y, l_ref, f_ref, z_ref, (32, 224))


def main_kernel(
    table_ref, ca_ref, cb_ref,
    xi_ref, ci_ref, oi_ref, yi_ref, q1i_ref, q2i_ref, zi_ref, ti_ref, own_ref,
    x2_ref, y2_hbm,
    side_ref, qs_ref, ys_ref, c_ref, q1_ref, q2_ref, tab_ref, t_ref, p_ref, a_ref, l_ref, f_ref,
    z_ref, xb_ref, x1_ref, y2_ref, sem,
):
    top_ok, bot_ok, left_ok, right_ok = flags()
    _, odd_col = parities()
    before, after = sides(ca_ref, cb_ref, odd_col)
    first, second = slice(0, 256), slice(256, 448)
    lf0, lf1, rt0, rt1 = before(first), before(second), after(first), after(second)
    gap = jnp.zeros((48, 128), F32)

    def from_row(value, count):
        return jnp.concatenate([gap[: count // 2 - 80], value[0:160], gap[: count // 2 - 80]], axis=0)

    lane = iota((1, 128), 1)
    total = jnp.full((1, 128), -1.0, F32)
    for r in range(3):
        total = jnp.where(lane == 8 * r, lf1[r : r + 1, 18:19], total)
        total = jnp.where(lane == 8 * r + 5, rt1[r : r + 1, 112:113], total)
    select_tables(table_ref, total, tab_ref)
    build_taps(tab_ref, t_ref, [8 * r + p for r in range(3) for p in (0, 5)])

    def taps(seg, patch):
        if 0 <= patch < 4:
            return own_ref[patch] if seg == 1 else ti_ref[2 * seg + patch]
        return t_ref[2 * seg + (patch == 4)]

    rr = iota((256, 128), 0)
    rows_ok = ((rr >= 64) | top_ok) & ((rr < 192) | bot_ok)
    shape = (256, 128)
    part = jnp.where(between(shape, 16, 80), lf0, 0.0)
    part += jnp.where(between(shape, 64, 80), lanes(from_row(lf1, 256), 80), 0.0)
    side_ref[0, 0:256] = xi_ref[0:256, 0:128] + jnp.where(rows_ok & left_ok, part, 0.0)
    part = jnp.where(between(shape, 80, 128), rt0, 0.0)
    part += jnp.where(between(shape, 80, 96), lanes(from_row(rt1, 256), 48), 0.0)
    side_ref[1, 0:256] = xi_ref[0:256, 512:640] + jnp.where(rows_ok & right_ok, part, 0.0)
    part = jnp.where(between(shape, 0, 16), rt0, 0.0)
    side_ref[2, 0:256] = xi_ref[0:256, 640:768] + jnp.where(rows_ok & right_ok, part, 0.0)
    side_ref[:, 256:272] = jnp.zeros((3, 16, 128), F32)
    shape = (192, 128)
    for comp, ref in enumerate((q1i_ref, q2i_ref)):
        part = lanes(lf1[0:192], 96 * comp)
        part += jnp.where(between(shape, 79, 80), lanes(lf1[0:192], 63 - comp), 0.0)
        qs_ref[comp, 0] = jnp.where(between(shape, 48, 80), part, ref[:, 0:128])
        part = lanes(rt1[0:192], 80 * comp)
        qs_ref[comp, 1] = jnp.where(between(shape, 80, 112), part, ref[:, 512:640])
    shape = (224, 128)
    part = lanes(lf0[0:224], 64) + jnp.where(between(shape, 48, 64), lanes(from_row(lf1, 224), 48), 0.0)
    c_first = jnp.where(between(shape, 16, 64), part, ci_ref[:, 0:128])
    part = lanes(rt0[0:224], 48) + jnp.where(between(shape, 64, 80), from_row(rt1, 224), 0.0)
    c_last = jnp.where(between(shape, 64, 112), part, ci_ref[:, 512:640])
    shape = (160, 128)
    o_first = jnp.where(between(shape, 48, 64), lanes(lf0[0:160], 48), oi_ref[:, 0:128])
    o_last = jnp.where(between(shape, 64, 80), rt0[0:160], oi_ref[:, 512:640])
    row_ok, col_ok = masks()

    def get_side(tile, first):
        which = {0: 0, 4: 1, 5: 2}[tile]
        return side_ref[which, first : first + 256]

    def put_side(seg, first, size, tile, blurred):
        c = (c_first if tile == 0 else c_last)[first : first + size]
        new = (c + SIGMA * blurred) * (1.0 / (1.0 + SIGMA))
        new = jnp.where(col_ok(tile, size) & row_ok(seg), new, 0.0)
        old = yi_ref[first : first + size, 128 * tile : 128 * tile + 128]
        inner = between((size, 128), 96, 128) if tile == 0 else between((size, 128), 0, 32)
        ys_ref[tile // 4, first : first + size] = jnp.where(inner, old, new)

    def get_side_y(first, size, tile):
        return ys_ref[tile // 4, first : first + size]

    windows(get_side, p_ref, (0, 1, 2, 17, 18, 19), 256)
    blur(SEGS1, OUTER, taps, p_ref, a_ref, put_side)

    def get_x(start, count):
        at = slice(32 + start, 32 + start + count)
        return jnp.concatenate([side_ref[0, at], xi_ref[at, 128:512], side_ref[1, at]], axis=1)

    def get_q(comp, start):
        at = slice(start, start + 16)
        ref = q2i_ref if comp else q1i_ref
        return jnp.concatenate([qs_ref[comp, 0, at], ref[at, 128:512], qs_ref[comp, 1, at]], axis=1)

    total_variation(get_x, get_q, q1_ref, q2_ref, range(12))
    z_ref[32:224] = zi_ref[32:224]
    adjoint(SEGS1, OUTER, taps, get_side_y, l_ref, f_ref, z_ref, (32, 224))
    lane = iota((16, 128), 1)
    for chunk in range(12):
        start = 16 * chunk
        ext = slice(32 + start, 48 + start)
        x = get_x(start, 16)
        new = x - TAU * (z_ref[ext, 0:WIDE] - divergence(q1_ref, q2_ref, start))
        ahead = 2.0 * new - x
        ahead = on_tile(ahead, 0, lambda part: unless((lane < XO) & jnp.logical_not(left_ok), part))
        past = (lane + 512 - XO >= COLS) & jnp.logical_not(right_ok)
        ahead = on_tile(ahead, 4, lambda part: unless(past, part))
        if chunk < 2 or chunk >= 10:
            ahead = jnp.where(top_ok if chunk < 2 else bot_ok, ahead, 0.0)
        xb_ref[start : start + 16, 0:WIDE] = ahead
        if 2 <= chunk < 10:
            x1_ref[start - 32 : start - 16] = new
    xb_ref[192:208, 0:WIDE] = jnp.zeros((16, WIDE), F32)
    xb_ref[:, WIDE:FULL] = jnp.zeros((208, FULL - WIDE), F32)
    c_ref[:, 0:128] = ys_ref[0, 32:192] - SIGMA * o_first
    c_ref[:, 128:512] = yi_ref[32:192, 128:512] - SIGMA * oi_ref[:, 128:512]
    c_ref[:, 512:640] = ys_ref[1, 32:192] - SIGMA * o_last

    def get_xb(tile, first):
        return xb_ref[first : first + 192, 128 * tile : 128 * tile + 128]

    def put(seg, first, size, tile, blurred):
        here = slice(128 * tile, 128 * tile + 128)
        new = (c_ref[first : first + size, here] + SIGMA * blurred) * (1.0 / (1.0 + SIGMA))
        if seg != 1 or tile in (0, 4):
            new = jnp.where(col_ok(tile, size) & row_ok(seg), new, 0.0)
        c_ref[first : first + size, here] = new

    def get_y(first, size, tile):
        return c_ref[first : first + size, 128 * tile : 128 * tile + 128]

    windows(get_xb, p_ref, range(1, 19), 192)
    blur(SEGS2, ALL, taps, p_ref, a_ref, put)
    for chunk in range(8):
        span = slice(16 * chunk, 16 * chunk + 16)
        y2_ref[span] = lanes(c_ref[16 + 16 * chunk : 32 + 16 * chunk], -YO)[:, :COLS]
    total_variation(
        lambda start, count: xb_ref[start : start + count, 0:WIDE],
        lambda comp, start: (q2_ref if comp else q1_ref)[start : start + 16],
        q1_ref, q2_ref, range(1, 10),
    )
    done = pltpu.make_async_copy(y2_ref, y2_hbm, sem.at[0])
    done.start()
    z_ref[32:160] = jnp.zeros((128, WIDE), F32)
    adjoint(SEGS2, ALL, taps, get_y, l_ref, f_ref, z_ref, (32, 160))
    for chunk in range(8):
        span = slice(16 * chunk, 16 * chunk + 16)
        ext = slice(32 + 16 * chunk, 48 + 16 * chunk)
        div = divergence(q1_ref, q2_ref, 32 + 16 * chunk)
        new = x1_ref[span] - TAU * (z_ref[ext, 0:WIDE] - div)
        x2_ref[span] = lanes(new, -XO)[:, :COLS]
    done.wait()


def field(*shape, dtype=F32):
    return jax.ShapeDtypeStruct(shape, dtype)


def call(kernel, outs, scratch, *args, name, room=4, far=0, flops=0, out_far=0):
    spaces = [pltpu.HBM] * far + [pltpu.VMEM] * (len(args) - far)
    return pl.pallas_call(
        kernel,
        out_shape=outs,
        out_specs=tuple(
            pl.BlockSpec(memory_space=pltpu.HBM if i >= len(outs) - out_far else pltpu.VMEM)
            for i in range(len(outs))
        ),
        in_specs=[pl.BlockSpec(memory_space=space) for space in spaces],
        scratch_shapes=scratch,
        compiler_params=pltpu.CompilerParams(vmem_limit_bytes=int(room * 1024 * 1024)),
        cost_estimate=pl.CostEstimate(flops=flops, bytes_accessed=0, transcendentals=0)
        if flops
        else None,
        name=name,
    )(*args)


def swap(block, axis, first):
    high, wide = lax.axis_size("row"), lax.axis_size("col")

    def partner(row, col):
        if axis == "row":
            to = ((row - first) ^ 1) + first
            return (to, col) if 0 <= to < high else (row, col ^ 2 if wide > 2 else col ^ 1)
        to = ((col - first) ^ 1) + first
        return (row, to) if 0 <= to < wide else (row ^ 1, col)

    pairs = []
    for row in range(high):
        for col in range(wide):
            to_row, to_col = partner(row, col)
            pairs.append((row * wide + col, to_row * wide + to_col))
    return lax.ppermute(block, ("row", "col"), pairs)


def per_device(observed, psf_table, psf_index, start_image, blur_dual, tv_dual):
    own = (start_image, blur_dual, observed, tv_dual)
    block = pltpu.VMEM((ROWS, COLS), F32)
    strip = field(STRIP, COLS, dtype=BF16)
    side = field(448, 128, dtype=BF16)
    a, b = call(
        pack_rows_kernel, (strip, strip),
        [block, block, block, pltpu.VMEM((2, ROWS, COLS), F32), pltpu.SemaphoreType.DMA((4,))],
        *own, psf_index, name="pack_rows", far=4, room=53.3,
    )
    ra = swap(a, "row", 0)
    rb = swap(b, "row", 1)
    table = psf_table.astype(F32)
    normed = (table / jnp.sum(table, axis=(1, 2), keepdims=True)).astype(BF16)
    normed = jnp.pad(normed[:, :, ::-1], ((0, 0), (1, 0), (0, 1))).reshape(64, 1024)
    a, b = call(
        pack_cols_kernel, (side, side), [], *own, psf_index, ra, rb, name="pack_cols"
    )
    ca = swap(a, "col", 0)
    cb = swap(b, "col", 1)
    work = [
        pltpu.VMEM((20, 256, 128), BF16), pltpu.VMEM((20, 144, 128), F32),
        pltpu.VMEM((20, 144, 256), BF16), pltpu.VMEM((20, 176, 128), F32),
    ]
    wide = field(192, WIDE)
    local = field(ROWS, WIDE)
    *fields, taps = call(
        local_kernel,
        (field(ROWS, FULL), local, local, local, local, field(4, 256, 256, dtype=BF16)),
        [pltpu.VMEM((24, 1024), F32)],
        *own, psf_index, normed, name="local", room=4, flops=1 << 32,
    )
    ready = call(
        middle_kernel,
        (
            field(272, FULL), field(224, WIDE), field(160, WIDE), field(224, WIDE), wide, wide,
            field(224, WIDE), field(8, 256, 256, dtype=BF16),
        ),
        [pltpu.VMEM((24, 1024), F32)] + work,
        *fields, taps, normed, ra, rb, name="middle", room=16, flops=1 << 33,
    )
    return call(
        main_kernel,
        (field(ROWS, COLS), field(ROWS, COLS)),
        [
            pltpu.VMEM((3, 272, 128), F32), pltpu.VMEM((2, 2, 192, 128), F32),
            pltpu.VMEM((2, 224, 128), F32), pltpu.VMEM((160, WIDE), F32),
            pltpu.VMEM((192, WIDE), F32), pltpu.VMEM((192, WIDE), F32),
            pltpu.VMEM((24, 1024), F32), pltpu.VMEM((6, 256, 256), BF16),
        ] + work + [
            pltpu.VMEM((224, WIDE), F32), pltpu.VMEM((208, FULL), F32), pltpu.VMEM((ROWS, WIDE), F32),
            pltpu.VMEM((ROWS, COLS), F32), pltpu.SemaphoreType.DMA((1,)),
        ],
        normed, ca, cb, *ready, taps, name="main", room=20, out_far=1,
    )


def solution(mesh):
    placed = (
        P("row", "col"),
        P(),
        P("row", "col"),
        P("row", "col"),
        P("row", "col"),
        P(None, "row", "col"),
    )
    return jax.shard_map(
        per_device,
        mesh=mesh,
        in_specs=placed,
        out_specs=(P("row", "col"), P("row", "col")),
        check_vma=False,
    )
```

```python
import jax
import jax.numpy as jnp
from jax import lax
from jax.experimental import pallas as pl
from jax.experimental.pallas import tpu as pltpu
from jax.sharding import PartitionSpec as P

SIGMA = 0.15
TAU = 0.6
TV = 0.5
F32 = jnp.float32
BF16 = jnp.bfloat16

ROWS = 128
COLS = 512
XO = 80
YO = 64
WIDE = 640
FULL = 768
SEGS1 = ((0, 48, 64), (48, 128, 144), (176, 48, 64))
SEGS2 = ((0, 16, 32), (16, 128, 144), (144, 16, 32))
PATCHES2 = ((1,), (2, 3, 4, 5), (6, 7, 8, 9), (10, 11, 12, 13), (14, 15, 16, 17), (18,))
INNER = ((0, (3, 4, 5)), (1, (6, 7, 8, 9)), (2, (10, 11, 12, 13)), (3, (14, 15, 16)))
OUTER = ((-1, (0, 1)), (0, (2,)), (3, (17,)), (4, (18, 19)))
ALL = tuple((patch - 1, blocks) for patch, blocks in enumerate(PATCHES2))
SX, SXL, SC, SCL, SO, S1, S2, SM, STRIP = 0, 64, 80, 128, 144, 160, 192, 224, 240


def iota(shape, dim):
    return lax.broadcasted_iota(jnp.int32, shape, dim)


def split(value):
    hi = value.astype(BF16).astype(F32)
    return hi, value - hi


def lanes(value, shift):
    shift = shift % value.shape[1]
    return pltpu.roll(value, shift, 1) if shift else value


def rows(value, shift):
    shift = shift % value.shape[0]
    return pltpu.roll(value, shift, 0) if shift else value


def between(shape, lo, hi):
    lane = iota(shape, 1)
    return (lane >= lo) & (lane < hi)


def flags():
    row = lax.axis_index("row")
    col = lax.axis_index("col")
    return (
        row > 0,
        row < lax.axis_size("row") - 1,
        col > 0,
        col < lax.axis_size("col") - 1,
    )


def index_line(idx_ref, width):
    lane = iota((1, width), 1)
    line = jnp.zeros((1, width), F32)
    for j in range(4):
        line = jnp.where(lane == 1 + j, idx_ref[0:1, j : j + 1].astype(F32), line)
    return line


def parities():
    return lax.axis_index("row") % 2 == 1, lax.axis_index("col") % 2 == 1


def chosen(flag, one_ref, two_ref):
    def read(at):
        return jnp.where(flag, one_ref[at].astype(F32), two_ref[at].astype(F32))

    return read


def sides(a_ref, b_ref, odd):
    return chosen(odd, a_ref, b_ref), chosen(odd, b_ref, a_ref)


def pack_rows_kernel(x_hbm, y_hbm, o_hbm, q_hbm, idx_ref, a_ref, b_ref, x_ref, y_ref, o_ref, q_ref, sems):
    copies = [
        pltpu.make_async_copy(src, dst, sems.at[i])
        for i, (src, dst) in enumerate(((x_hbm, x_ref), (y_hbm, y_ref), (o_hbm, o_ref), (q_hbm, q_ref)))
    ]
    for copy in copies:
        copy.start()
    line = index_line(idx_ref, COLS)
    odd, _ = parities()

    def put(at, count, down, up):
        a_ref[at : at + count] = jnp.where(odd, up, down).astype(BF16)
        b_ref[at : at + count] = jnp.where(odd, down, up).astype(BF16)

    copies[0].wait()
    put(SX, 64, x_ref[64:128], x_ref[0:64])
    put(SXL, 16, split(x_ref[112:128])[1], split(x_ref[0:16])[1])
    copies[1].wait()
    copies[2].wait()
    up = y_ref[0:48] - SIGMA * o_ref[0:48]
    down = y_ref[80:128] - SIGMA * o_ref[80:128]
    put(SC, 48, down, up)
    put(SCL, 16, split(down[32:48])[1], split(up[0:16])[1])
    put(SO, 16, o_ref[112:128], o_ref[0:16])
    copies[3].wait()
    put(S1, 32, q_ref[0, 96:128], q_ref[0, 0:32])
    put(S2, 32, q_ref[1, 96:128], q_ref[1, 0:32])
    row = iota((16, COLS), 0)
    rest = []
    for edge in (127, 0):
        misc = jnp.zeros((16, COLS), F32)
        for comp in range(2):
            misc = jnp.where(row == comp, split(q_ref[comp, edge : edge + 1])[1], misc)
        rest.append(jnp.where(row == 2, line, misc))
    put(SM, 16, *rest)


def pack_cols_kernel(x_ref, y_ref, o_ref, q_ref, idx_ref, ra_ref, rb_ref, a_ref, b_ref):
    odd_row, odd_col = parities()
    top, bot = sides(ra_ref, rb_ref, odd_row)
    made = []
    for base in (384, 0):
        right = base > 0
        own = slice(base, base + 128)

        def strip(read, at, count, own=own):
            return read((slice(at, at + count), own))

        def column(middle, at, count, shift):
            parts = [strip(top, at, count), middle, strip(bot, at, count)]
            return lanes(jnp.concatenate(parts, axis=0), shift)

        seen = o_ref[:, own]
        x_hi, x_lo = split(x_ref[:, own])
        c_hi, c_lo = split(y_ref[:, own] - SIGMA * seen)
        zeros = jnp.zeros((128, 128), F32)
        buf = column(x_hi, SX, 64, 80)
        part = jnp.concatenate([column(c_hi, SC, 48, 0 if right else 16), zeros[:32]], axis=0)
        at = 80 if right else 16
        buf = jnp.where(between((256, 128), at, at + 48), part, buf)
        part = jnp.concatenate([column(seen, SO, 16, 16 if right else 64), zeros[:96]], axis=0)
        at = 0 if right else 64
        buf = jnp.where(between((256, 128), at, at + 16), part, buf)
        made.append(buf)
        buf = jnp.concatenate([column(q_ref[0, :, own], S1, 32, 80)], axis=0)
        part = jnp.concatenate(
            [column(q_ref[1, :, own], S2, 32, 112 if right else 0)], axis=0
        )
        at = 80 if right else 0
        buf = jnp.where(between((192, 128), at, at + 32), part, buf)
        shift = 0 if right else 32
        part = jnp.concatenate(
            [
                lanes(strip(top, SXL, 16), shift),
                lanes(x_lo, shift),
                lanes(strip(bot, SXL, 16), shift),
                zeros[:32],
            ],
            axis=0,
        )
        at = 112 if right else 32
        buf = jnp.where(between((192, 128), at, at + 16), part, buf)
        shift = 16 if right else 64
        part = jnp.concatenate(
            [
                lanes(strip(top, SCL, 16), shift),
                lanes(c_lo, shift),
                lanes(strip(bot, SCL, 16), shift),
                zeros[:32],
            ],
            axis=0,
        )
        at = 0 if right else 64
        buf = jnp.where(between((192, 128), at, at + 16), part, buf)
        if right:
            for comp in range(2):
                low = lanes(split(q_ref[comp, :, own])[1], 17 + comp)
                part = jnp.concatenate([zeros[:32], low, zeros[:32]], axis=0)
                buf = jnp.where(between((192, 128), 16 + comp, 17 + comp), part, buf)
        row = iota((192, 1), 0)
        spot = 4 if right else 1
        first = top((slice(SM, SM + 16), slice(0, 128)))[2:3, spot : spot + 1]
        last = bot((slice(SM, SM + 16), slice(0, 128)))[2:3, spot : spot + 1]
        mine = idx_ref[0:1, spot - 1 : spot].astype(F32)
        entry = jnp.where(row == 0, first, jnp.where(row == 1, mine, last))
        at = 18 if right else 112
        buf = jnp.where(between((192, 128), at, at + 1), entry, buf)
        made.append(buf)
    for tile, span in enumerate((slice(0, 256), slice(256, 448))):
        a_ref[span] = jnp.where(odd_col, made[2 + tile], made[tile]).astype(BF16)
        b_ref[span] = jnp.where(odd_col, made[tile], made[2 + tile]).astype(BF16)


def build_taps(tab_ref, t_ref, places):
    size = 8 * len(places)
    sub = iota((size, 128), 0)
    bits = [(sub // (1 << n)) % 2 == 1 for n in range(3)]
    for e in range(8):
        a1, half = 2 * (e // 4) + e % 2, e // 2 % 2
        here = slice(128 * half, 128 * half + 128)
        skew = jnp.concatenate(
            [
                jnp.broadcast_to(
                    tab_ref[at : at + 1, 128 * e : 128 * e + 128], (8, 128)
                )
                for at in places
            ],
            axis=0,
        )
        for n in range(3):
            skew = jnp.where(bits[n], lanes(skew, 1 << n), skew)
        lower_all = [iota((size, 128), 1) % 32 <= sub % 8 + 8 * v for v in range(4)]
        low = [jnp.where(lower_all[v], lanes(skew, 8 * v - 31), 0.0) for v in range(4)]
        high = [jnp.where(lower_all[v], 0.0, lanes(skew, 8 * v + 1)) for v in range(4)]
        for patch in range(len(places)):
            own = slice(8 * patch, 8 * patch + 8)
            block = jnp.concatenate([part[own] for part in low + high], axis=0)
            t_ref[patch, 64 * a1 : 64 * a1 + 64, here] = block.astype(BF16)


def windows(get, p_ref, blocks, count):
    low = between((count, 128), 0, 64)
    tail = between((count, 128), 96, 128)
    for b in blocks:
        tile, place = b // 4, b % 4
        x0, x4 = get(tile, 0), get(tile, 4)
        if place == 0:
            part = jnp.where(low, x0, lanes(x4, 64))
        elif place == 1:
            part = jnp.where(low, lanes(x0, 96), lanes(x4, 32))
        elif place == 2:
            part = jnp.where(low, lanes(x0, 64), x4)
        else:
            w0 = jnp.where(tail, x0, get(tile + 1, 0))
            w4 = jnp.where(tail, x4, get(tile + 1, 4))
            part = jnp.where(low, lanes(w0, 32), lanes(w4, 96))
        p_ref[b, 0:count] = part.astype(BF16)


def blur(segs, groups, taps, p_ref, a_ref, put):
    present = [b for _, blocks in groups for b in blocks]
    for seg, (first, size, padded) in enumerate(segs):
        for patch, blocks in groups:
            lhs = jnp.concatenate(
                [
                    jnp.concatenate(
                        [
                            p_ref[b, first : first + padded],
                            p_ref[b, first + 16 : first + 16 + padded],
                        ],
                        axis=1,
                    )
                    for b in blocks
                ],
                axis=0,
            )
            v = jnp.dot(lhs, taps(seg, patch), preferred_element_type=F32)
            for place, b in enumerate(blocks):
                part = v[place * padded : place * padded + padded]
                a_ref[b, 0:padded] = part[:, :128] + rows(part[:, 128:], -8)
        low = between((padded, 128), 0, 64)
        even = iota((padded, 128), 1) % 64 < 32
        for tile in sorted({b // 4 for b in present}):
            a = [
                a_ref[4 * tile + p, 0:padded]
                if 4 * tile + p in present
                else jnp.zeros((padded, 128), F32)
                for p in range(4)
            ]
            e = []
            for p in range(2):
                z = lanes(jnp.where(low, a[p + 2], a[p]), 64)
                e.append(jnp.where(low, a[p], z) + rows(jnp.where(low, z, a[p + 2]), -2))
            m1 = jnp.where(even, e[0], lanes(e[1], 32))
            m2 = jnp.where(even, lanes(e[0], 96), e[1])
            blurred = (m1 + rows(m2, -1))[0:size]
            put(seg, first, size, tile, blurred)


def adjoint(segs, groups, taps, get, l_ref, f_ref, z_ref, keep):
    present = [b for _, blocks in groups for b in blocks]
    tiles = sorted({b // 4 for b in present})
    for seg, (first, size, padded) in enumerate(segs):
        low = between((padded, 128), 0, 64)
        even = iota((padded, 128), 1) % 64 < 32
        for tile in tiles:
            o = jnp.concatenate(
                [get(first, size, tile), jnp.zeros((padded - size, 128), F32)], axis=0
            )
            o1 = rows(o, 1)
            e = [jnp.where(even, o, lanes(o1, 32)), jnp.where(even, lanes(o, 96), o1)]
            for p in range(2):
                s = rows(e[p], 2)
                for place in (p, p + 2):
                    b = 4 * tile + place
                    if b not in present:
                        continue
                    if place < 2:
                        part = jnp.where(low, e[p], lanes(s, 64))
                    else:
                        part = jnp.where(low, lanes(e[p], 64), s)
                    l_ref[b, 0:padded, 0:128] = part.astype(BF16)
                    l_ref[b, 0:padded, 128:256] = rows(part, 8).astype(BF16)
        for patch, blocks in groups:
            lhs = jnp.concatenate([l_ref[b, 0:padded] for b in blocks], axis=0)
            g = lax.dot_general(
                lhs, taps(seg, patch), (((1,), (1,)), ((), ())), preferred_element_type=F32
            )
            zero = jnp.zeros((16, 128), F32)
            for place, b in enumerate(blocks):
                part = g[place * padded : place * padded + padded]
                f_ref[b, 0:8] = zero[0:8]
                f_ref[b, 8 : padded + 24] = jnp.concatenate(
                    [part[:, :128], zero], axis=0
                ) + jnp.concatenate([zero, part[:, 128:]], axis=0)
                f_ref[b, padded + 24 : padded + 32] = zero[0:8]
        begin, end = max(first, keep[0]), min(first + padded + 24, keep[1])
        tall, skip = end - begin, begin - first
        low = between((tall, 128), 0, 64)
        head = between((tall, 128), 0, 32)

        def both_ways(b):
            if b not in present:
                zero = jnp.zeros((tall, 128), F32)
                return zero, zero
            return f_ref[b, 8 + skip : 8 + skip + tall], f_ref[b, 4 + skip : 4 + skip + tall]

        spill = None
        for tile in tiles:
            both = []
            for p in range(2):
                a0, a8 = both_ways(4 * tile + p)
                b0, b8 = both_ways(4 * tile + p + 2)
                both.append(jnp.where(low, a0, b8) + lanes(jnp.where(low, b0, a8), 64))
            turned = lanes(both[1], 32)
            here = slice(128 * tile, 128 * tile + 128)
            after = slice(128 * tile + 128, 128 * tile + 256)
            span = slice(begin, end)
            if spill is None:
                turned_here = jnp.where(head, 0.0, turned)
            else:
                turned_here = jnp.where(head, spill, turned)
            z_ref[span, here] += both[0] + turned_here
            spill = turned
            if tile < 4 and tile + 1 not in tiles:
                z_ref[span, after] += jnp.where(head, turned, 0.0)
                spill = None


def on_tile(value, tile, change):
    parts = [value[:, 128 * k : 128 * k + 128] for k in range(5)]
    parts[tile] = change(parts[tile])
    return jnp.concatenate(parts, axis=1)


def unless(bad, value):
    return jnp.where(bad, 0.0, value)


CHUNK = 32


def chunks(first, count, body):
    def step(i, carry):
        body(pl.multiple_of(first + CHUNK * i, CHUNK))
        return carry

    lax.fori_loop(0, count // CHUNK, step, 0)


def total_variation(get_x, get_q, q1_ref, q2_ref, count):
    _, bot_ok, _, right_ok = flags()

    def body(start):
        lane = iota((CHUNK, 128), 1)
        past = (lane + 512 - XO >= COLS - 1) & jnp.logical_not(right_ok)
        tall = get_x(start, CHUNK + 8)
        x = tall[0:CHUNK]
        row = start - 32 + iota((CHUNK, WIDE), 0)
        g1 = unless((row >= ROWS - 1) & jnp.logical_not(bot_ok), rows(tall, -1)[0:CHUNK] - x)
        g2 = on_tile(lanes(x, -1) - x, 4, lambda part: unless(past, part))
        u1 = get_q(0, start) + SIGMA * g1
        u2 = get_q(1, start) + SIGMA * g2
        scale = jnp.minimum(1.0, TV * lax.rsqrt(u1 * u1 + u2 * u2))
        q1_ref[pl.ds(start + 8, CHUNK)] = u1 * scale
        q2_ref[pl.ds(start + 8, CHUNK)] = u2 * scale

    chunks(0, count, body)


def divergence(q1_ref, q2_ref, start):
    top_ok, bot_ok, left_ok, right_ok = flags()
    m1 = q1_ref[pl.ds(start, CHUNK + 8)]
    m2 = q2_ref[pl.ds(start + 8, CHUNK)]
    row = start - 40 + iota(m1.shape, 0)
    out = ((row < 0) & jnp.logical_not(top_ok)) | ((row >= ROWS - 1) & jnp.logical_not(bot_ok))
    m1 = unless(out, m1)
    lane = iota((CHUNK, 128), 1)
    m2 = on_tile(m2, 0, lambda part: unless((lane < XO) & jnp.logical_not(left_ok), part))
    past = (lane + 512 - XO >= COLS - 1) & jnp.logical_not(right_ok)
    m2 = on_tile(m2, 4, lambda part: unless(past, part))
    return (m1 - rows(m1, 1))[8:] + (m2 - lanes(m2, 1))


def masks():
    top, bot, left, right = flags()

    def row_ok(seg):
        if seg == 1:
            return jnp.bool_(True)
        return top if seg == 0 else bot

    def col_ok(tile, size):
        lane = iota((size, 128), 1)
        if tile == 0:
            return (lane >= YO) | left
        if tile == 4:
            return (lane < YO) | right
        return jnp.ones((size, 128), jnp.bool_)

    return row_ok, col_ok


def widen(value, shift, width=WIDE):
    pad = jnp.zeros((value.shape[0], width - COLS), F32)
    return lanes(jnp.concatenate([value, pad], axis=1), shift)


def select_tables(table_ref, total, tab_ref):
    onehot = jnp.where(total == iota((64, 128), 0).astype(F32), 1.0, 0.0).astype(BF16)
    picked = lax.dot_general(
        onehot, table_ref[...], (((0,), (0,)), ((), ())), preferred_element_type=F32
    )
    tab_ref[...] = picked[0:24]


def tile_of(value, tile):
    return value[:, 128 * tile : 128 * tile + 128]


def local_kernel(
    x_ref, y_ref, o_ref, q_ref, idx_ref, table_ref,
    xw_ref, cw_ref, ow_ref, q1w_ref, q2w_ref, t_ref,
    tab_ref,
):
    select_tables(table_ref, index_line(idx_ref, 128), tab_ref)
    build_taps(tab_ref, t_ref, range(1, 5))
    xw_ref[...] = widen(x_ref[...], XO, FULL)
    seen = o_ref[...]
    cw_ref[...] = widen(y_ref[...] - SIGMA * seen, YO)
    ow_ref[...] = widen(seen, YO)
    q1w_ref[...] = widen(q_ref[0], XO)
    q2w_ref[...] = widen(q_ref[1], XO)


def middle_kernel(
    xw_ref, cw_ref, ow_ref, q1w_ref, q2w_ref, own_ref, table_ref, ra_ref, rb_ref,
    xe_ref, c_ref, ob_ref, ys_ref, q1_ref, q2_ref, z_ref, t_ref,
    tab_ref, p_ref, a_ref, l_ref, f_ref,
):
    top_ok, bot_ok, _, _ = flags()
    odd, _ = parities()
    top, bot = sides(ra_ref, rb_ref, odd)
    misc = slice(SM, SM + 16)
    lane = iota((1, 128), 1)
    upper = top((misc, slice(0, 128)))[2:3]
    lower = bot((misc, slice(0, 128)))[2:3]
    select_tables(table_ref, jnp.where(lane < 8, upper, lanes(lower, 8)), tab_ref)
    build_taps(tab_ref, t_ref, [1, 2, 3, 4, 9, 10, 11, 12])

    def part(read, at, count):
        return read(slice(at, at + count))

    zero = jnp.zeros((48, COLS), F32)
    above = part(top, SX, 64) + jnp.concatenate([zero, part(top, SXL, 16)], axis=0)
    below = part(bot, SX, 64) + jnp.concatenate([part(bot, SXL, 16), zero], axis=0)
    xe_ref[0:64] = widen(jnp.where(top_ok, above, 0.0), XO, FULL)
    xe_ref[64:192] = xw_ref[...]
    xe_ref[192:256] = widen(jnp.where(bot_ok, below, 0.0), XO, FULL)
    xe_ref[256:272] = jnp.zeros((16, FULL), F32)
    c_ref[48:176] = cw_ref[...]
    ob_ref[16:144] = ow_ref[...]
    zero = jnp.zeros((32, COLS), F32)
    above = part(top, SC, 48) + jnp.concatenate([zero, part(top, SCL, 16)], axis=0)
    below = part(bot, SC, 48) + jnp.concatenate([part(bot, SCL, 16), zero], axis=0)
    c_ref[0:48] = widen(above, YO)
    c_ref[176:224] = widen(below, YO)
    ob_ref[0:16] = widen(part(top, SO, 16), YO)
    ob_ref[144:160] = widen(part(bot, SO, 16), YO)
    rix = iota((32, COLS), 0)
    rest = top(misc)
    for comp, (ref, section, own) in enumerate(((q1_ref, S1, q1w_ref), (q2_ref, S2, q2w_ref))):
        above = part(top, section, 32) + jnp.where(rix == 31, rest[comp : comp + 1], 0.0)
        ref[0:32] = widen(above, XO)
        ref[32:160] = own[...]
        ref[160:192] = widen(part(bot, section, 32), XO)
    row_ok, _ = masks()

    def taps(seg, patch):
        return own_ref[patch] if seg == 1 else t_ref[2 * seg + patch]

    def get_x(tile, first):
        return xe_ref[first : first + 256, 128 * tile : 128 * tile + 128]

    def put(seg, first, size, tile, blurred):
        here = slice(128 * tile, 128 * tile + 128)
        new = (c_ref[first : first + size, here] + SIGMA * blurred) * (1.0 / (1.0 + SIGMA))
        ys_ref[first : first + size, here] = new if seg == 1 else jnp.where(row_ok(seg), new, 0.0)

    def get_y(first, size, tile):
        return ys_ref[first : first + size, 128 * tile : 128 * tile + 128]

    windows(get_x, p_ref, range(3, 17), 256)
    blur(SEGS1, INNER, taps, p_ref, a_ref, put)
    z_ref[...] = jnp.zeros_like(z_ref)
    adjoint(SEGS1, INNER, taps, get_y, l_ref, f_ref, z_ref, (32, 224))


def main_kernel(
    table_ref, ca_ref, cb_ref,
    xi_ref, ci_ref, oi_ref, yi_ref, q1i_ref, q2i_ref, zi_ref, ti_ref, own_ref,
    x2_ref, y2_hbm,
    side_ref, qs_ref, ys_ref, c_ref, q1_ref, q2_ref, tab_ref, t_ref, p_ref, a_ref, l_ref, f_ref,
    z_ref, xb_ref, x1_ref, y2_ref, sem,
):
    top_ok, bot_ok, left_ok, right_ok = flags()
    _, odd_col = parities()
    before, after = sides(ca_ref, cb_ref, odd_col)
    first, second = slice(0, 256), slice(256, 448)
    lf0, lf1, rt0, rt1 = before(first), before(second), after(first), after(second)
    gap = jnp.zeros((48, 128), F32)

    def from_row(value, count):
        return jnp.concatenate([gap[: count // 2 - 80], value[0:160], gap[: count // 2 - 80]], axis=0)

    lane = iota((1, 128), 1)
    total = jnp.full((1, 128), -1.0, F32)
    for r in range(3):
        total = jnp.where(lane == 8 * r, lf1[r : r + 1, 18:19], total)
        total = jnp.where(lane == 8 * r + 5, rt1[r : r + 1, 112:113], total)
    select_tables(table_ref, total, tab_ref)
    build_taps(tab_ref, t_ref, [8 * r + p for r in range(3) for p in (0, 5)])

    def taps(seg, patch):
        if 0 <= patch < 4:
            return own_ref[patch] if seg == 1 else ti_ref[2 * seg + patch]
        return t_ref[2 * seg + (patch == 4)]

    rr = iota((256, 128), 0)
    rows_ok = ((rr >= 64) | top_ok) & ((rr < 192) | bot_ok)
    shape = (256, 128)
    part = jnp.where(between(shape, 16, 80), lf0, 0.0)
    part += jnp.where(between(shape, 64, 80), lanes(from_row(lf1, 256), 80), 0.0)
    side_ref[0, 0:256] = xi_ref[0:256, 0:128] + jnp.where(rows_ok & left_ok, part, 0.0)
    part = jnp.where(between(shape, 80, 128), rt0, 0.0)
    part += jnp.where(between(shape, 80, 96), lanes(from_row(rt1, 256), 48), 0.0)
    side_ref[1, 0:256] = xi_ref[0:256, 512:640] + jnp.where(rows_ok & right_ok, part, 0.0)
    part = jnp.where(between(shape, 0, 16), rt0, 0.0)
    side_ref[2, 0:256] = xi_ref[0:256, 640:768] + jnp.where(rows_ok & right_ok, part, 0.0)
    side_ref[:, 256:272] = jnp.zeros((3, 16, 128), F32)
    shape = (192, 128)
    for comp, ref in enumerate((q1i_ref, q2i_ref)):
        part = lanes(lf1[0:192], 96 * comp)
        part += jnp.where(between(shape, 79, 80), lanes(lf1[0:192], 63 - comp), 0.0)
        qs_ref[comp, 0] = jnp.where(between(shape, 48, 80), part, ref[:, 0:128])
        part = lanes(rt1[0:192], 80 * comp)
        qs_ref[comp, 1] = jnp.where(between(shape, 80, 112), part, ref[:, 512:640])
    shape = (224, 128)
    part = lanes(lf0[0:224], 64) + jnp.where(between(shape, 48, 64), lanes(from_row(lf1, 224), 48), 0.0)
    c_first = jnp.where(between(shape, 16, 64), part, ci_ref[:, 0:128])
    part = lanes(rt0[0:224], 48) + jnp.where(between(shape, 64, 80), from_row(rt1, 224), 0.0)
    c_last = jnp.where(between(shape, 64, 112), part, ci_ref[:, 512:640])
    shape = (160, 128)
    o_first = jnp.where(between(shape, 48, 64), lanes(lf0[0:160], 48), oi_ref[:, 0:128])
    o_last = jnp.where(between(shape, 64, 80), rt0[0:160], oi_ref[:, 512:640])
    row_ok, col_ok = masks()

    def get_side(tile, first):
        which = {0: 0, 4: 1, 5: 2}[tile]
        return side_ref[which, first : first + 256]

    def put_side(seg, first, size, tile, blurred):
        c = (c_first if tile == 0 else c_last)[first : first + size]
        new = (c + SIGMA * blurred) * (1.0 / (1.0 + SIGMA))
        new = jnp.where(col_ok(tile, size) & row_ok(seg), new, 0.0)
        old = yi_ref[first : first + size, 128 * tile : 128 * tile + 128]
        inner = between((size, 128), 96, 128) if tile == 0 else between((size, 128), 0, 32)
        ys_ref[tile // 4, first : first + size] = jnp.where(inner, old, new)

    def get_side_y(first, size, tile):
        return ys_ref[tile // 4, first : first + size]

    windows(get_side, p_ref, (0, 1, 2, 17, 18, 19), 256)
    blur(SEGS1, OUTER, taps, p_ref, a_ref, put_side)

    def get_x(start, count):
        at = pl.ds(start + 32, count)
        return jnp.concatenate([side_ref[0, at], xi_ref[at, 128:512], side_ref[1, at]], axis=1)

    def get_q(comp, start):
        at = pl.ds(start, CHUNK)
        ref = q2i_ref if comp else q1i_ref
        return jnp.concatenate([qs_ref[comp, 0, at], ref[at, 128:512], qs_ref[comp, 1, at]], axis=1)

    q1_ref[0:8] = jnp.zeros((8, WIDE), F32)
    total_variation(get_x, get_q, q1_ref, q2_ref, 192)
    z_ref[32:224] = zi_ref[32:224]
    adjoint(SEGS1, OUTER, taps, get_side_y, l_ref, f_ref, z_ref, (32, 224))

    def first_update(start):
        lane = iota((CHUNK, 128), 1)
        x = get_x(start, CHUNK)
        new = x - TAU * (z_ref[pl.ds(start + 32, CHUNK)] - divergence(q1_ref, q2_ref, start))
        ahead = 2.0 * new - x
        ahead = on_tile(ahead, 0, lambda part: unless((lane < XO) & jnp.logical_not(left_ok), part))
        past = (lane + 512 - XO >= COLS) & jnp.logical_not(right_ok)
        ahead = on_tile(ahead, 4, lambda part: unless(past, part))
        row = start - 32 + iota((CHUNK, WIDE), 0)
        keep = ((row >= 0) | top_ok) & ((row < ROWS) | bot_ok)
        xb_ref[pl.ds(start, CHUNK), 0:WIDE] = jnp.where(keep, ahead, 0.0)
        x1_ref[pl.ds(start, CHUNK)] = new

    chunks(0, 192, first_update)
    xb_ref[192:208, 0:WIDE] = jnp.zeros((16, WIDE), F32)
    xb_ref[:, WIDE:FULL] = jnp.zeros((208, FULL - WIDE), F32)
    c_ref[:, 0:128] = ys_ref[0, 32:192] - SIGMA * o_first
    c_ref[:, 128:512] = yi_ref[32:192, 128:512] - SIGMA * oi_ref[:, 128:512]
    c_ref[:, 512:640] = ys_ref[1, 32:192] - SIGMA * o_last

    def get_xb(tile, first):
        return xb_ref[first : first + 192, 128 * tile : 128 * tile + 128]

    def put(seg, first, size, tile, blurred):
        here = slice(128 * tile, 128 * tile + 128)
        new = (c_ref[first : first + size, here] + SIGMA * blurred) * (1.0 / (1.0 + SIGMA))
        if seg != 1 or tile in (0, 4):
            new = jnp.where(col_ok(tile, size) & row_ok(seg), new, 0.0)
        c_ref[first : first + size, here] = new

    def get_y(first, size, tile):
        return c_ref[first : first + size, 128 * tile : 128 * tile + 128]

    windows(get_xb, p_ref, range(1, 19), 192)
    blur(SEGS2, ALL, taps, p_ref, a_ref, put)

    def put_y(start):
        y2_ref[pl.ds(start, CHUNK)] = lanes(c_ref[pl.ds(start + 16, CHUNK)], -YO)[:, :COLS]

    chunks(0, ROWS, put_y)
    total_variation(
        lambda start, count: xb_ref[pl.ds(start, count), 0:WIDE],
        lambda comp, start: (q2_ref if comp else q1_ref)[pl.ds(start + 8, CHUNK)],
        q1_ref, q2_ref, 160,
    )
    done = pltpu.make_async_copy(y2_ref, y2_hbm, sem.at[0])
    done.start()
    z_ref[32:160] = jnp.zeros((128, WIDE), F32)
    adjoint(SEGS2, ALL, taps, get_y, l_ref, f_ref, z_ref, (32, 160))

    def second_update(start):
        div = divergence(q1_ref, q2_ref, start)
        new = x1_ref[pl.ds(start, CHUNK)] - TAU * (z_ref[pl.ds(start, CHUNK)] - div)
        x2_ref[pl.ds(start - 32, CHUNK)] = lanes(new, -XO)[:, :COLS]

    chunks(32, ROWS, second_update)
    done.wait()


def field(*shape, dtype=F32):
    return jax.ShapeDtypeStruct(shape, dtype)


def call(kernel, outs, scratch, *args, name, room=4, far=0, flops=0, out_far=0):
    spaces = [pltpu.HBM] * far + [pltpu.VMEM] * (len(args) - far)
    return pl.pallas_call(
        kernel,
        out_shape=outs,
        out_specs=tuple(
            pl.BlockSpec(memory_space=pltpu.HBM if i >= len(outs) - out_far else pltpu.VMEM)
            for i in range(len(outs))
        ),
        in_specs=[pl.BlockSpec(memory_space=space) for space in spaces],
        scratch_shapes=scratch,
        compiler_params=pltpu.CompilerParams(vmem_limit_bytes=int(room * 1024 * 1024)),
        cost_estimate=pl.CostEstimate(flops=flops, bytes_accessed=0, transcendentals=0)
        if flops
        else None,
        name=name,
    )(*args)


def swap(block, axis, first):
    high, wide = lax.axis_size("row"), lax.axis_size("col")

    def partner(row, col):
        if axis == "row":
            to = ((row - first) ^ 1) + first
            return (to, col) if 0 <= to < high else (row, col ^ 2 if wide > 2 else col ^ 1)
        to = ((col - first) ^ 1) + first
        return (row, to) if 0 <= to < wide else (row ^ 1, col)

    pairs = []
    for row in range(high):
        for col in range(wide):
            to_row, to_col = partner(row, col)
            pairs.append((row * wide + col, to_row * wide + to_col))
    return lax.ppermute(block, ("row", "col"), pairs)


def per_device(observed, psf_table, psf_index, start_image, blur_dual, tv_dual):
    own = (start_image, blur_dual, observed, tv_dual)
    block = pltpu.VMEM((ROWS, COLS), F32)
    strip = field(STRIP, COLS, dtype=BF16)
    side = field(448, 128, dtype=BF16)
    a, b = call(
        pack_rows_kernel, (strip, strip),
        [block, block, block, pltpu.VMEM((2, ROWS, COLS), F32), pltpu.SemaphoreType.DMA((4,))],
        *own, psf_index, name="pack_rows", far=4, room=53.3,
    )
    ra = swap(a, "row", 0)
    rb = swap(b, "row", 1)
    table = psf_table.astype(F32)
    normed = (table / jnp.sum(table, axis=(1, 2), keepdims=True)).astype(BF16)
    normed = jnp.pad(normed[:, :, ::-1], ((0, 0), (1, 0), (0, 1))).reshape(64, 1024)
    a, b = call(
        pack_cols_kernel, (side, side), [], *own, psf_index, ra, rb, name="pack_cols"
    )
    ca = swap(a, "col", 0)
    cb = swap(b, "col", 1)
    work = [
        pltpu.VMEM((20, 256, 128), BF16), pltpu.VMEM((20, 144, 128), F32),
        pltpu.VMEM((20, 144, 256), BF16), pltpu.VMEM((20, 176, 128), F32),
    ]
    wide = field(192, WIDE)
    local = field(ROWS, WIDE)
    *fields, taps = call(
        local_kernel,
        (field(ROWS, FULL), local, local, local, local, field(4, 256, 256, dtype=BF16)),
        [pltpu.VMEM((24, 1024), F32)],
        *own, psf_index, normed, name="local", room=4, flops=1 << 32,
    )
    ready = call(
        middle_kernel,
        (
            field(272, FULL), field(224, WIDE), field(160, WIDE), field(224, WIDE), wide, wide,
            field(224, WIDE), field(8, 256, 256, dtype=BF16),
        ),
        [pltpu.VMEM((24, 1024), F32)] + work,
        *fields, taps, normed, ra, rb, name="middle", room=16, flops=1 << 33,
    )
    return call(
        main_kernel,
        (field(ROWS, COLS), field(ROWS, COLS)),
        [
            pltpu.VMEM((3, 272, 128), F32), pltpu.VMEM((2, 2, 192, 128), F32),
            pltpu.VMEM((2, 224, 128), F32), pltpu.VMEM((160, WIDE), F32),
            pltpu.VMEM((200, WIDE), F32), pltpu.VMEM((200, WIDE), F32),
            pltpu.VMEM((24, 1024), F32), pltpu.VMEM((6, 256, 256), BF16),
        ] + work + [
            pltpu.VMEM((224, WIDE), F32), pltpu.VMEM((208, FULL), F32), pltpu.VMEM((192, WIDE), F32),
            pltpu.VMEM((ROWS, COLS), F32), pltpu.SemaphoreType.DMA((1,)),
        ],
        normed, ca, cb, *ready, taps, name="main", room=20, out_far=1,
    )


def solution(mesh):
    placed = (
        P("row", "col"),
        P(),
        P("row", "col"),
        P("row", "col"),
        P("row", "col"),
        P(None, "row", "col"),
    )
    return jax.shard_map(
        per_device,
        mesh=mesh,
        in_specs=placed,
        out_specs=(P("row", "col"), P("row", "col")),
        check_vma=False,
    )
```
